32 devices in a mesh: dp: 2 (over x), tp: 16 (over z, y, core).
Axes of the slice: x: 2, y: 2, z: 4, core: 2. Of those that a mesh axis runs over, the one named last changes fastest.
Arguments:
- x_norm: bfloat16 [8192, 2048], P(('dp', 'tp')), parts along dimension 0
- grad_y: bfloat16 [8192, 2048], P(('dp', 'tp')), parts along dimension 0
- u_gate: bfloat16 [8192, 11008], P('dp', 'tp'), parts along dimension 0
- u_up: bfloat16 [8192, 11008], P('dp', 'tp'), parts along dimension 0
- w_gate: bfloat16 [2048, 11008], P(None, 'tp')
- w_up: bfloat16 [2048, 11008], P(None, 'tp')
- w_down: bfloat16 [11008, 2048], P('tp')
- x_in: bfloat16 [8192, 2048], P(('dp', 'tp')), parts along dimension 0
- gamma: bfloat16 [2048], replicated
- grad_res: bfloat16 [8192, 2048], P(('dp', 'tp')), parts along dimension 0
- attn_out: bfloat16 [8192, 2048], P('dp', 'tp'), parts along dimension 0
- w_out: bfloat16 [2048, 2048], P('tp')
Outputs:
- output 1: bfloat16 [8192, 2048], P(('dp', 'tp')), parts along dimension 0
- output 2: bfloat16 [8192, 2048], P('dp', 'tp'), parts along dimension 0
- output 3: float32 [4096, 11008], P('dp', 'tp'), parts along dimension 0
- output 4: float32 [4096, 11008], P('dp', 'tp'), parts along dimension 0
- output 5: float32 [22016, 2048], P(('dp', 'tp')), parts along dimension 0
- output 6: float32 [4096, 2048], P(('dp', 'tp')), parts along dimension 0
There are 2 independent parts. The reference program is written for one: setup_inputs(seed, part) draws one part's arguments, and reference() takes and returns one part's arrays. A program takes and returns all parts, laid end to end along the dimension named above; an argument that names none is the same for every part.
All inputs are finite; a program needn't handle non-finite values.
Results may differ from the reference program's by a relative error of at most 0.0148682.
Values are sent between devices in bfloat16 or wider.
A program may use at most 1 GiB of HBM per device.

```python
import jax
import jax.numpy as jnp
from jax import lax

HIDDEN = 2048
FFN_DIM = 11008
TOKENS = 4096
NORM_EPS = 1e-5


def setup_inputs(seed: int = 0, part: int = 0) -> dict:
    part_keys = jax.random.split(jax.random.fold_in(jax.random.key(seed), part), 7)
    weight_keys = jax.random.split(jax.random.key(seed + 1), 5)
    xin_keys = jax.random.split(part_keys[4], 2)
    act_shape = (TOKENS, HIDDEN)
    ffn_shape = (TOKENS, FFN_DIM)
    x_norm = jax.random.normal(part_keys[0], act_shape, jnp.float32)
    grad_y = jax.random.normal(part_keys[1], act_shape, jnp.float32)
    u_gate = jax.random.normal(part_keys[2], ffn_shape, jnp.float32)
    u_up = jax.random.normal(part_keys[3], ffn_shape, jnp.float32)
    xin_scale = jnp.exp(jax.random.uniform(xin_keys[0], (TOKENS, 1), jnp.float32, -1.0, 1.0))
    x_in = jax.random.normal(xin_keys[1], act_shape, jnp.float32) * xin_scale
    grad_res = 0.5 * jax.random.normal(part_keys[5], act_shape, jnp.float32)
    attn_out = jax.random.normal(part_keys[6], act_shape, jnp.float32)
    w_gate = jax.random.normal(weight_keys[0], (HIDDEN, FFN_DIM), jnp.float32) * HIDDEN ** -0.5
    w_up = jax.random.normal(weight_keys[1], (HIDDEN, FFN_DIM), jnp.float32) * HIDDEN ** -0.5
    w_down = jax.random.normal(weight_keys[2], (FFN_DIM, HIDDEN), jnp.float32) * FFN_DIM ** -0.5
    w_out = jax.random.normal(weight_keys[3], (HIDDEN, HIDDEN), jnp.float32) * HIDDEN ** -0.5
    gamma = 1.0 + 0.3 * jax.random.normal(weight_keys[4], (HIDDEN,), jnp.float32)
    return dict(
        x_norm=x_norm.astype(jnp.bfloat16),
        grad_y=grad_y.astype(jnp.bfloat16),
        u_gate=u_gate.astype(jnp.bfloat16),
        u_up=u_up.astype(jnp.bfloat16),
        w_gate=w_gate.astype(jnp.bfloat16),
        w_up=w_up.astype(jnp.bfloat16),
        w_down=w_down.astype(jnp.bfloat16),
        x_in=x_in.astype(jnp.bfloat16),
        gamma=gamma.astype(jnp.bfloat16),
        grad_res=grad_res.astype(jnp.bfloat16),
        attn_out=attn_out.astype(jnp.bfloat16),
        w_out=w_out.astype(jnp.bfloat16),
    )


def reference(x_norm, grad_y, u_gate, u_up, w_gate, w_up, w_down, x_in, gamma, grad_res, attn_out, w_out):
    gate_f = u_gate.astype(jnp.float32)
    up_f = u_up.astype(jnp.float32)
    sig_gate = jax.nn.sigmoid(gate_f)
    act_gate = gate_f * sig_gate
    silu_grad = sig_gate * (1.0 + gate_f * (1.0 - sig_gate))
    hidden_z = (act_gate * up_f).astype(jnp.bfloat16)
    gw_down = jnp.dot(hidden_z.T, grad_y, preferred_element_type=jnp.float32)
    grad_h = jnp.dot(grad_y, w_down.T, preferred_element_type=jnp.float32)
    grad_up = (grad_h * act_gate).astype(jnp.bfloat16)
    grad_gate = (grad_h * up_f * silu_grad).astype(jnp.bfloat16)
    grad_x = (jnp.dot(grad_gate, w_gate.T, preferred_element_type=jnp.float32)
              + jnp.dot(grad_up, w_up.T, preferred_element_type=jnp.float32)).astype(jnp.bfloat16)
    gw_gate = jnp.dot(x_norm.T, grad_gate, preferred_element_type=jnp.float32)
    gw_up = jnp.dot(x_norm.T, grad_up, preferred_element_type=jnp.float32)
    xin_f = x_in.astype(jnp.float32)
    inv_rms = lax.rsqrt(jnp.mean(xin_f * xin_f, axis=-1, keepdims=True) + NORM_EPS)
    scaled = grad_x.astype(jnp.float32) * gamma.astype(jnp.float32)
    proj_mean = jnp.mean(scaled * xin_f, axis=-1, keepdims=True)
    grad_sum = (grad_res.astype(jnp.float32)
                + inv_rms * (scaled - xin_f * (inv_rms * inv_rms) * proj_mean)).astype(jnp.bfloat16)
    grad_attn = jnp.dot(grad_sum, w_out.T, preferred_element_type=jnp.float32).astype(jnp.bfloat16)
    gw_out = jnp.dot(attn_out.T, grad_sum, preferred_element_type=jnp.float32)
    return grad_sum, grad_attn, gw_gate, gw_up, gw_down, gw_out
```

```python
import jax
import jax.numpy as jnp
from jax import lax
from jax.experimental import pallas as pl
from jax.experimental.pallas import tpu as pltpu
from jax.sharding import PartitionSpec as P

NORM_EPS = 1e-5
MESH = pl.DeviceIdType.MESH
BF16 = jnp.bfloat16
F32 = jnp.float32

CHIPS = 8
QUARTER = 128
HALF = 64
ROWS = 4 * QUARTER
LAST = CHIPS - 1


def dot_cols(a, b):
    return lax.dot_general(a, b, (((1,), (1,)), ((), ())), preferred_element_type=F32)


def dot_plain(a, b):
    return lax.dot_general(a, b, (((1,), (0,)), ((), ())), preferred_element_type=F32)


def kernel(x, gy, ug, uu, wg, wu, wd, xin, gamma, gres, att, wo,
           out_ds, out_do, out_wg, out_wu, out_wd, out_wo, gy_all, x_all, ds_all,
           wg_v, wu_v, wd_v, acc_g, acc_u, acc_d,
           gy_b, x_b, ug_b, uu_b, z_b, dg_b, du_b, zt_b, xt_b,
           p_own, p_send, p_recv, rs_send, rs_recv, own_sum,
           att_v, wo_v, do_v, acc_o,
           gy_ss, gy_rs, gy_ps, gy_pr, x_ss, x_rs, x_ps, x_pr,
           ds_ss, ds_rs, ds_ps, ds_pr, ps_sem, pr_sem, rss_sem, rsr_sem,
           w_sem, gy_sem, x_sem, ug_sem, uu_sem, o_sem):
    hidden = gy.shape[1]
    t = lax.axis_index("tp")
    core = t % 2
    y = (t // 2) % 2
    z = t // 4
    pos = z + y * (7 - 2 * z)

    def device(chip, c):
        upper = chip // 4
        return 4 * (chip + upper * (7 - 2 * chip)) + 2 * upper + c

    right = device((pos + 1) % CHIPS, core)
    left = device((pos + LAST) % CHIPS, core)
    onward = (right, left)
    twin = t + 1 - 2 * core

    barrier = pltpu.get_barrier_semaphore()
    for other in (right, left, twin):
        pl.semaphore_signal(barrier, inc=1, device_id={"tp": other}, device_id_type=MESH)
    pl.semaphore_wait(barrier, 3)

    def row(s, d, c):
        source = (pos + (CHIPS - s if d == 0 else s)) % CHIPS
        return pl.multiple_of(device(source, c) * 2 * QUARTER + d * QUARTER, QUARTER)

    def remote(src, dst, send, recv, to):
        return pltpu.make_async_remote_copy(src_ref=src, dst_ref=dst, send_sem=send, recv_sem=recv,
                                            device_id={"tp": to}, device_id_type=MESH)

    def pass_on(full, ss, rs, s, d, src=None):
        rows = pl.ds(row(s - 1, d, core), QUARTER)
        return remote(full.at[rows, :] if src is None else src, full.at[rows, :],
                      ss.at[s, d], rs.at[s, d], onward[d])

    def arriving(full, ss, rs, s, d):
        rows = pl.ds(row(s, d, core), QUARTER)
        return remote(full.at[rows, :], full.at[rows, :], ss.at[s, d], rs.at[s, d], onward[d])

    def to_twin(full, ss, rs, s, d, src=None):
        rows = pl.ds(row(s, d, core), QUARTER)
        return remote(full.at[rows, :] if src is None else src, full.at[rows, :],
                      ss.at[s, d], rs.at[s, d], twin)

    def from_twin(full, ss, rs, s, d):
        rows = pl.ds(row(s, d, 1 - core), QUARTER)
        return remote(full.at[rows, :], full.at[rows, :], ss.at[s, d], rs.at[s, d], twin)

    streams = ((gy, gy_all, gy_ss, gy_rs, gy_ps, gy_pr), (x, x_all, x_ss, x_rs, x_ps, x_pr))
    for own, full, ss, rs, ps, pr in streams:
        for d in (0, 1):
            mine = own.at[pl.ds(d * QUARTER, QUARTER), :]
            pass_on(full, ss, rs, 1, d, mine).start()
            to_twin(full, ps, pr, 0, d, mine).start()

    def load(src, dst, i):
        return pltpu.make_async_copy(src, dst, w_sem.at[i])

    loads = [load(a, b, i) for i, (a, b) in enumerate(
        ((wd, wd_v), (wg, wg_v), (wu, wu_v), (att, att_v), (wo, wo_v)))]
    for copy in loads:
        copy.start()

    def load_u(s):
        copies = []
        for d in (0, 1):
            for k in (0, 1):
                c = core if k == 0 else 1 - core
                rows = pl.ds(row(s, d, c), QUARTER)
                at = pl.ds((2 * k + d) * QUARTER, QUARTER)
                copies.append(pltpu.make_async_copy(ug.at[rows, :], ug_b.at[at, :], ug_sem.at[2 * k + d]))
                copies.append(pltpu.make_async_copy(uu.at[rows, :], uu_b.at[at, :], uu_sem.at[2 * k + d]))
        return copies

    for copy in load_u(0):
        copy.start()

    acc_g[...] = jnp.zeros_like(acc_g)
    acc_u[...] = jnp.zeros_like(acc_u)
    acc_d[...] = jnp.zeros_like(acc_d)
    acc_o[...] = jnp.zeros_like(acc_o)
    rs_recv[1] = jnp.zeros_like(rs_recv[1])

    def block_load(own, full, buf, sem, s, d, k):
        c = core if k == 0 else 1 - core
        at = pl.ds((2 * k + d) * QUARTER, QUARTER)
        if own is not None:
            return pltpu.make_async_copy(own.at[pl.ds(d * QUARTER, QUARTER), :], buf.at[at, :], sem.at[2 * k + d])
        return pltpu.make_async_copy(full.at[pl.ds(row(s, d, c), QUARTER), :], buf.at[at, :], sem.at[2 * k + d])

    def receive(stream, buf, sem, s):
        own, full, ss, rs, ps, pr = stream

        @pl.when(s > 0)
        def _():
            for d in (0, 1):
                arriving(full, ss, rs, s, d).wait_recv()

                @pl.when(s < LAST)
                def _():
                    pass_on(full, ss, rs, s + 1, d).start()
                to_twin(full, ps, pr, s, d).start()
            for d in (0, 1):
                block_load(None, full, buf, sem, s, d, 0).start()

        @pl.when(s == 0)
        def _():
            for d in (0, 1):
                block_load(own, full, buf, sem, s, d, 0).start()
        for d in (0, 1):
            from_twin(full, ps, pr, s, d).wait_recv()
            block_load(None, full, buf, sem, s, d, 1).start()

    def landed(full, buf, sem, s):
        for k in (0, 1):
            for d in (0, 1):
                block_load(None, full, buf, sem, s, d, k).wait()

    def swap(s):
        return remote(p_send, p_recv.at[s % 2], ps_sem, pr_sem.at[s % 2], twin)

    def sum_on(s, d):
        return remote(rs_send.at[s % 2, d], rs_recv.at[(s + 1) % 3, d],
                      rss_sem.at[s % 2, d], rsr_sem.at[(s + 1) % 3, d], onward[d])

    def sum_in(s, d):
        return remote(rs_send.at[0, d], rs_recv.at[s % 3, d],
                      rss_sem.at[0, d], rsr_sem.at[s % 3, d], onward[d])

    def step(s, carry):
        receive(streams[0], gy_b, gy_sem, s)
        for copy in load_u(s):
            copy.wait()

        @pl.when(s == 0)
        def _():
            for copy in loads:
                copy.wait()
        landed(gy_all, gy_b, gy_sem, s)

        def hidden_tile(i, carry):
            at = pl.ds(pl.multiple_of(i * 128, 128), 128)
            grad_h = dot_cols(gy_b[at, :], wd_v[...])
            gate = ug_b[at, :].astype(F32)
            up = uu_b[at, :].astype(F32)
            sig = jax.nn.sigmoid(gate)
            act = gate * sig
            z_b[at, :] = (act * up).astype(BF16)
            du_b[at, :] = (grad_h * act).astype(BF16)
            dg_b[at, :] = (grad_h * up * (sig * (1.0 + gate * (1.0 - sig)))).astype(BF16)
            return carry
        lax.fori_loop(0, ROWS // 128, hidden_tile, 0)

        @pl.when(s < LAST)
        def _():
            for copy in load_u(s + 1):
                copy.start()

        @pl.when(s > 0)
        def _():
            swap(s - 1).wait_send()

        def part_tile(j, carry):
            at = pl.ds(pl.multiple_of(j * 512, 512), 512)
            part = dot_cols(dg_b[...], wg_v[at, :]) + dot_cols(du_b[...], wu_v[at, :])
            p_own[:, at] = part[:2 * QUARTER]
            p_send[:, at] = part[2 * QUARTER:].astype(BF16)
            return carry
        lax.fori_loop(0, hidden // 512, part_tile, 0)
        swap(s).start()

        receive(streams[1], x_b, x_sem, s)

        def zt_tile(i, carry):
            at = pl.ds(pl.multiple_of(i * 128, 128), 128)
            zt_b[:, at] = z_b[at, :].T
            return carry
        lax.fori_loop(0, ROWS // 128, zt_tile, 0)

        swap(s).wait_recv()

        @pl.when(s == 0)
        def _():
            def tile(i, carry):
                at = pl.ds(pl.multiple_of(i * 32, 32), 32)
                own_sum[at, :] = p_own[at, :] + p_recv[0, at, :].astype(F32)
                return carry
            lax.fori_loop(0, 2 * QUARTER // 32, tile, 0)

        @pl.when(s > 0)
        def _():
            for d in (0, 1):
                @pl.when(s > 1)
                def _():
                    sum_in(s, d).wait_recv()

                @pl.when(s > 2)
                def _():
                    sum_on(s - 2, d).wait_send()

                def tile(i, carry):
                    at = pl.ds(pl.multiple_of(i * 32, 32), 32)
                    here = pl.ds(pl.multiple_of(d * QUARTER + i * 32, 32), 32)
                    total = (p_own[here, :] + p_recv[s % 2, here, :].astype(F32)
                             + rs_recv[s % 3, d, at, :].astype(F32))
                    rs_send[s % 2, d, at, :] = total.astype(BF16)
                    return carry
                lax.fori_loop(0, QUARTER // 32, tile, 0)
                sum_on(s, d).start()

        def down_tile(j, carry):
            at = pl.ds(pl.multiple_of(j * 512, 512), 512)
            acc_d[:, at] += dot_plain(zt_b[...], gy_b[:, at])
            return carry
        lax.fori_loop(0, hidden // 512, down_tile, 0)

        landed(x_all, x_b, x_sem, s)

        def xt_tile(i, carry):
            at = pl.ds(pl.multiple_of(i * 128, 128), 128)
            xt_b[at, :] = x_b[:, at].T
            return carry
        lax.fori_loop(0, hidden // 128, xt_tile, 0)

        def up_tile(i, carry):
            at = pl.ds(pl.multiple_of(i * 512, 512), 512)
            acc_g[at, :] += dot_plain(xt_b[at, :], dg_b[...])
            acc_u[at, :] += dot_plain(xt_b[at, :], du_b[...])
            return carry
        lax.fori_loop(0, hidden // 512, up_tile, 0)
        return carry

    lax.fori_loop(0, CHIPS, step, 0)

    stores = [pltpu.make_async_copy(a, b, o_sem.at[i]) for i, (a, b) in enumerate(
        ((acc_g, out_wg), (acc_u, out_wu), (acc_d, out_wd)))]
    for copy in stores:
        copy.start()

    norm_loads = [pltpu.make_async_copy(src, x_b.at[pl.ds(k * 2 * QUARTER, 2 * QUARTER), :], x_sem.at[k])
                  for k, src in enumerate((xin, gres))]
    for copy in norm_loads:
        copy.start()
    for copy in norm_loads:
        copy.wait()
    swap(LAST).wait_send()

    def ds_next(s, d, h, src=None):
        rows = pl.ds(pl.multiple_of(row(s - 1, d, core) + h * HALF, HALF), HALF)
        return remote(ds_all.at[rows, :] if src is None else src, ds_all.at[rows, :],
                      ds_ss.at[s, 2 * d + h], ds_rs.at[s, 2 * d + h], onward[d])

    def ds_here(s, d, h):
        rows = pl.ds(pl.multiple_of(row(s, d, core) + h * HALF, HALF), HALF)
        return remote(ds_all.at[rows, :], ds_all.at[rows, :],
                      ds_ss.at[s, 2 * d + h], ds_rs.at[s, 2 * d + h], onward[d])

    def ds_twin(s, d, h, src=None):
        rows = pl.ds(pl.multiple_of(row(s, d, core) + h * HALF, HALF), HALF)
        return remote(ds_all.at[rows, :] if src is None else src, ds_all.at[rows, :],
                      ds_ps.at[s, 2 * d + h], ds_pr.at[s, 2 * d + h], twin)

    def ds_from_twin(s, d, h):
        rows = pl.ds(pl.multiple_of(row(s, d, 1 - core) + h * HALF, HALF), HALF)
        return remote(ds_all.at[rows, :], ds_all.at[rows, :],
                      ds_ps.at[s, 2 * d + h], ds_pr.at[s, 2 * d + h], twin)

    gain = gamma[...].astype(F32)
    for d in (0, 1):
        sum_in(CHIPS, d).wait_recv()
    for h in (0, 1):
        for d in (0, 1):
            def norm_tile(i, carry):
                at = pl.ds(pl.multiple_of(h * HALF + i * 16, 16), 16)
                here = pl.ds(pl.multiple_of(d * QUARTER + h * HALF + i * 16, 16), 16)
                skip = pl.ds(pl.multiple_of(2 * QUARTER + d * QUARTER + h * HALF + i * 16, 16), 16)
                grad_x = (own_sum[here, :] + rs_recv[CHIPS % 3, d, at, :].astype(F32)).astype(BF16).astype(F32)
                xin_f = x_b[here, :].astype(F32)
                inv_rms = lax.rsqrt(jnp.mean(xin_f * xin_f, axis=-1, keepdims=True) + NORM_EPS)
                scaled = grad_x * gain
                proj = jnp.mean(scaled * xin_f, axis=-1, keepdims=True)
                grad_s = (x_b[skip, :].astype(F32)
                          + inv_rms * (scaled - xin_f * (inv_rms * inv_rms) * proj)).astype(BF16)
                p_send[here, :] = grad_s
                gy_b[here, :] = grad_s
                return carry
            lax.fori_loop(0, HALF // 16, norm_tile, 0)
            mine = p_send.at[pl.ds(d * QUARTER + h * HALF, HALF), :]
            ds_next(1, d, h, mine).start()
            ds_twin(0, d, h, mine).start()
    store_ds = pltpu.make_async_copy(p_send, out_ds, o_sem.at[3])
    store_ds.start()

    def project(s):
        for d in (0, 1):
            for h in (0, 1):
                ds_from_twin(s, d, h).wait_recv()
            block_load(None, ds_all, gy_b, gy_sem, s, d, 1).start()
        for d in (0, 1):
            block_load(None, ds_all, gy_b, gy_sem, s, d, 1).wait()
        for k in (0, 1):
            for d in (0, 1):
                c = core if k == 0 else 1 - core
                rows = pl.ds(row(s, d, c), QUARTER)
                at = pl.ds((2 * k + d) * QUARTER, QUARTER)
                zt_b[pl.ds(0, QUARTER), at] = att_v[rows, :].T
        grad_o = dot_cols(gy_b[...], wo_v[...]).astype(BF16)
        for k in (0, 1):
            for d in (0, 1):
                c = core if k == 0 else 1 - core
                do_v[pl.ds(row(s, d, c), QUARTER), :] = grad_o[(2 * k + d) * QUARTER:(2 * k + d + 1) * QUARTER]
        for j in range(0, hidden, 512):
            acc_o[:, j:j + 512] += dot_plain(zt_b[pl.ds(0, QUARTER), :], gy_b[:, j:j + 512])

    def ds_relay(s, h):
        for d in (0, 1):
            ds_here(s, d, h).wait_recv()

            @pl.when(s < LAST)
            def _():
                ds_next(s + 1, d, h).start()
            ds_twin(s, d, h).start()

    def ds_step(s, carry):
        ds_relay(s, 0)
        project(s - 1)
        ds_relay(s, 1)
        for d in (0, 1):
            block_load(None, ds_all, gy_b, gy_sem, s, d, 0).start()
        for d in (0, 1):
            block_load(None, ds_all, gy_b, gy_sem, s, d, 0).wait()
        return carry

    lax.fori_loop(1, CHIPS, ds_step, 0)
    project(LAST)

    last = [pltpu.make_async_copy(do_v, out_do, o_sem.at[4]), pltpu.make_async_copy(acc_o, out_wo, o_sem.at[5])]
    for copy in last:
        copy.start()

    def drain(s, carry):
        for d in (0, 1):
            to_twin(gy_all, gy_ps, gy_pr, s, d).wait_send()
            to_twin(x_all, x_ps, x_pr, s, d).wait_send()
            for h in (0, 1):
                ds_twin(s, d, h).wait_send()

            @pl.when(s > 0)
            def _():
                arriving(gy_all, gy_ss, gy_rs, s, d).wait_send()
                arriving(x_all, x_ss, x_rs, s, d).wait_send()
                for h in (0, 1):
                    ds_here(s, d, h).wait_send()
        return carry
    lax.fori_loop(0, CHIPS, drain, 0)
    for d in (0, 1):
        sum_on(LAST - 1, d).wait_send()
        sum_on(LAST, d).wait_send()
    for copy in stores + [store_ds] + last:
        copy.wait()


def solution(mesh):
    token_spec = P(("dp", "tp"), None)
    split_cols = P("dp", "tp")
    weight_cols = P(None, "tp")
    weight_rows = P("tp", None)

    def local_backward(x_norm, grad_y, u_gate, u_up, w_gate, w_up, w_down, x_in, gamma, grad_res, attn_out, w_out):
        own, hidden = x_norm.shape
        tokens, ffn = u_gate.shape
        cols = attn_out.shape[1]
        anywhere = pl.BlockSpec(memory_space=pl.ANY)
        shape = jax.ShapeDtypeStruct
        dma = pltpu.SemaphoreType.DMA
        outs = pl.pallas_call(
            kernel,
            out_shape=[
                shape((own, hidden), BF16), shape((tokens, cols), BF16),
                shape((hidden, ffn), F32), shape((hidden, ffn), F32), shape((ffn, hidden), F32),
                shape((cols, hidden), F32),
                shape((tokens, hidden), BF16), shape((tokens, hidden), BF16), shape((tokens, hidden), BF16),
            ],
            in_specs=[anywhere] * 8 + [pl.BlockSpec(memory_space=pltpu.VMEM)] + [anywhere] * 3,
            out_specs=[anywhere] * 9,
            scratch_shapes=[
                pltpu.VMEM((hidden, ffn), BF16), pltpu.VMEM((hidden, ffn), BF16), pltpu.VMEM((ffn, hidden), BF16),
                pltpu.VMEM((hidden, ffn), F32), pltpu.VMEM((hidden, ffn), F32), pltpu.VMEM((ffn, hidden), F32),
                pltpu.VMEM((ROWS, hidden), BF16), pltpu.VMEM((ROWS, hidden), BF16),
                pltpu.VMEM((ROWS, ffn), BF16), pltpu.VMEM((ROWS, ffn), BF16),
                pltpu.VMEM((ROWS, ffn), BF16), pltpu.VMEM((ROWS, ffn), BF16), pltpu.VMEM((ROWS, ffn), BF16),
                pltpu.VMEM((ffn, ROWS), BF16), pltpu.VMEM((hidden, ROWS), BF16),
                pltpu.VMEM((own, hidden), F32), pltpu.VMEM((own, hidden), BF16), pltpu.VMEM((2, own, hidden), BF16),
                pltpu.VMEM((2, 2, QUARTER, hidden), BF16), pltpu.VMEM((3, 2, QUARTER, hidden), BF16),
                pltpu.VMEM((own, hidden), F32),
                pltpu.VMEM((tokens, cols), BF16), pltpu.VMEM((cols, hidden), BF16),
                pltpu.VMEM((tokens, cols), BF16), pltpu.VMEM((cols, hidden), F32),
                dma((CHIPS, 2)), dma((CHIPS, 2)), dma((CHIPS, 2)), dma((CHIPS, 2)),
                dma((CHIPS, 2)), dma((CHIPS, 2)), dma((CHIPS, 2)), dma((CHIPS, 2)),
                dma((CHIPS, 4)), dma((CHIPS, 4)), dma((CHIPS, 4)), dma((CHIPS, 4)),
                dma, dma((2,)), dma((2, 2)), dma((3, 2)),
                dma((5,)), dma((4,)), dma((4,)), dma((4,)), dma((4,)), dma((6,)),
            ],
            compiler_params=pltpu.CompilerParams(
                collective_id=0, has_side_effects=True, vmem_limit_bytes=67_043_328),
            name="mlp_backward",
        )(x_norm, grad_y, u_gate, u_up, w_gate, w_up, w_down, x_in, gamma.reshape(1, hidden), grad_res,
          attn_out, w_out)
        return tuple(outs[:6])

    return jax.shard_map(
        local_backward,
        mesh=mesh,
        in_specs=(token_spec, token_spec, split_cols, split_cols, weight_cols, weight_cols, weight_rows,
                  token_spec, P(None), token_spec, split_cols, weight_rows),
        out_specs=(token_spec, split_cols, split_cols, split_cols, token_spec, token_spec),
        check_vma=False,
    )
```

```python
import jax
import jax.numpy as jnp
from jax import lax
from jax.experimental import pallas as pl
from jax.experimental.pallas import tpu as pltpu
from jax.sharding import PartitionSpec as P

NORM_EPS = 1e-5
MESH = pl.DeviceIdType.MESH
BF16 = jnp.bfloat16
F32 = jnp.float32

CHIPS = 8
QUARTER = 128
HALF = 64
ROWS = 4 * QUARTER
LAST = CHIPS - 1


def dot_cols(a, b):
    return lax.dot_general(a, b, (((1,), (1,)), ((), ())), preferred_element_type=F32)


def dot_plain(a, b):
    return lax.dot_general(a, b, (((1,), (0,)), ((), ())), preferred_element_type=F32)


def kernel(x, gy, ug, uu, wg, wu, wd, xin, gamma, gres, att, wo,
           out_ds, do_v, acc_g, acc_u, acc_d, acc_o, gy_all, x_all, ds_all,
           wg_v, wu_v, wd_v,
           gy_b, x_b, ug_b, uu_b, z_b, dg_b, du_b, dgt_b, dut_b,
           p_own, p_send, p_recv, rs_send, rs_recv, own_sum,
           att_v, wo_v,
           gy_ss, gy_rs, gy_ps, gy_pr, x_ss, x_rs, x_ps, x_pr,
           ds_ss, ds_rs, ds_ps, ds_pr, ps_sem, pr_sem, rss_sem, rsr_sem,
           w_sem, gy_sem, x_sem, ug_sem, uu_sem):
    hidden = gy.shape[1]
    t = lax.axis_index("tp")
    core = t % 2
    y = (t // 2) % 2
    z = t // 4
    pos = z + y * (7 - 2 * z)

    def device(chip, c):
        upper = chip // 4
        return 4 * (chip + upper * (7 - 2 * chip)) + 2 * upper + c

    right = device((pos + 1) % CHIPS, core)
    left = device((pos + LAST) % CHIPS, core)
    onward = (right, left)
    twin = t + 1 - 2 * core

    barrier = pltpu.get_barrier_semaphore()
    for other in (right, left, twin):
        pl.semaphore_signal(barrier, inc=1, device_id={"tp": other}, device_id_type=MESH)
    pl.semaphore_wait(barrier, 3)

    def row(s, d, c):
        source = (pos + (CHIPS - s if d == 0 else s)) % CHIPS
        return pl.multiple_of(device(source, c) * 2 * QUARTER + d * QUARTER, QUARTER)

    def remote(src, dst, send, recv, to):
        return pltpu.make_async_remote_copy(src_ref=src, dst_ref=dst, send_sem=send, recv_sem=recv,
                                            device_id={"tp": to}, device_id_type=MESH)

    def pass_on(full, ss, rs, s, d, src=None):
        rows = pl.ds(row(s - 1, d, core), QUARTER)
        return remote(full.at[rows, :] if src is None else src, full.at[rows, :],
                      ss.at[s, d], rs.at[s, d], onward[d])

    def arriving(full, ss, rs, s, d):
        rows = pl.ds(row(s, d, core), QUARTER)
        return remote(full.at[rows, :], full.at[rows, :], ss.at[s, d], rs.at[s, d], onward[d])

    def to_twin(full, ss, rs, s, d, src=None):
        rows = pl.ds(row(s, d, core), QUARTER)
        return remote(full.at[rows, :] if src is None else src, full.at[rows, :],
                      ss.at[s, d], rs.at[s, d], twin)

    def from_twin(full, ss, rs, s, d):
        rows = pl.ds(row(s, d, 1 - core), QUARTER)
        return remote(full.at[rows, :], full.at[rows, :], ss.at[s, d], rs.at[s, d], twin)

    streams = ((gy, gy_all, gy_ss, gy_rs, gy_ps, gy_pr), (x, x_all, x_ss, x_rs, x_ps, x_pr))
    for own, full, ss, rs, ps, pr in streams:
        for d in (0, 1):
            mine = own.at[pl.ds(d * QUARTER, QUARTER), :]
            pass_on(full, ss, rs, 1, d, mine).start()
            to_twin(full, ps, pr, 0, d, mine).start()

    def load(src, dst, i):
        return pltpu.make_async_copy(src, dst, w_sem.at[i])

    loads = [load(a, b, i) for i, (a, b) in enumerate(
        ((wd, wd_v), (wg, wg_v), (wu, wu_v), (att, att_v), (wo, wo_v)))]
    for copy in loads:
        copy.start()

    def load_u(s):
        copies = []
        for d in (0, 1):
            for k in (0, 1):
                c = core if k == 0 else 1 - core
                rows = pl.ds(row(s, d, c), QUARTER)
                at = pl.ds((2 * k + d) * QUARTER, QUARTER)
                copies.append(pltpu.make_async_copy(ug.at[:, rows], ug_b.at[:, at], ug_sem.at[2 * k + d]))
                copies.append(pltpu.make_async_copy(uu.at[:, rows], uu_b.at[:, at], uu_sem.at[2 * k + d]))
        return copies

    for copy in load_u(0):
        copy.start()

    acc_g[...] = jnp.zeros_like(acc_g)
    acc_u[...] = jnp.zeros_like(acc_u)
    acc_d[...] = jnp.zeros_like(acc_d)
    acc_o[...] = jnp.zeros_like(acc_o)
    rs_recv[1] = jnp.zeros_like(rs_recv[1])

    def block_load(own, full, buf, sem, s, d, k):
        c = core if k == 0 else 1 - core
        at = pl.ds((2 * k + d) * QUARTER, QUARTER)
        if own is not None:
            return pltpu.make_async_copy(own.at[pl.ds(d * QUARTER, QUARTER), :], buf.at[at, :], sem.at[2 * k + d])
        return pltpu.make_async_copy(full.at[pl.ds(row(s, d, c), QUARTER), :], buf.at[at, :], sem.at[2 * k + d])

    def receive(stream, buf, sem, s):
        own, full, ss, rs, ps, pr = stream

        @pl.when(s > 0)
        def _():
            for d in (0, 1):
                arriving(full, ss, rs, s, d).wait_recv()

                @pl.when(s < LAST)
                def _():
                    pass_on(full, ss, rs, s + 1, d).start()
                to_twin(full, ps, pr, s, d).start()
            for d in (0, 1):
                block_load(None, full, buf, sem, s, d, 0).start()

        @pl.when(s == 0)
        def _():
            for d in (0, 1):
                block_load(own, full, buf, sem, s, d, 0).start()
        for d in (0, 1):
            from_twin(full, ps, pr, s, d).wait_recv()
            block_load(None, full, buf, sem, s, d, 1).start()

    def landed(full, buf, sem, s):
        for k in (0, 1):
            for d in (0, 1):
                block_load(None, full, buf, sem, s, d, k).wait()

    def swap(s):
        return remote(p_send, p_recv.at[s % 2], ps_sem, pr_sem.at[s % 2], twin)

    def sum_on(s, d):
        return remote(rs_send.at[s % 2, d], rs_recv.at[(s + 1) % 3, d],
                      rss_sem.at[s % 2, d], rsr_sem.at[(s + 1) % 3, d], onward[d])

    def sum_in(s, d):
        return remote(rs_send.at[0, d], rs_recv.at[s % 3, d],
                      rss_sem.at[0, d], rsr_sem.at[s % 3, d], onward[d])

    def step(s, carry):
        receive(streams[0], gy_b, gy_sem, s)
        for copy in load_u(s):
            copy.wait()

        @pl.when(s == 0)
        def _():
            for copy in loads:
                copy.wait()
        landed(gy_all, gy_b, gy_sem, s)

        def hidden_tile(i, carry):
            at = pl.ds(pl.multiple_of(i * 256, 256), 256)
            grad_h = dot_cols(wd_v[...], gy_b[at, :])
            gate = ug_b[:, at].astype(F32)
            up = uu_b[:, at].astype(F32)
            sig = jax.nn.sigmoid(gate)
            act = gate * sig
            z_b[:, at] = (act * up).astype(BF16)
            grad_up = (grad_h * act).astype(BF16)
            grad_gate = (grad_h * up * (sig * (1.0 + gate * (1.0 - sig)))).astype(BF16)
            du_b[:, at] = grad_up
            dg_b[:, at] = grad_gate
            dut_b[at, :] = grad_up.T
            dgt_b[at, :] = grad_gate.T
            return carry
        lax.fori_loop(0, ROWS // 256, hidden_tile, 0)

        @pl.when(s < LAST)
        def _():
            for copy in load_u(s + 1):
                copy.start()

        @pl.when(s > 0)
        def _():
            swap(s - 1).wait_send()

        def part_tile(j, carry):
            at = pl.ds(pl.multiple_of(j * 512, 512), 512)
            part = dot_plain(dgt_b[...], wg_v[:, at]) + dot_plain(dut_b[...], wu_v[:, at])
            p_own[:, at] = part[:2 * QUARTER]
            p_send[:, at] = part[2 * QUARTER:].astype(BF16)
            return carry
        lax.fori_loop(0, hidden // 512, part_tile, 0)
        swap(s).start()

        receive(streams[1], x_b, x_sem, s)

        swap(s).wait_recv()

        @pl.when(s == 0)
        def _():
            def tile(i, carry):
                at = pl.ds(pl.multiple_of(i * 32, 32), 32)
                own_sum[at, :] = p_own[at, :] + p_recv[0, at, :].astype(F32)
                return carry
            lax.fori_loop(0, 2 * QUARTER // 32, tile, 0)

        @pl.when(s > 0)
        def _():
            for d in (0, 1):
                @pl.when(s > 1)
                def _():
                    sum_in(s, d).wait_recv()

                @pl.when(s > 2)
                def _():
                    sum_on(s - 2, d).wait_send()

                def tile(i, carry):
                    at = pl.ds(pl.multiple_of(i * 32, 32), 32)
                    here = pl.ds(pl.multiple_of(d * QUARTER + i * 32, 32), 32)
                    total = (p_own[here, :] + p_recv[s % 2, here, :].astype(F32)
                             + rs_recv[s % 3, d, at, :].astype(F32))
                    rs_send[s % 2, d, at, :] = total.astype(BF16)
                    return carry
                lax.fori_loop(0, QUARTER // 32, tile, 0)
                sum_on(s, d).start()

        def down_tile(j, carry):
            at = pl.ds(pl.multiple_of(j * 512, 512), 512)
            acc_d[:, at] += dot_plain(z_b[...], gy_b[:, at])
            return carry
        lax.fori_loop(0, hidden // 512, down_tile, 0)

        landed(x_all, x_b, x_sem, s)

        def up_tile(j, carry):
            at = pl.ds(pl.multiple_of(j * 512, 512), 512)
            acc_g[:, at] += dot_plain(dg_b[...], x_b[:, at])
            acc_u[:, at] += dot_plain(du_b[...], x_b[:, at])
            return carry
        lax.fori_loop(0, hidden // 512, up_tile, 0)
        return carry

    lax.fori_loop(0, CHIPS, step, 0)

    norm_loads = [pltpu.make_async_copy(src, x_b.at[pl.ds(k * 2 * QUARTER, 2 * QUARTER), :], x_sem.at[k])
                  for k, src in enumerate((xin, gres))]
    for copy in norm_loads:
        copy.start()
    for copy in norm_loads:
        copy.wait()
    swap(LAST).wait_send()

    def ds_next(s, d, h, src=None):
        rows = pl.ds(pl.multiple_of(row(s - 1, d, core) + h * HALF, HALF), HALF)
        return remote(ds_all.at[rows, :] if src is None else src, ds_all.at[rows, :],
                      ds_ss.at[s, 2 * d + h], ds_rs.at[s, 2 * d + h], onward[d])

    def ds_here(s, d, h):
        rows = pl.ds(pl.multiple_of(row(s, d, core) + h * HALF, HALF), HALF)
        return remote(ds_all.at[rows, :], ds_all.at[rows, :],
                      ds_ss.at[s, 2 * d + h], ds_rs.at[s, 2 * d + h], onward[d])

    def ds_twin(s, d, h, src=None):
        rows = pl.ds(pl.multiple_of(row(s, d, core) + h * HALF, HALF), HALF)
        return remote(ds_all.at[rows, :] if src is None else src, ds_all.at[rows, :],
                      ds_ps.at[s, 2 * d + h], ds_pr.at[s, 2 * d + h], twin)

    def ds_from_twin(s, d, h):
        rows = pl.ds(pl.multiple_of(row(s, d, 1 - core) + h * HALF, HALF), HALF)
        return remote(ds_all.at[rows, :], ds_all.at[rows, :],
                      ds_ps.at[s, 2 * d + h], ds_pr.at[s, 2 * d + h], twin)

    gain = gamma[...].astype(F32)[None, :]
    for d in (0, 1):
        sum_in(CHIPS, d).wait_recv()
    for h in (0, 1):
        for d in (0, 1):
            def norm_tile(i, carry):
                at = pl.ds(pl.multiple_of(h * HALF + i * 16, 16), 16)
                here = pl.ds(pl.multiple_of(d * QUARTER + h * HALF + i * 16, 16), 16)
                skip = pl.ds(pl.multiple_of(2 * QUARTER + d * QUARTER + h * HALF + i * 16, 16), 16)
                grad_x = (own_sum[here, :] + rs_recv[CHIPS % 3, d, at, :].astype(F32)).astype(BF16).astype(F32)
                xin_f = x_b[here, :].astype(F32)
                inv_rms = lax.rsqrt(jnp.mean(xin_f * xin_f, axis=-1, keepdims=True) + NORM_EPS)
                scaled = grad_x * gain
                proj = jnp.mean(scaled * xin_f, axis=-1, keepdims=True)
                grad_s = (x_b[skip, :].astype(F32)
                          + inv_rms * (scaled - xin_f * (inv_rms * inv_rms) * proj)).astype(BF16)
                out_ds[here, :] = grad_s
                gy_b[here, :] = grad_s
                return carry
            lax.fori_loop(0, HALF // 16, norm_tile, 0)
            mine = out_ds.at[pl.ds(d * QUARTER + h * HALF, HALF), :]
            ds_next(1, d, h, mine).start()
            ds_twin(0, d, h, mine).start()

    def project(s):
        for d in (0, 1):
            for h in (0, 1):
                ds_from_twin(s, d, h).wait_recv()
            block_load(None, ds_all, gy_b, gy_sem, s, d, 1).start()
        for d in (0, 1):
            block_load(None, ds_all, gy_b, gy_sem, s, d, 1).wait()
        for k in (0, 1):
            for d in (0, 1):
                c = core if k == 0 else 1 - core
                rows = pl.ds(row(s, d, c), QUARTER)
                at = pl.ds((2 * k + d) * QUARTER, QUARTER)
                z_b[pl.ds(0, QUARTER), at] = att_v[rows, :].T
        grad_o = dot_cols(gy_b[...], wo_v[...]).astype(BF16)
        for k in (0, 1):
            for d in (0, 1):
                c = core if k == 0 else 1 - core
                do_v[pl.ds(row(s, d, c), QUARTER), :] = grad_o[(2 * k + d) * QUARTER:(2 * k + d + 1) * QUARTER]
        for j in range(0, hidden, 512):
            acc_o[:, j:j + 512] += dot_plain(z_b[pl.ds(0, QUARTER), :], gy_b[:, j:j + 512])

    def ds_relay(s, h):
        for d in (0, 1):
            ds_here(s, d, h).wait_recv()

            @pl.when(s < LAST)
            def _():
                ds_next(s + 1, d, h).start()
            ds_twin(s, d, h).start()

    def ds_step(s, carry):
        ds_relay(s, 0)
        project(s - 1)
        ds_relay(s, 1)
        for d in (0, 1):
            block_load(None, ds_all, gy_b, gy_sem, s, d, 0).start()
        for d in (0, 1):
            block_load(None, ds_all, gy_b, gy_sem, s, d, 0).wait()
        return carry

    lax.fori_loop(1, CHIPS, ds_step, 0)
    project(LAST)

    def drain(s, carry):
        for d in (0, 1):
            to_twin(gy_all, gy_ps, gy_pr, s, d).wait_send()
            to_twin(x_all, x_ps, x_pr, s, d).wait_send()
            for h in (0, 1):
                ds_twin(s, d, h).wait_send()

            @pl.when(s > 0)
            def _():
                arriving(gy_all, gy_ss, gy_rs, s, d).wait_send()
                arriving(x_all, x_ss, x_rs, s, d).wait_send()
                for h in (0, 1):
                    ds_here(s, d, h).wait_send()
        return carry
    lax.fori_loop(0, CHIPS, drain, 0)
    for d in (0, 1):
        sum_on(LAST - 1, d).wait_send()
        sum_on(LAST, d).wait_send()


def solution(mesh):
    token_spec = P(("dp", "tp"), None)
    split_cols = P("dp", "tp")
    weight_cols = P(None, "tp")
    weight_rows = P("tp", None)

    def local_backward(x_norm, grad_y, u_gate, u_up, w_gate, w_up, w_down, x_in, gamma, grad_res, attn_out, w_out):
        own, hidden = x_norm.shape
        tokens, ffn = u_gate.shape
        cols = attn_out.shape[1]
        anywhere = pl.BlockSpec(memory_space=pl.ANY)
        inside = pl.BlockSpec(memory_space=pltpu.VMEM)
        shape = jax.ShapeDtypeStruct
        dma = pltpu.SemaphoreType.DMA
        outs = pl.pallas_call(
            kernel,
            out_shape=[
                pltpu.VMEM((own, hidden), BF16), pltpu.VMEM((tokens, cols), BF16),
                pltpu.VMEM((ffn, hidden), F32), pltpu.VMEM((ffn, hidden), F32), pltpu.VMEM((ffn, hidden), F32),
                pltpu.VMEM((cols, hidden), F32),
                shape((tokens, hidden), BF16), shape((tokens, hidden), BF16), shape((tokens, hidden), BF16),
            ],
            in_specs=[anywhere] * 8 + [inside] + [anywhere] * 3,
            out_specs=[inside] * 6 + [anywhere] * 3,
            scratch_shapes=[
                pltpu.VMEM((ffn, hidden), BF16), pltpu.VMEM((ffn, hidden), BF16), pltpu.VMEM((ffn, hidden), BF16),
                pltpu.VMEM((ROWS, hidden), BF16), pltpu.VMEM((ROWS, hidden), BF16),
                pltpu.VMEM((ffn, ROWS), BF16), pltpu.VMEM((ffn, ROWS), BF16),
                pltpu.VMEM((ffn, ROWS), BF16), pltpu.VMEM((ffn, ROWS), BF16), pltpu.VMEM((ffn, ROWS), BF16),
                pltpu.VMEM((ROWS, ffn), BF16), pltpu.VMEM((ROWS, ffn), BF16),
                pltpu.VMEM((own, hidden), F32), pltpu.VMEM((own, hidden), BF16), pltpu.VMEM((2, own, hidden), BF16),
                pltpu.VMEM((2, 2, QUARTER, hidden), BF16), pltpu.VMEM((3, 2, QUARTER, hidden), BF16),
                pltpu.VMEM((own, hidden), F32),
                pltpu.VMEM((tokens, cols), BF16), pltpu.VMEM((cols, hidden), BF16),
                dma((CHIPS, 2)), dma((CHIPS, 2)), dma((CHIPS, 2)), dma((CHIPS, 2)),
                dma((CHIPS, 2)), dma((CHIPS, 2)), dma((CHIPS, 2)), dma((CHIPS, 2)),
                dma((CHIPS, 4)), dma((CHIPS, 4)), dma((CHIPS, 4)), dma((CHIPS, 4)),
                dma, dma((2,)), dma((2, 2)), dma((3, 2)),
                dma((5,)), dma((4,)), dma((4,)), dma((4,)), dma((4,)),
            ],
            compiler_params=pltpu.CompilerParams(
                collective_id=0, has_side_effects=True, vmem_limit_bytes=44 * 2 ** 20),
            name="mlp_backward",
        )(x_norm, grad_y, u_gate.T, u_up.T, w_gate.T, w_up.T, w_down, x_in, gamma, grad_res, attn_out, w_out)
        grad_sum, grad_attn, gw_gate, gw_up, gw_down, gw_out = outs[:6]
        return grad_sum, grad_attn, gw_gate.T, gw_up.T, gw_down, gw_out

    return jax.shard_map(
        local_backward,
        mesh=mesh,
        in_specs=(token_spec, token_spec, split_cols, split_cols, weight_cols, weight_cols, weight_rows,
                  token_spec, P(None), token_spec, split_cols, weight_rows),
        out_specs=(token_spec, split_cols, split_cols, split_cols, token_spec, token_spec),
        check_vma=False,
    )
```

```python
import jax
import jax.numpy as jnp
from jax import lax
from jax.experimental import pallas as pl
from jax.experimental.pallas import tpu as pltpu
from jax.sharding import PartitionSpec as P

NORM_EPS = 1e-5
MESH = pl.DeviceIdType.MESH
BF16 = jnp.bfloat16
F32 = jnp.float32

CHIPS = 8
QUARTER = 128
HALF = 64
ROWS = 4 * QUARTER
LAST = CHIPS - 1


def dot_cols(a, b):
    return lax.dot_general(a, b, (((1,), (1,)), ((), ())), preferred_element_type=F32)


def dot_plain(a, b):
    return lax.dot_general(a, b, (((1,), (0,)), ((), ())), preferred_element_type=F32)


def kernel(x, gy, ug, uu, wg, wu, wd, xin, gamma, gres, att, wo,
           out_ds, do_v, acc_g, acc_u, acc_d, acc_o, gy_all, x_all, ds_all, rs_in, z_all, dg_all, du_all,
           wg_v, wu_v, wd_v,
           gy_b, x_b, ug_b, uu_b, z_b, dg_b, du_b, dgt_b, dut_b,
           p_own, p_send, p_recv, hold, own_sum, stage, y_in,
           att_v, wo_v,
           gy_zs, gy_zr, gy_ys, gy_yr, gy_ts, gy_tr, x_zs, x_zr, x_ys, x_yr, x_ts, x_tr,
           ds_ss, ds_rs, ds_ps, ds_pr, ps_sem, pr_sem, rss_sem, rsr_sem, yss_sem, ysr_sem,
           w_sem, gy_sem, x_sem, u_sem, keep_sem, stage_sem):
    hidden = gy.shape[1]
    own = gy.shape[0]
    t = lax.axis_index("tp")
    core = t % 2
    y = (t // 2) % 2
    z = t // 4
    edge = z % 3 == 0
    inner = z % 3 != 0
    pos = z + y * (7 - 2 * z)

    def device(chip, c):
        upper = chip // 4
        return 4 * (chip + upper * (7 - 2 * chip)) + 2 * upper + c

    onward = (device((pos + 1) % CHIPS, core), device((pos + LAST) % CHIPS, core))
    twin = t + 1 - 2 * core
    over = t + 2 - 4 * y
    beside = (t + 4 - 4 * (z // 3), t - 4 + 4 * ((3 - z) // 3))

    def signal(other):
        pl.semaphore_signal(barrier, inc=1, device_id={"tp": other}, device_id_type=MESH)

    barrier = pltpu.get_barrier_semaphore()
    signal(over)
    signal(twin)

    @pl.when(z < 3)
    def _():
        signal(beside[0])

    @pl.when(z > 0)
    def _():
        signal(beside[1])

    @pl.when(edge)
    def _():
        pl.semaphore_wait(barrier, 3)

    @pl.when(inner)
    def _():
        pl.semaphore_wait(barrier, 4)

    def remote(src, dst, send, recv, to):
        return pltpu.make_async_remote_copy(src_ref=src, dst_ref=dst, send_sem=send, recv_sem=recv,
                                            device_id={"tp": to}, device_id_type=MESH)

    def column(k):
        far = z // 2
        near = z + far * (3 - 2 * z)
        late = k // 2
        col = (1 - near) * k + near * ((1 - late) * (1 - k) + late * k)
        return col + far * (3 - 2 * col)

    def line(r):
        return y + r - 2 * y * r

    def first_row(col, r, c):
        return pl.multiple_of(((col * 2 + line(r)) * 2 + c) * own, own)

    def half(col, r, c, h):
        return pl.ds(pl.multiple_of(first_row(col, r, c) + h * QUARTER, QUARTER), QUARTER)

    class Stream:
        def __init__(self, own_ref, full, zs, zr, ys, yr, ts, tr):
            self.own, self.full = own_ref, full
            self.zs, self.zr, self.ys, self.yr, self.ts, self.tr = zs, zr, ys, yr, ts, tr

        def part(self, col, r, c, h):
            return self.full.at[half(col, r, c, h), :]

        def mine(self, h):
            return self.own.at[pl.ds(h * QUARTER, QUARTER), :]

        def along(self, col, h, side, src=None):
            dst = self.part(col, 0, core, h)
            return remote(dst if src is None else src, dst, self.zs.at[side, col, h], self.zr.at[col, h], beside[side])

        def across(self, col, h, src=None):
            dst = self.part(col, 0, core, h)
            return remote(dst if src is None else src, dst, self.ys.at[col, h], self.yr.at[col, h], over)

        def from_over(self, col, h):
            dst = self.part(col, 1, core, h)
            return remote(dst, dst, self.ys.at[col, h], self.yr.at[col, h], over)

        def hand(self, col, r, h, src=None):
            dst = self.part(col, r, core, h)
            return remote(dst if src is None else src, dst, self.ts.at[r, col, h], self.tr.at[r, col, h], twin)

        def from_twin(self, col, r, h):
            dst = self.part(col, r, 1 - core, h)
            return remote(dst, dst, self.ts.at[r, col, h], self.tr.at[r, col, h], twin)

        def relay_row(self, dist, h):
            @pl.when(z >= dist)
            def _():
                self.along(z - dist, h, 0).wait_recv()

                @pl.when(z < 3)
                def _():
                    self.along(z - dist, h, 0).start()
                self.across(z - dist, h).start()
                self.hand(z - dist, 0, h).start()

            @pl.when(z + dist < 4)
            def _():
                self.along(z + dist, h, 1).wait_recv()

                @pl.when(z > 0)
                def _():
                    self.along(z + dist, h, 1).start()
                self.across(z + dist, h).start()
                self.hand(z + dist, 0, h).start()

        def relay_over(self, k, h):
            self.from_over(column(k), h).wait_recv()
            self.hand(column(k), 1, h).start()

        def start_row(self):
            for h in (0, 1):
                @pl.when(z < 3)
                def _():
                    self.along(z, h, 0, self.mine(h)).start()

                @pl.when(z > 0)
                def _():
                    self.along(z, h, 1, self.mine(h)).start()

        def start_rest(self):
            for h in (0, 1):
                self.across(z, h, self.mine(h)).start()
                self.hand(z, 0, h, self.mine(h)).start()

        def load(self, n, buf, sem):
            k, r = n // 2, n % 2

            @pl.when(n == 0)
            def _():
                pltpu.make_async_copy(self.own, buf.at[pl.ds(0, own), :], sem.at[0]).start()

            @pl.when(n > 0)
            def _():
                self.block(n, core, buf, sem, 0).start()
            for h in (0, 1):
                self.from_twin(column(k), r, h).wait_recv()
            self.block(n, 1 - core, buf, sem, 1).start()

        def block(self, n, c, buf, sem, i):
            rows = pl.ds(first_row(column(n // 2), n % 2, c), own)
            return pltpu.make_async_copy(self.full.at[rows, :], buf.at[pl.ds(i * own, own), :], sem.at[i])

        def landed(self, n, buf, sem):
            for i in (0, 1):
                self.block(n, core, buf, sem, i).wait()

        def drain(self, col):
            for h in (0, 1):
                self.across(col, h).wait_send()
                for r in (0, 1):
                    self.hand(col, r, h).wait_send()

                @pl.when((z < 3) & (col <= z))
                def _():
                    self.along(col, h, 0).wait_send()

                @pl.when((z > 0) & (col >= z))
                def _():
                    self.along(col, h, 1).wait_send()

    gys = Stream(gy, gy_all, gy_zs, gy_zr, gy_ys, gy_yr, gy_ts, gy_tr)
    xs = Stream(x, x_all, x_zs, x_zr, x_ys, x_yr, x_ts, x_tr)
    gys.start_row()
    gys.start_rest()

    @pl.when(edge)
    def _():
        xs.start_row()

    loads = [pltpu.make_async_copy(a, b, w_sem.at[i]) for i, (a, b) in enumerate(
        ((wd, wd_v), (wg, wg_v), (wu, wu_v), (att, att_v), (wo, wo_v)))]
    for copy in loads:
        copy.start()

    def load_u(n):
        copies = []
        for i in (0, 1):
            c = core if i == 0 else 1 - core
            rows = pl.ds(first_row(column(n // 2), n % 2, c), own)
            at = pl.ds(i * own, own)
            copies.append(pltpu.make_async_copy(ug.at[:, rows], ug_b.at[:, at], u_sem.at[i]))
            copies.append(pltpu.make_async_copy(uu.at[:, rows], uu_b.at[:, at], u_sem.at[2 + i]))
        return copies

    for copy in load_u(0):
        copy.start()

    acc_g[...] = jnp.zeros_like(acc_g)
    acc_u[...] = jnp.zeros_like(acc_u)
    acc_d[...] = jnp.zeros_like(acc_d)
    acc_o[...] = jnp.zeros_like(acc_o)

    def keep(n):
        return [pltpu.make_async_copy(a, b.at[n], keep_sem.at[i])
                for i, (a, b) in enumerate(((z_b, z_all), (dg_b, dg_all), (du_b, du_all)))]

    def swap(n):
        return remote(p_send, p_recv.at[n % 2], ps_sem, pr_sem.at[n % 2], twin)

    def rs_slot(side, col, r, h):
        rows = pl.multiple_of((((side * 4 + col) * 2 + line(r)) * 2 + h) * QUARTER, QUARTER)
        return rs_in.at[pl.ds(rows, QUARTER), :], rsr_sem.at[side, col, line(r), h]

    def send_sum(k, r, h):
        col = column(k)
        up = (col - z + 3) // 4
        dst, sem = rs_slot(1 - up, col, r, h)
        return remote(hold.at[(k - 1) * 2 + r, pl.ds(h * QUARTER, QUARTER), :], dst,
                      rss_sem.at[k - 1, r, h], sem, t - 4 + 8 * up)

    def take_sum(side, col, r, h, slot):
        src, sem = rs_slot(side, col, r, h)
        remote(stage.at[slot], src, rss_sem.at[0, 0, 0], sem, twin).wait_recv()
        copy = pltpu.make_async_copy(src, stage.at[slot], stage_sem.at[slot])
        copy.start()
        return copy

    def finish(n):
        k, r = n // 2, n % 2
        swap(n).wait_recv()

        @pl.when(k == 0)
        def _():
            def tile(i, carry):
                at = pl.ds(pl.multiple_of(i * 32, 32), 32)
                own_sum[r, at, :] = p_own[at, :] + p_recv[n % 2, at, :].astype(F32)
                return carry
            lax.fori_loop(0, own // 32, tile, 0)

        @pl.when(k > 0)
        def _():
            def tile(i, carry):
                at = pl.ds(pl.multiple_of(i * 32, 32), 32)
                hold[(k - 1) * 2 + r, at, :] = (p_own[at, :] + p_recv[n % 2, at, :].astype(F32)).astype(BF16)
                return carry
            lax.fori_loop(0, own // 32, tile, 0)

            @pl.when(edge & (k == 1))
            def _():
                for h in (0, 1):
                    send_sum(k, r, h).start()

            @pl.when(edge & (k > 1) & (r == 1))
            def _():
                for q in (1, 0):
                    for h in (0, 1):
                        send_sum(k, q, h).start()

    def hidden_step(n, carry):
        k, h = n // 2, n % 2
        gys.relay_row(k + 1, h)
        gys.relay_over(k, h)

        @pl.when(n > 0)
        def _():
            finish(n - 1)

        @pl.when(inner & (n == 4))
        def _():
            xs.start_row()

        @pl.when(n == 6)
        def _():
            xs.start_rest()
            for q in (0, 1):
                xs.relay_row(1, q)

        gys.load(n, gy_b, gy_sem)
        for copy in load_u(n):
            copy.wait()

        @pl.when(n == 0)
        def _():
            for copy in loads:
                copy.wait()

        @pl.when(n > 0)
        def _():
            for copy in keep(n - 1):
                copy.wait()
            swap(n - 1).wait_send()
        gys.landed(n, gy_b, gy_sem)

        def hidden_tile(i, carry):
            at = pl.ds(pl.multiple_of(i * 256, 256), 256)
            grad_h = dot_cols(wd_v[...], gy_b[at, :])
            gate = ug_b[:, at].astype(F32)
            up = uu_b[:, at].astype(F32)
            sig = jax.nn.sigmoid(gate)
            act = gate * sig
            z_b[:, at] = (act * up).astype(BF16)
            grad_up = (grad_h * act).astype(BF16)
            grad_gate = (grad_h * up * (sig * (1.0 + gate * (1.0 - sig)))).astype(BF16)
            du_b[:, at] = grad_up
            dg_b[:, at] = grad_gate
            dut_b[at, :] = grad_up.T
            dgt_b[at, :] = grad_gate.T
            return carry
        lax.fori_loop(0, ROWS // 256, hidden_tile, 0)
        for copy in keep(n):
            copy.start()

        @pl.when(n < LAST)
        def _():
            for copy in load_u(n + 1):
                copy.start()

        def part_tile(j, carry):
            at = pl.ds(pl.multiple_of(j * 512, 512), 512)
            part = dot_plain(dgt_b[...], wg_v[:, at]) + dot_plain(dut_b[...], wu_v[:, at])
            p_own[:, at] = part[:own]
            p_send[:, at] = part[own:].astype(BF16)
            return carry
        lax.fori_loop(0, hidden // 512, part_tile, 0)
        swap(n).start()
        return carry

    lax.fori_loop(0, CHIPS, hidden_step, 0)
    finish(LAST)
    for copy in keep(LAST):
        copy.wait()
    swap(LAST).wait_send()

    def carry_on(k, m):
        r, h = 1 - m // 2, m % 2
        col = column(k)
        up = (col - z + 3) // 4
        take_sum(1 - up, col, r, h, m % 2).wait()
        base = h * QUARTER

        def tile(i, carry):
            at = pl.ds(pl.multiple_of(base + i * 32, 32), 32)
            here = pl.ds(pl.multiple_of(i * 32, 32), 32)
            total = hold[(k - 1) * 2 + r, at, :].astype(F32) + stage[m % 2, here, :].astype(F32)
            hold[(k - 1) * 2 + r, at, :] = total.astype(BF16)
            return carry
        lax.fori_loop(0, QUARTER // 32, tile, 0)
        send_sum(k, r, h).start()

    def settle(side, r):
        copies = [take_sum(side, z, r, h, h) for h in (0, 1)]
        for h in (0, 1):
            copies[h].wait()

            def tile(i, carry):
                at = pl.ds(pl.multiple_of(h * QUARTER + i * 32, 32), 32)
                here = pl.ds(pl.multiple_of(i * 32, 32), 32)
                own_sum[r, at, :] = own_sum[r, at, :] + stage[h, here, :].astype(F32)
                return carry
            lax.fori_loop(0, QUARTER // 32, tile, 0)

    def give(h):
        rows = pl.ds(h * QUARTER, QUARTER)
        return remote(p_send.at[rows, :], y_in.at[rows, :], yss_sem.at[h], ysr_sem.at[h], over)

    def give_over():
        for h in (0, 1):
            def tile(i, carry):
                at = pl.ds(pl.multiple_of(h * QUARTER + i * 32, 32), 32)
                p_send[at, :] = own_sum[1, at, :].astype(BF16)
                return carry
            lax.fori_loop(0, QUARTER // 32, tile, 0)
            give(h).start()

    def weight_step(n, carry):
        xs.load(n, x_b, x_sem)
        for i, c in ((0, core), (1, 1 - core)):
            @pl.when((n > 0) | (i == 1))
            def _():
                gys.block(n, c, gy_b, gy_sem, i).start()

        @pl.when(n == 0)
        def _():
            pltpu.make_async_copy(gy, gy_b.at[pl.ds(0, own), :], gy_sem.at[0]).start()
        back = [pltpu.make_async_copy(b.at[n], a, keep_sem.at[i])
                for i, (a, b) in enumerate(((z_b, z_all), (dg_b, dg_all), (du_b, du_all)))]
        for copy in back:
            copy.start()
        for copy in back:
            copy.wait()
        gys.landed(n, gy_b, gy_sem)
        xs.landed(n, x_b, x_sem)

        def tile(j, carry):
            at = pl.ds(pl.multiple_of(j * 512, 512), 512)
            acc_d[:, at] += dot_plain(z_b[...], gy_b[:, at])
            acc_g[:, at] += dot_plain(dg_b[...], x_b[:, at])
            acc_u[:, at] += dot_plain(du_b[...], x_b[:, at])
            return carry
        lax.fori_loop(0, hidden // 512, tile, 0)
        return carry

    def late_step(i, carry):
        for h in (0, 1):
            xs.relay_row(i + 2, h)

        @pl.when(inner & (i == 0))
        def _():
            for r in (0, 1):
                settle(z - 1, r)
            carry_on(2, 0)
            carry_on(2, 1)

        @pl.when(inner & (i == 1))
        def _():
            carry_on(2, 2)
            carry_on(2, 3)

        @pl.when(inner & (i == 2))
        def _():
            carry_on(3, 0)
        for h in (0, 1):
            xs.relay_over(i, h)

        @pl.when(inner & (i == 2))
        def _():
            settle(2 - z, 1)
            give_over()
            carry_on(3, 1)
            carry_on(1, 0)
            settle(2 - z, 0)
        lax.fori_loop(2 * i, 2 * i + 2, weight_step, 0)
        return carry

    lax.fori_loop(0, 3, late_step, 0)

    @pl.when(inner)
    def _():
        carry_on(3, 2)
        carry_on(1, 1)
    xs.relay_over(3, 0)

    @pl.when(inner)
    def _():
        carry_on(3, 3)
        carry_on(1, 2)
    xs.relay_over(3, 1)

    norm_loads = [pltpu.make_async_copy(src, x_b.at[pl.ds(k * own, own), :], x_sem.at[k])
                  for k, src in enumerate((xin, gres))]
    for copy in norm_loads:
        copy.start()

    @pl.when(inner)
    def _():
        carry_on(1, 3)

    @pl.when(edge)
    def _():
        settle((3 - z) // 3, 1)
        give_over()
        settle((3 - z) // 3, 0)
    for copy in norm_loads:
        copy.wait()

    def row(s, d, c):
        source = (pos + (CHIPS - s if d == 0 else s)) % CHIPS
        return pl.multiple_of(device(source, c) * 2 * QUARTER + d * QUARTER, QUARTER)

    def block_load(s, d, k):
        c = core if k == 0 else 1 - core
        at = pl.ds((2 * k + d) * QUARTER, QUARTER)
        return pltpu.make_async_copy(ds_all.at[pl.ds(row(s, d, c), QUARTER), :], gy_b.at[at, :], gy_sem.at[2 * k + d])

    def ds_next(s, d, h, src=None):
        rows = pl.ds(pl.multiple_of(row(s - 1, d, core) + h * HALF, HALF), HALF)
        return remote(ds_all.at[rows, :] if src is None else src, ds_all.at[rows, :],
                      ds_ss.at[s, 2 * d + h], ds_rs.at[s, 2 * d + h], onward[d])

    def ds_here(s, d, h):
        rows = pl.ds(pl.multiple_of(row(s, d, core) + h * HALF, HALF), HALF)
        return remote(ds_all.at[rows, :], ds_all.at[rows, :],
                      ds_ss.at[s, 2 * d + h], ds_rs.at[s, 2 * d + h], onward[d])

    def ds_twin(s, d, h, src=None):
        rows = pl.ds(pl.multiple_of(row(s, d, core) + h * HALF, HALF), HALF)
        return remote(ds_all.at[rows, :] if src is None else src, ds_all.at[rows, :],
                      ds_ps.at[s, 2 * d + h], ds_pr.at[s, 2 * d + h], twin)

    def ds_from_twin(s, d, h):
        rows = pl.ds(pl.multiple_of(row(s, d, 1 - core) + h * HALF, HALF), HALF)
        return remote(ds_all.at[rows, :], ds_all.at[rows, :],
                      ds_ps.at[s, 2 * d + h], ds_pr.at[s, 2 * d + h], twin)

    gain = gamma[...].astype(F32)[None, :]
    for d in (0, 1):
        give(d).wait_recv()
    for h in (0, 1):
        for d in (0, 1):
            def norm_tile(i, carry):
                here = pl.ds(pl.multiple_of(d * QUARTER + h * HALF + i * 16, 16), 16)
                skip = pl.ds(pl.multiple_of(2 * QUARTER + d * QUARTER + h * HALF + i * 16, 16), 16)
                grad_x = (own_sum[0, here, :] + y_in[here, :].astype(F32)).astype(BF16).astype(F32)
                xin_f = x_b[here, :].astype(F32)
                inv_rms = lax.rsqrt(jnp.mean(xin_f * xin_f, axis=-1, keepdims=True) + NORM_EPS)
                scaled = grad_x * gain
                proj = jnp.mean(scaled * xin_f, axis=-1, keepdims=True)
                grad_s = (x_b[skip, :].astype(F32)
                          + inv_rms * (scaled - xin_f * (inv_rms * inv_rms) * proj)).astype(BF16)
                out_ds[here, :] = grad_s
                return carry
            lax.fori_loop(0, HALF // 16, norm_tile, 0)
            mine = out_ds.at[pl.ds(d * QUARTER + h * HALF, HALF), :]
            ds_next(1, d, h, mine).start()
            ds_twin(0, d, h, mine).start()

    lax.fori_loop(6, 8, weight_step, 0)
    for d in (0, 1):
        gy_b[pl.ds(d * QUARTER, QUARTER), :] = out_ds[pl.ds(d * QUARTER, QUARTER), :]

    def project(s):
        for d in (0, 1):
            for h in (0, 1):
                ds_from_twin(s, d, h).wait_recv()
            block_load(s, d, 1).start()
        for d in (0, 1):
            block_load(s, d, 1).wait()
        for k in (0, 1):
            for d in (0, 1):
                c = core if k == 0 else 1 - core
                rows = pl.ds(row(s, d, c), QUARTER)
                at = pl.ds((2 * k + d) * QUARTER, QUARTER)
                z_b[pl.ds(0, QUARTER), at] = att_v[rows, :].T
        grad_o = dot_cols(gy_b[...], wo_v[...]).astype(BF16)
        for k in (0, 1):
            for d in (0, 1):
                c = core if k == 0 else 1 - core
                do_v[pl.ds(row(s, d, c), QUARTER), :] = grad_o[(2 * k + d) * QUARTER:(2 * k + d + 1) * QUARTER]
        for j in range(0, hidden, 512):
            acc_o[:, j:j + 512] += dot_plain(z_b[pl.ds(0, QUARTER), :], gy_b[:, j:j + 512])

    def ds_relay(s, h):
        for d in (0, 1):
            ds_here(s, d, h).wait_recv()

            @pl.when(s < LAST)
            def _():
                ds_next(s + 1, d, h).start()
            ds_twin(s, d, h).start()

    def ds_step(s, carry):
        ds_relay(s, 0)
        project(s - 1)
        ds_relay(s, 1)
        for d in (0, 1):
            block_load(s, d, 0).start()
        for d in (0, 1):
            block_load(s, d, 0).wait()
        return carry

    lax.fori_loop(1, CHIPS, ds_step, 0)
    project(LAST)

    def drain(s, carry):
        for d in (0, 1):
            for h in (0, 1):
                ds_twin(s, d, h).wait_send()

            @pl.when(s > 0)
            def _():
                for h in (0, 1):
                    ds_here(s, d, h).wait_send()
        return carry
    lax.fori_loop(0, CHIPS, drain, 0)

    def drain_columns(col, carry):
        gys.drain(col)
        xs.drain(col)

        @pl.when(col > 0)
        def _():
            for r in (0, 1):
                for h in (0, 1):
                    send_sum(col, r, h).wait_send()
        return carry
    lax.fori_loop(0, 4, drain_columns, 0)
    for h in (0, 1):
        give(h).wait_send()


def solution(mesh):
    token_spec = P(("dp", "tp"), None)
    split_cols = P("dp", "tp")
    weight_cols = P(None, "tp")
    weight_rows = P("tp", None)

    def local_backward(x_norm, grad_y, u_gate, u_up, w_gate, w_up, w_down, x_in, gamma, grad_res, attn_out, w_out):
        own, hidden = x_norm.shape
        tokens, ffn = u_gate.shape
        cols = attn_out.shape[1]
        anywhere = pl.BlockSpec(memory_space=pl.ANY)
        inside = pl.BlockSpec(memory_space=pltpu.VMEM)
        shape = jax.ShapeDtypeStruct
        dma = pltpu.SemaphoreType.DMA
        outs = pl.pallas_call(
            kernel,
            out_shape=[
                pltpu.VMEM((own, hidden), BF16), pltpu.VMEM((tokens, cols), BF16),
                pltpu.VMEM((ffn, hidden), F32), pltpu.VMEM((ffn, hidden), F32), pltpu.VMEM((ffn, hidden), F32),
                pltpu.VMEM((cols, hidden), F32),
                shape((tokens, hidden), BF16), shape((tokens, hidden), BF16), shape((tokens, hidden), BF16),
                shape((32 * QUARTER, hidden), BF16),
                shape((CHIPS, ffn, ROWS), BF16), shape((CHIPS, ffn, ROWS), BF16), shape((CHIPS, ffn, ROWS), BF16),
            ],
            in_specs=[anywhere] * 8 + [inside] + [anywhere] * 3,
            out_specs=[inside] * 6 + [anywhere] * 7,
            scratch_shapes=[
                pltpu.VMEM((ffn, hidden), BF16), pltpu.VMEM((ffn, hidden), BF16), pltpu.VMEM((ffn, hidden), BF16),
                pltpu.VMEM((ROWS, hidden), BF16), pltpu.VMEM((ROWS, hidden), BF16),
                pltpu.VMEM((ffn, ROWS), BF16), pltpu.VMEM((ffn, ROWS), BF16),
                pltpu.VMEM((ffn, ROWS), BF16), pltpu.VMEM((ffn, ROWS), BF16), pltpu.VMEM((ffn, ROWS), BF16),
                pltpu.VMEM((ROWS, ffn), BF16), pltpu.VMEM((ROWS, ffn), BF16),
                pltpu.VMEM((own, hidden), F32), pltpu.VMEM((own, hidden), BF16), pltpu.VMEM((2, own, hidden), BF16),
                pltpu.VMEM((6, own, hidden), BF16), pltpu.VMEM((2, own, hidden), F32),
                pltpu.VMEM((2, QUARTER, hidden), BF16), pltpu.VMEM((own, hidden), BF16),
                pltpu.VMEM((tokens, cols), BF16), pltpu.VMEM((cols, hidden), BF16),
                dma((2, 4, 2)), dma((4, 2)), dma((4, 2)), dma((4, 2)), dma((2, 4, 2)), dma((2, 4, 2)),
                dma((2, 4, 2)), dma((4, 2)), dma((4, 2)), dma((4, 2)), dma((2, 4, 2)), dma((2, 4, 2)),
                dma((CHIPS, 4)), dma((CHIPS, 4)), dma((CHIPS, 4)), dma((CHIPS, 4)),
                dma, dma((2,)), dma((3, 2, 2)), dma((2, 4, 2, 2)), dma((2,)), dma((2,)),
                dma((5,)), dma((4,)), dma((2,)), dma((4,)), dma((3,)), dma((2,)),
            ],
            compiler_params=pltpu.CompilerParams(
                collective_id=0, has_side_effects=True, vmem_limit_bytes=44 * 2 ** 20),
            name="mlp_backward",
        )(x_norm, grad_y, u_gate.T, u_up.T, w_gate.T, w_up.T, w_down, x_in, gamma, grad_res, attn_out, w_out)
        grad_sum, grad_attn, gw_gate, gw_up, gw_down, gw_out = outs[:6]
        return grad_sum, grad_attn, gw_gate.T, gw_up.T, gw_down, gw_out

    return jax.shard_map(
        local_backward,
        mesh=mesh,
        in_specs=(token_spec, token_spec, split_cols, split_cols, weight_cols, weight_cols, weight_rows,
                  token_spec, P(None), token_spec, split_cols, weight_rows),
        out_specs=(token_spec, split_cols, split_cols, split_cols, token_spec, token_spec),
        check_vma=False,
    )
```

```python
import jax
import jax.numpy as jnp
from jax import lax
from jax.experimental import pallas as pl
from jax.experimental.pallas import tpu as pltpu
from jax.sharding import PartitionSpec as P

NORM_EPS = 1e-5
MESH = pl.DeviceIdType.MESH
BF16 = jnp.bfloat16
F32 = jnp.float32

CHIPS = 8
QUARTER = 128
HALF = 64
ROWS = 4 * QUARTER
LAST = CHIPS - 1


def dot_cols(a, b):
    return lax.dot_general(a, b, (((1,), (1,)), ((), ())), preferred_element_type=F32)


def dot_plain(a, b):
    return lax.dot_general(a, b, (((1,), (0,)), ((), ())), preferred_element_type=F32)


def kernel(x, gy, ug, uu, wg, wu, wd, xin, gamma, gres, att, wo,
           out_ds, do_v, acc_g, acc_u, acc_d, acc_o, gy_all, x_all, ds_all, rs_in, z_all, dg_all, du_all,
           wg_v, wu_v, wd_v,
           gy_b, x_b, ug_b, uu_b, z_b, dg_b, du_b, dgt_b, dut_b,
           p_own, p_send, p_recv, hold, own_sum, stage, y_in,
           att_v, wo_v,
           gy_zs, gy_zr, gy_ys, gy_yr, gy_ts, gy_tr, x_zs, x_zr, x_ys, x_yr, x_ts, x_tr,
           ds_ss, ds_rs, ds_ps, ds_pr, ps_sem, pr_sem, rss_sem, rsr_sem, yss_sem, ysr_sem,
           w_sem, gy_sem, x_sem, u_sem, keep_sem, stage_sem):
    hidden = gy.shape[1]
    own = gy.shape[0]
    t = lax.axis_index("tp")
    core = t % 2
    y = (t // 2) % 2
    z = t // 4
    edge = z % 3 == 0
    inner = z % 3 != 0
    pos = z + y * (7 - 2 * z)

    def device(chip, c):
        upper = chip // 4
        return 4 * (chip + upper * (7 - 2 * chip)) + 2 * upper + c

    onward = (device((pos + 1) % CHIPS, core), device((pos + LAST) % CHIPS, core))
    twin = t + 1 - 2 * core
    over = t + 2 - 4 * y
    beside = (t + 4 - 4 * (z // 3), t - 4 + 4 * ((3 - z) // 3))

    def signal(other):
        pl.semaphore_signal(barrier, inc=1, device_id={"tp": other}, device_id_type=MESH)

    barrier = pltpu.get_barrier_semaphore()
    signal(over)
    signal(twin)

    @pl.when(z < 3)
    def _():
        signal(beside[0])

    @pl.when(z > 0)
    def _():
        signal(beside[1])

    @pl.when(edge)
    def _():
        pl.semaphore_wait(barrier, 3)

    @pl.when(inner)
    def _():
        pl.semaphore_wait(barrier, 4)

    def remote(src, dst, send, recv, to):
        return pltpu.make_async_remote_copy(src_ref=src, dst_ref=dst, send_sem=send, recv_sem=recv,
                                            device_id={"tp": to}, device_id_type=MESH)

    def column(k):
        far = z // 2
        near = z + far * (3 - 2 * z)
        late = k // 2
        col = (1 - near) * k + near * ((1 - late) * (1 - k) + late * k)
        return col + far * (3 - 2 * col)

    def line(r):
        return y + r - 2 * y * r

    def first_row(col, r, c):
        return pl.multiple_of(((col * 2 + line(r)) * 2 + c) * own, own)

    def half(col, r, c, h):
        return pl.ds(pl.multiple_of(first_row(col, r, c) + h * QUARTER, QUARTER), QUARTER)

    class Stream:
        def __init__(self, own_ref, full, zs, zr, ys, yr, ts, tr):
            self.own, self.full = own_ref, full
            self.zs, self.zr, self.ys, self.yr, self.ts, self.tr = zs, zr, ys, yr, ts, tr

        def part(self, col, r, c, h):
            return self.full.at[half(col, r, c, h), :]

        def mine(self, h):
            return self.own.at[pl.ds(h * QUARTER, QUARTER), :]

        def along(self, col, h, side, src=None):
            dst = self.part(col, 0, core, h)
            return remote(dst if src is None else src, dst, self.zs.at[side, col, h], self.zr.at[col, h], beside[side])

        def across(self, col, h, src=None):
            dst = self.part(col, 0, core, h)
            return remote(dst if src is None else src, dst, self.ys.at[col, h], self.yr.at[col, h], over)

        def from_over(self, col, h):
            dst = self.part(col, 1, core, h)
            return remote(dst, dst, self.ys.at[col, h], self.yr.at[col, h], over)

        def hand(self, col, r, h, src=None):
            dst = self.part(col, r, core, h)
            return remote(dst if src is None else src, dst, self.ts.at[r, col, h], self.tr.at[r, col, h], twin)

        def from_twin(self, col, r, h):
            dst = self.part(col, r, 1 - core, h)
            return remote(dst, dst, self.ts.at[r, col, h], self.tr.at[r, col, h], twin)

        def relay(self, dist, h, side, held=False):
            col = z - dist if side == 0 else z + dist
            self.along(col, h, side).wait_recv()

            @pl.when(z < 3 if side == 0 else z > 0)
            def _():
                self.along(col, h, side).start()
            self.hand(col, 0, h).start()
            if not held:
                self.across(col, h).start()
            else:
                second = inner & (dist == 1) & (z == 2 - side)

                @pl.when(jnp.logical_not(second))
                def _():
                    self.across(col, h).start()

        def relay_row(self, dist, h, held=False):
            @pl.when(z >= dist)
            def _():
                self.relay(dist, h, 0, held)

            @pl.when(z + dist < 4)
            def _():
                self.relay(dist, h, 1, held)

            if held and h == 1:
                @pl.when(inner & (dist == 1))
                def _():
                    for q in (0, 1):
                        self.across(column(2), q).start()

        def relay_over(self, k, h):
            self.from_over(column(k), h).wait_recv()
            self.hand(column(k), 1, h).start()

        def start_row(self):
            for h in (0, 1):
                @pl.when(z < 3)
                def _():
                    self.along(z, h, 0, self.mine(h)).start()

                @pl.when(z > 0)
                def _():
                    self.along(z, h, 1, self.mine(h)).start()

        def start_rest(self):
            for h in (0, 1):
                self.across(z, h, self.mine(h)).start()
                self.hand(z, 0, h, self.mine(h)).start()

        def load(self, n, buf, sem):
            k, r = n // 2, n % 2

            @pl.when(n == 0)
            def _():
                pltpu.make_async_copy(self.own, buf.at[pl.ds(0, own), :], sem.at[0]).start()

            @pl.when(n > 0)
            def _():
                self.block(n, core, buf, sem, 0).start()
            for h in (0, 1):
                self.from_twin(column(k), r, h).wait_recv()
            self.block(n, 1 - core, buf, sem, 1).start()

        def block(self, n, c, buf, sem, i):
            rows = pl.ds(first_row(column(n // 2), n % 2, c), own)
            return pltpu.make_async_copy(self.full.at[rows, :], buf.at[pl.ds(i * own, own), :], sem.at[i])

        def landed(self, n, buf, sem):
            for i in (0, 1):
                self.block(n, core, buf, sem, i).wait()

        def drain(self, col):
            for h in (0, 1):
                self.across(col, h).wait_send()
                for r in (0, 1):
                    self.hand(col, r, h).wait_send()

                @pl.when((z < 3) & (col <= z))
                def _():
                    self.along(col, h, 0).wait_send()

                @pl.when((z > 0) & (col >= z))
                def _():
                    self.along(col, h, 1).wait_send()

    gys = Stream(gy, gy_all, gy_zs, gy_zr, gy_ys, gy_yr, gy_ts, gy_tr)
    xs = Stream(x, x_all, x_zs, x_zr, x_ys, x_yr, x_ts, x_tr)
    gys.start_row()
    gys.start_rest()

    @pl.when(edge)
    def _():
        xs.start_row()

    loads = [pltpu.make_async_copy(a, b, w_sem.at[i]) for i, (a, b) in enumerate(
        ((wd, wd_v), (wg, wg_v), (wu, wu_v), (att, att_v), (wo, wo_v)))]
    for copy in loads:
        copy.start()

    def load_u(n):
        copies = []
        for i in (0, 1):
            c = core if i == 0 else 1 - core
            rows = pl.ds(first_row(column(n // 2), n % 2, c), own)
            at = pl.ds(i * own, own)
            copies.append(pltpu.make_async_copy(ug.at[:, rows], ug_b.at[:, at], u_sem.at[i]))
            copies.append(pltpu.make_async_copy(uu.at[:, rows], uu_b.at[:, at], u_sem.at[2 + i]))
        return copies

    for copy in load_u(0):
        copy.start()

    acc_g[...] = jnp.zeros_like(acc_g)
    acc_u[...] = jnp.zeros_like(acc_u)
    acc_d[...] = jnp.zeros_like(acc_d)
    acc_o[...] = jnp.zeros_like(acc_o)

    def keep(n):
        return [pltpu.make_async_copy(a, b.at[n], keep_sem.at[i])
                for i, (a, b) in enumerate(((z_b, z_all), (dg_b, dg_all), (du_b, du_all)))]

    def swap(n):
        return remote(p_send, p_recv.at[n % 2], ps_sem, pr_sem.at[n % 2], twin)

    def rs_slot(side, col, r, h):
        rows = pl.multiple_of((((side * 4 + col) * 2 + line(r)) * 2 + h) * QUARTER, QUARTER)
        return rs_in.at[pl.ds(rows, QUARTER), :], rsr_sem.at[side, col, line(r), h]

    def send_sum(k, r, h):
        col = column(k)
        up = (col - z + 3) // 4
        dst, sem = rs_slot(1 - up, col, r, h)
        return remote(hold.at[(k - 1) * 2 + r, pl.ds(pl.multiple_of(h * QUARTER, QUARTER), QUARTER), :], dst,
                      rss_sem.at[k - 1, r, h], sem, t - 4 + 8 * up)

    def take_sum(side, col, r, h, slot):
        src, sem = rs_slot(side, col, r, h)
        remote(stage.at[slot], src, rss_sem.at[0, 0, 0], sem, twin).wait_recv()
        copy = pltpu.make_async_copy(src, stage.at[slot], stage_sem.at[slot])
        copy.start()
        return copy

    def finish(n):
        k, r = n // 2, n % 2
        swap(n).wait_recv()

        @pl.when(k == 0)
        def _():
            def tile(i, carry):
                at = pl.ds(pl.multiple_of(i * 32, 32), 32)
                own_sum[r, at, :] = p_own[at, :] + p_recv[n % 2, at, :].astype(F32)
                return carry
            lax.fori_loop(0, own // 32, tile, 0)

        @pl.when(k > 0)
        def _():
            def tile(i, carry):
                at = pl.ds(pl.multiple_of(i * 32, 32), 32)
                hold[(k - 1) * 2 + r, at, :] = (p_own[at, :] + p_recv[n % 2, at, :].astype(F32)).astype(BF16)
                return carry
            lax.fori_loop(0, own // 32, tile, 0)

            @pl.when(edge & (k == 1))
            def _():
                for h in (0, 1):
                    send_sum(k, r, h).start()

            @pl.when(edge & (k > 1) & (r == 1))
            def _():
                for q in (1, 0):
                    for h in (0, 1):
                        send_sum(k, q, h).start()

    def hidden_step(n, buf, sem):
        for copy in load_u(n):
            copy.wait()

        @pl.when(n > 0)
        def _():
            for copy in keep(n - 1):
                copy.wait()
        gys.landed(n, buf, sem)

        def hidden_tile(i, carry):
            at = pl.ds(pl.multiple_of(i * 256, 256), 256)
            grad_h = dot_cols(wd_v[...], buf[at, :])
            gate = ug_b[:, at].astype(F32)
            up = uu_b[:, at].astype(F32)
            sig = jax.nn.sigmoid(gate)
            act = gate * sig
            z_b[:, at] = (act * up).astype(BF16)
            grad_up = (grad_h * act).astype(BF16)
            grad_gate = (grad_h * up * (sig * (1.0 + gate * (1.0 - sig)))).astype(BF16)
            du_b[:, at] = grad_up
            dg_b[:, at] = grad_gate
            dut_b[at, :] = grad_up.T
            dgt_b[at, :] = grad_gate.T
            return carry
        lax.fori_loop(0, ROWS // 256, hidden_tile, 0)
        for copy in keep(n):
            copy.start()

        @pl.when(n < LAST)
        def _():
            for copy in load_u(n + 1):
                copy.start()

        @pl.when((n > 0) & (n % 2 == 0))
        def _():
            finish(n - 1)

        @pl.when(n > 0)
        def _():
            swap(n - 1).wait_send()

        def part_tile(j, carry):
            at = pl.ds(pl.multiple_of(j * 512, 512), 512)
            part = dot_plain(dgt_b[...], wg_v[:, at]) + dot_plain(dut_b[...], wu_v[:, at])
            p_own[:, at] = part[:own]
            p_send[:, at] = part[own:].astype(BF16)
            return carry
        lax.fori_loop(0, hidden // 512, part_tile, 0)
        swap(n).start()

    gys.load(0, gy_b, gy_sem)
    for copy in loads:
        copy.wait()
    hidden_step(0, gy_b, gy_sem)

    def hidden_pair(k, carry):
        finish(2 * k)
        for h in (0, 1):
            gys.relay_row(k + 1, h, held=True)
            gys.relay_over(k, h)

            @pl.when(edge & (k == 3))
            def _():
                for side in (0, 1):
                    @pl.when(z // 2 == 1 - side)
                    def _():
                        xs.relay(1, h, side)

        gys.load(2 * k + 1, x_b, x_sem)

        @pl.when(k < 3)
        def _():
            gys.load(2 * k + 2, gy_b, gy_sem)

        @pl.when(inner & (k == 1))
        def _():
            xs.start_row()
            xs.start_rest()
            for side in (0, 1):
                @pl.when(z == 1 + side)
                def _():
                    for h in (0, 1):
                        xs.relay(1, h, side)

        @pl.when(edge & (k == 2))
        def _():
            xs.start_rest()

        @pl.when(inner & (k == 3))
        def _():
            for side in (0, 1):
                @pl.when(z == 2 - side)
                def _():
                    for h in (0, 1):
                        xs.relay(1, h, side)
        hidden_step(2 * k + 1, x_b, x_sem)

        @pl.when(k < 3)
        def _():
            hidden_step(2 * k + 2, gy_b, gy_sem)
        return carry

    lax.fori_loop(0, 4, hidden_pair, 0)
    finish(LAST)
    for copy in keep(LAST):
        copy.wait()
    swap(LAST).wait_send()

    def carry_on(k, m):
        r, h = 1 - m // 2, m % 2
        col = column(k)
        up = (col - z + 3) // 4
        take_sum(1 - up, col, r, h, m % 2).wait()
        base = h * QUARTER

        def tile(i, carry):
            at = pl.ds(pl.multiple_of(base + i * 32, 32), 32)
            here = pl.ds(pl.multiple_of(i * 32, 32), 32)
            total = hold[(k - 1) * 2 + r, at, :].astype(F32) + stage[m % 2, here, :].astype(F32)
            hold[(k - 1) * 2 + r, at, :] = total.astype(BF16)
            return carry
        lax.fori_loop(0, QUARTER // 32, tile, 0)
        send_sum(k, r, h).start()

    def settle(side, r):
        copies = [take_sum(side, z, r, h, h) for h in (0, 1)]
        for h in (0, 1):
            copies[h].wait()

            def tile(i, carry):
                at = pl.ds(pl.multiple_of(h * QUARTER + i * 32, 32), 32)
                here = pl.ds(pl.multiple_of(i * 32, 32), 32)
                own_sum[r, at, :] = own_sum[r, at, :] + stage[h, here, :].astype(F32)
                return carry
            lax.fori_loop(0, QUARTER // 32, tile, 0)

    def give(h):
        rows = pl.ds(h * QUARTER, QUARTER)
        return remote(p_send.at[rows, :], y_in.at[rows, :], yss_sem.at[h], ysr_sem.at[h], over)

    def give_over():
        for h in (0, 1):
            def tile(i, carry):
                at = pl.ds(pl.multiple_of(h * QUARTER + i * 32, 32), 32)
                p_send[at, :] = own_sum[1, at, :].astype(BF16)
                return carry
            lax.fori_loop(0, QUARTER // 32, tile, 0)
            give(h).start()

    def weight_step(n):
        xs.load(n, x_b, x_sem)
        for i, c in ((0, core), (1, 1 - core)):
            @pl.when((n > 0) | (i == 1))
            def _():
                gys.block(n, c, gy_b, gy_sem, i).start()

        @pl.when(n == 0)
        def _():
            pltpu.make_async_copy(gy, gy_b.at[pl.ds(0, own), :], gy_sem.at[0]).start()
        back = [pltpu.make_async_copy(b.at[n], a, keep_sem.at[i])
                for i, (a, b) in enumerate(((z_b, z_all), (dg_b, dg_all), (du_b, du_all)))]
        for copy in back:
            copy.start()
        for copy in back:
            copy.wait()
        gys.landed(n, gy_b, gy_sem)
        xs.landed(n, x_b, x_sem)

        def tile(j, carry):
            at = pl.ds(pl.multiple_of(j * 512, 512), 512)
            acc_d[:, at] += dot_plain(z_b[...], gy_b[:, at])
            acc_g[:, at] += dot_plain(dg_b[...], x_b[:, at])
            acc_u[:, at] += dot_plain(du_b[...], x_b[:, at])
            return carry
        lax.fori_loop(0, hidden // 512, tile, 0)

    def late_step(i, carry):
        @pl.when(inner & (i == 0))
        def _():
            for r in (0, 1):
                settle(z - 1, r)

        @pl.when(inner)
        def _():
            carry_on(2, i)

        @pl.when(i < 2)
        def _():
            for h in (0, 1):
                xs.relay_row(i + 2, h)
        xs.relay_over(i // 2, i % 2)
        weight_step(i)
        return carry

    lax.fori_loop(0, 4, late_step, 0)

    @pl.when(inner)
    def _():
        carry_on(3, 0)
        settle(2 - z, 1)
        give_over()
        carry_on(3, 1)
        carry_on(1, 0)
        settle(2 - z, 0)
    for h in (0, 1):
        xs.relay_over(2, h)

    @pl.when(inner)
    def _():
        for m in (1, 2):
            carry_on(3, m + 1)
            carry_on(1, m)
    for h in (0, 1):
        xs.relay_over(3, h)

    norm_loads = [pltpu.make_async_copy(src, x_b.at[pl.ds(k * own, own), :], x_sem.at[k])
                  for k, src in enumerate((xin, gres))]
    for copy in norm_loads:
        copy.start()

    @pl.when(inner)
    def _():
        carry_on(1, 3)

    @pl.when(edge)
    def _():
        settle((3 - z) // 3, 1)
        give_over()
        settle((3 - z) // 3, 0)
    for copy in norm_loads:
        copy.wait()

    def row(s, d, c):
        source = (pos + (CHIPS - s if d == 0 else s)) % CHIPS
        return pl.multiple_of(device(source, c) * 2 * QUARTER + d * QUARTER, QUARTER)

    def block_load(s, d, k):
        c = core if k == 0 else 1 - core
        at = pl.ds((2 * k + d) * QUARTER, QUARTER)
        return pltpu.make_async_copy(ds_all.at[pl.ds(row(s, d, c), QUARTER), :], gy_b.at[at, :], gy_sem.at[2 * k + d])

    def ds_next(s, d, h, src=None):
        rows = pl.ds(pl.multiple_of(row(s - 1, d, core) + h * HALF, HALF), HALF)
        return remote(ds_all.at[rows, :] if src is None else src, ds_all.at[rows, :],
                      ds_ss.at[s, 2 * d + h], ds_rs.at[s, 2 * d + h], onward[d])

    def ds_here(s, d, h):
        rows = pl.ds(pl.multiple_of(row(s, d, core) + h * HALF, HALF), HALF)
        return remote(ds_all.at[rows, :], ds_all.at[rows, :],
                      ds_ss.at[s, 2 * d + h], ds_rs.at[s, 2 * d + h], onward[d])

    def ds_twin(s, d, h, src=None):
        rows = pl.ds(pl.multiple_of(row(s, d, core) + h * HALF, HALF), HALF)
        return remote(ds_all.at[rows, :] if src is None else src, ds_all.at[rows, :],
                      ds_ps.at[s, 2 * d + h], ds_pr.at[s, 2 * d + h], twin)

    def ds_from_twin(s, d, h):
        rows = pl.ds(pl.multiple_of(row(s, d, 1 - core) + h * HALF, HALF), HALF)
        return remote(ds_all.at[rows, :], ds_all.at[rows, :],
                      ds_ps.at[s, 2 * d + h], ds_pr.at[s, 2 * d + h], twin)

    gain = gamma[...].astype(F32)[None, :]
    for d in (0, 1):
        give(d).wait_recv()
    for h in (0, 1):
        for d in (0, 1):
            def norm_tile(i, carry):
                here = pl.ds(pl.multiple_of(d * QUARTER + h * HALF + i * 16, 16), 16)
                skip = pl.ds(pl.multiple_of(2 * QUARTER + d * QUARTER + h * HALF + i * 16, 16), 16)
                grad_x = (own_sum[0, here, :] + y_in[here, :].astype(F32)).astype(BF16).astype(F32)
                xin_f = x_b[here, :].astype(F32)
                inv_rms = lax.rsqrt(jnp.mean(xin_f * xin_f, axis=-1, keepdims=True) + NORM_EPS)
                scaled = grad_x * gain
                proj = jnp.mean(scaled * xin_f, axis=-1, keepdims=True)
                grad_s = (x_b[skip, :].astype(F32)
                          + inv_rms * (scaled - xin_f * (inv_rms * inv_rms) * proj)).astype(BF16)
                out_ds[here, :] = grad_s
                return carry
            lax.fori_loop(0, HALF // 16, norm_tile, 0)
            mine = out_ds.at[pl.ds(d * QUARTER + h * HALF, HALF), :]
            ds_next(1, d, h, mine).start()
            ds_twin(0, d, h, mine).start()

    for d in (0, 1):
        gy_b[pl.ds(d * QUARTER, QUARTER), :] = out_ds[pl.ds(d * QUARTER, QUARTER), :]

    def project(s):
        for d in (0, 1):
            for h in (0, 1):
                ds_from_twin(s, d, h).wait_recv()
            block_load(s, d, 1).start()
        for d in (0, 1):
            block_load(s, d, 1).wait()
        for k in (0, 1):
            for d in (0, 1):
                c = core if k == 0 else 1 - core
                rows = pl.ds(row(s, d, c), QUARTER)
                at = pl.ds((2 * k + d) * QUARTER, QUARTER)
                z_b[pl.ds(0, QUARTER), at] = att_v[rows, :].T
        grad_o = dot_cols(gy_b[...], wo_v[...]).astype(BF16)
        for k in (0, 1):
            for d in (0, 1):
                c = core if k == 0 else 1 - core
                do_v[pl.ds(row(s, d, c), QUARTER), :] = grad_o[(2 * k + d) * QUARTER:(2 * k + d + 1) * QUARTER]
        for j in range(0, hidden, 512):
            acc_o[:, j:j + 512] += dot_plain(z_b[pl.ds(0, QUARTER), :], gy_b[:, j:j + 512])

    def ds_relay(s, h):
        for d in (0, 1):
            ds_here(s, d, h).wait_recv()

            @pl.when(s < LAST)
            def _():
                ds_next(s + 1, d, h).start()
            ds_twin(s, d, h).start()

    def ds_step(s, carry):
        ds_relay(s, 0)
        project(s - 1)

        @pl.when(s < 5)
        def _():
            weight_step(s + 3)
        ds_relay(s, 1)
        for d in (0, 1):
            block_load(s, d, 0).start()
        for d in (0, 1):
            block_load(s, d, 0).wait()
        return carry

    lax.fori_loop(1, CHIPS, ds_step, 0)
    project(LAST)

    def drain(s, carry):
        for d in (0, 1):
            for h in (0, 1):
                ds_twin(s, d, h).wait_send()

            @pl.when(s > 0)
            def _():
                for h in (0, 1):
                    ds_here(s, d, h).wait_send()
        return carry
    lax.fori_loop(0, CHIPS, drain, 0)

    def drain_columns(col, carry):
        gys.drain(col)
        xs.drain(col)

        @pl.when(col > 0)
        def _():
            for r in (0, 1):
                for h in (0, 1):
                    send_sum(col, r, h).wait_send()
        return carry
    lax.fori_loop(0, 4, drain_columns, 0)
    for h in (0, 1):
        give(h).wait_send()


def solution(mesh):
    token_spec = P(("dp", "tp"), None)
    split_cols = P("dp", "tp")
    weight_cols = P(None, "tp")
    weight_rows = P("tp", None)

    def local_backward(x_norm, grad_y, u_gate, u_up, w_gate, w_up, w_down, x_in, gamma, grad_res, attn_out, w_out):
        own, hidden = x_norm.shape
        tokens, ffn = u_gate.shape
        cols = attn_out.shape[1]
        anywhere = pl.BlockSpec(memory_space=pl.ANY)
        inside = pl.BlockSpec(memory_space=pltpu.VMEM)
        shape = jax.ShapeDtypeStruct
        dma = pltpu.SemaphoreType.DMA
        outs = pl.pallas_call(
            kernel,
            out_shape=[
                pltpu.VMEM((own, hidden), BF16), pltpu.VMEM((tokens, cols), BF16),
                pltpu.VMEM((ffn, hidden), F32), pltpu.VMEM((ffn, hidden), F32), pltpu.VMEM((ffn, hidden), F32),
                pltpu.VMEM((cols, hidden), F32),
                shape((tokens, hidden), BF16), shape((tokens, hidden), BF16), shape((tokens, hidden), BF16),
                shape((32 * QUARTER, hidden), BF16),
                shape((CHIPS, ffn, ROWS), BF16), shape((CHIPS, ffn, ROWS), BF16), shape((CHIPS, ffn, ROWS), BF16),
            ],
            in_specs=[anywhere] * 8 + [inside] + [anywhere] * 3,
            out_specs=[inside] * 6 + [anywhere] * 7,
            scratch_shapes=[
                pltpu.VMEM((ffn, hidden), BF16), pltpu.VMEM((ffn, hidden), BF16), pltpu.VMEM((ffn, hidden), BF16),
                pltpu.VMEM((ROWS, hidden), BF16), pltpu.VMEM((ROWS, hidden), BF16),
                pltpu.VMEM((ffn, ROWS), BF16), pltpu.VMEM((ffn, ROWS), BF16),
                pltpu.VMEM((ffn, ROWS), BF16), pltpu.VMEM((ffn, ROWS), BF16), pltpu.VMEM((ffn, ROWS), BF16),
                pltpu.VMEM((ROWS, ffn), BF16), pltpu.VMEM((ROWS, ffn), BF16),
                pltpu.VMEM((own, hidden), F32), pltpu.VMEM((own, hidden), BF16), pltpu.VMEM((2, own, hidden), BF16),
                pltpu.VMEM((6, own, hidden), BF16), pltpu.VMEM((2, own, hidden), F32),
                pltpu.VMEM((2, QUARTER, hidden), BF16), pltpu.VMEM((own, hidden), BF16),
                pltpu.VMEM((tokens, cols), BF16), pltpu.VMEM((cols, hidden), BF16),
                dma((2, 4, 2)), dma((4, 2)), dma((4, 2)), dma((4, 2)), dma((2, 4, 2)), dma((2, 4, 2)),
                dma((2, 4, 2)), dma((4, 2)), dma((4, 2)), dma((4, 2)), dma((2, 4, 2)), dma((2, 4, 2)),
                dma((CHIPS, 4)), dma((CHIPS, 4)), dma((CHIPS, 4)), dma((CHIPS, 4)),
                dma, dma((2,)), dma((3, 2, 2)), dma((2, 4, 2, 2)), dma((2,)), dma((2,)),
                dma((5,)), dma((4,)), dma((2,)), dma((4,)), dma((3,)), dma((2,)),
            ],
            compiler_params=pltpu.CompilerParams(
                collective_id=0, has_side_effects=True, vmem_limit_bytes=44 * 2 ** 20),
            name="mlp_backward",
        )(x_norm, grad_y, u_gate.T, u_up.T, w_gate.T, w_up.T, w_down, x_in, gamma, grad_res, attn_out, w_out)
        grad_sum, grad_attn, gw_gate, gw_up, gw_down, gw_out = outs[:6]
        return grad_sum, grad_attn, gw_gate.T, gw_up.T, gw_down, gw_out

    return jax.shard_map(
        local_backward,
        mesh=mesh,
        in_specs=(token_spec, token_spec, split_cols, split_cols, weight_cols, weight_cols, weight_rows,
                  token_spec, P(None), token_spec, split_cols, weight_rows),
        out_specs=(token_spec, split_cols, split_cols, split_cols, token_spec, token_spec),
        check_vma=False,
    )
```

```python
import jax
import jax.numpy as jnp
from jax import lax
from jax.experimental import pallas as pl
from jax.experimental.pallas import tpu as pltpu
from jax.sharding import PartitionSpec as P

NORM_EPS = 1e-5
MESH = pl.DeviceIdType.MESH
BF16 = jnp.bfloat16
F32 = jnp.float32

CHIPS = 8
QUARTER = 128
HALF = 64
ROWS = 4 * QUARTER
LAST = CHIPS - 1
BOTH = (0, 1)
TILE = 32
WIDE = 512
PART = 64
PARTS = 2 * QUARTER // PART


def tile_at(i, size, base=0):
    return pl.ds(pl.multiple_of(base + i * size, size), size)


def dot_cols(a, b):
    return lax.dot_general(a, b, (((1,), (1,)), ((), ())), preferred_element_type=F32)


def dot_plain(a, b):
    return lax.dot_general(a, b, (((1,), (0,)), ((), ())), preferred_element_type=F32)


def kernel(x, gy, ug, uu, wg, wu, wd, xin, gamma, gres, att, wo,
           out_ds, do_v, acc_g, acc_u, acc_d, acc_o, gy_all, x_all, ds_all, rs_in, z_all, dg_all, du_all,
           wg_v, wu_v, wd_v,
           gy_b, x_b, ug_b, uu_b, z_b, dg_b, du_b, dgt_b, dut_b,
           p_own, p_send, p_recv, hold, own_sum, stage, y_in,
           att_v, wo_v,
           gy_zs, gy_zr, gy_ys, gy_yr, gy_ts, gy_tr, x_zs, x_zr, x_ys, x_yr, x_ts, x_tr,
           ds_ss, ds_rs, ds_ps, ds_pr, ps_sem, pr_sem, rss_sem, rsr_sem, yss_sem, ysr_sem,
           w_sem, gy_sem, x_sem, u_sem, keep_sem, stage_sem):
    hidden = gy.shape[1]
    own = gy.shape[0]
    t = lax.axis_index("tp")
    core = t % 2
    y = (t // 2) % 2
    z = t // 4
    edge = z % 3 == 0
    inner = z % 3 != 0
    pos = z + y * (7 - 2 * z)

    def device(chip, c):
        upper = chip // 4
        return 4 * (chip + upper * (7 - 2 * chip)) + 2 * upper + c

    onward = (device((pos + 1) % CHIPS, core), device((pos + LAST) % CHIPS, core))
    twin = t + 1 - 2 * core
    over = t + 2 - 4 * y
    beside = (t + 4 - 4 * (z // 3), t - 4 + 4 * ((3 - z) // 3))

    def signal(other):
        pl.semaphore_signal(barrier, inc=1, device_id={"tp": other}, device_id_type=MESH)

    barrier = pltpu.get_barrier_semaphore()
    signal(over)
    signal(twin)

    @pl.when(z < 3)
    def _():
        signal(beside[0])

    @pl.when(z > 0)
    def _():
        signal(beside[1])

    @pl.when(edge)
    def _():
        pl.semaphore_wait(barrier, 3)

    @pl.when(inner)
    def _():
        pl.semaphore_wait(barrier, 4)

    def remote(src, dst, send, recv, to):
        return pltpu.make_async_remote_copy(src_ref=src, dst_ref=dst, send_sem=send, recv_sem=recv,
                                            device_id={"tp": to}, device_id_type=MESH)

    def column(k):
        far = z // 2
        near = z + far * (3 - 2 * z)
        late = k // 2
        col = (1 - near) * k + near * ((1 - late) * (1 - k) + late * k)
        return col + far * (3 - 2 * col)

    def line(r):
        return y + r - 2 * y * r

    def first_row(col, r, c):
        return pl.multiple_of(((col * 2 + line(r)) * 2 + c) * own, own)

    def half(col, r, c, h):
        return pl.ds(pl.multiple_of(first_row(col, r, c) + h * QUARTER, QUARTER), QUARTER)

    class Stream:
        def __init__(self, own_ref, full, zs, zr, ys, yr, ts, tr):
            self.own, self.full = own_ref, full
            self.zs, self.zr, self.ys, self.yr, self.ts, self.tr = zs, zr, ys, yr, ts, tr

        def part(self, col, r, c, h):
            return self.full.at[half(col, r, c, h), :]

        def mine(self, h):
            return self.own.at[pl.ds(h * QUARTER, QUARTER), :]

        def along(self, col, h, side, src=None):
            dst = self.part(col, 0, core, h)
            return remote(dst if src is None else src, dst, self.zs.at[side, col, h], self.zr.at[col, h], beside[side])

        def across(self, col, h, src=None):
            dst = self.part(col, 0, core, h)
            return remote(dst if src is None else src, dst, self.ys.at[col, h], self.yr.at[col, h], over)

        def from_over(self, col, h):
            dst = self.part(col, 1, core, h)
            return remote(dst, dst, self.ys.at[col, h], self.yr.at[col, h], over)

        def hand(self, col, r, h, src=None):
            dst = self.part(col, r, core, h)
            return remote(dst if src is None else src, dst, self.ts.at[r, col, h], self.tr.at[r, col, h], twin)

        def from_twin(self, col, r, h):
            dst = self.part(col, r, 1 - core, h)
            return remote(dst, dst, self.ts.at[r, col, h], self.tr.at[r, col, h], twin)

        def relay(self, dist, h, side, held=False):
            col = z - dist if side == 0 else z + dist
            self.along(col, h, side).wait_recv()

            @pl.when(z < 3 if side == 0 else z > 0)
            def _():
                self.along(col, h, side).start()
            self.hand(col, 0, h).start()
            if not held:
                self.across(col, h).start()
            else:
                second = inner & (dist == 1) & (z == 2 - side)

                @pl.when(jnp.logical_not(second))
                def _():
                    self.across(col, h).start()

        def relay_row(self, dist, h, held=False):
            @pl.when(z >= dist)
            def _():
                self.relay(dist, h, 0, held)

            @pl.when(z + dist < 4)
            def _():
                self.relay(dist, h, 1, held)

            if held and h == 1:
                @pl.when(inner & (dist == 1))
                def _():
                    for q in BOTH:
                        self.across(column(2), q).start()

        def relay_over(self, k, h):
            self.from_over(column(k), h).wait_recv()
            self.hand(column(k), 1, h).start()

        def start_row(self):
            for h in BOTH:
                @pl.when(z < 3)
                def _():
                    self.along(z, h, 0, self.mine(h)).start()

                @pl.when(z > 0)
                def _():
                    self.along(z, h, 1, self.mine(h)).start()

        def start_rest(self):
            for h in BOTH:
                self.across(z, h, self.mine(h)).start()
                self.hand(z, 0, h, self.mine(h)).start()

        def load(self, n, buf, sem):
            k, r = n // 2, n % 2

            @pl.when(n == 0)
            def _():
                pltpu.make_async_copy(self.own, buf.at[pl.ds(0, own), :], sem.at[0]).start()

            @pl.when(n > 0)
            def _():
                self.block(n, core, buf, sem, 0).start()
            for h in BOTH:
                self.from_twin(column(k), r, h).wait_recv()
            self.block(n, 1 - core, buf, sem, 1).start()

        def block(self, n, c, buf, sem, i):
            rows = pl.ds(first_row(column(n // 2), n % 2, c), own)
            return pltpu.make_async_copy(self.full.at[rows, :], buf.at[pl.ds(i * own, own), :], sem.at[i])

        def landed(self, n, buf, sem):
            for i in BOTH:
                self.block(n, core, buf, sem, i).wait()

        def drain(self, col):
            for h in BOTH:
                self.across(col, h).wait_send()
                for r in BOTH:
                    self.hand(col, r, h).wait_send()

                @pl.when((z < 3) & (col <= z))
                def _():
                    self.along(col, h, 0).wait_send()

                @pl.when((z > 0) & (col >= z))
                def _():
                    self.along(col, h, 1).wait_send()

    gys = Stream(gy, gy_all, gy_zs, gy_zr, gy_ys, gy_yr, gy_ts, gy_tr)
    xs = Stream(x, x_all, x_zs, x_zr, x_ys, x_yr, x_ts, x_tr)
    gys.start_row()
    gys.start_rest()

    @pl.when(edge)
    def _():
        xs.start_row()

    loads = [pltpu.make_async_copy(a, b, w_sem.at[i]) for i, (a, b) in enumerate(
        ((wd, wd_v), (wg, wg_v), (wu, wu_v), (att, att_v), (wo, wo_v)))]
    for copy in loads:
        copy.start()

    def load_u(n):
        copies = []
        for i in BOTH:
            c = core if i == 0 else 1 - core
            rows = pl.ds(first_row(column(n // 2), n % 2, c), own)
            at = pl.ds(i * own, own)
            copies.append(pltpu.make_async_copy(ug.at[:, rows], ug_b.at[:, at], u_sem.at[i]))
            copies.append(pltpu.make_async_copy(uu.at[:, rows], uu_b.at[:, at], u_sem.at[2 + i]))
        return copies

    for copy in load_u(0):
        copy.start()

    acc_g[...] = jnp.zeros_like(acc_g)
    acc_u[...] = jnp.zeros_like(acc_u)
    acc_d[...] = jnp.zeros_like(acc_d)
    acc_o[...] = jnp.zeros_like(acc_o)

    def keep(n):
        return [pltpu.make_async_copy(a, b.at[n], keep_sem.at[i])
                for i, (a, b) in enumerate(((z_b, z_all), (dg_b, dg_all), (du_b, du_all)))]

    def swap(n):
        return remote(p_send, p_recv.at[n % 2], ps_sem, pr_sem.at[n % 2], twin)

    def rs_slot(side, col, r, h):
        return (rs_in.at[tile_at(((side * 4 + col) * 2 + line(r)) * PARTS + h, PART), :],
                rsr_sem.at[side, col, line(r), h])

    def send_sum(k, r, h):
        col = column(k)
        up = (col - z + 3) // 4
        dst, sem = rs_slot(1 - up, col, r, h)
        return remote(hold.at[(k - 1) * 2 + r, tile_at(h, PART), :], dst,
                      rss_sem.at[k - 1, r, h], sem, t - 4 + 8 * up)

    def take_sum(side, col, r, h, slot):
        src, sem = rs_slot(side, col, r, h)
        remote(stage.at[slot], src, rss_sem.at[0, 0, 0], sem, twin).wait_recv()
        copy = pltpu.make_async_copy(src, stage.at[slot], stage_sem.at[slot])
        copy.start()
        return copy

    def finish(n):
        k, r = n // 2, n % 2
        swap(n).wait_recv()

        @pl.when(k == 0)
        def _():
            def tile(i, carry):
                at = tile_at(i, TILE)
                own_sum[r, at, :] = p_own[at, :] + p_recv[n % 2, at, :].astype(F32)
                return carry
            lax.fori_loop(0, own // TILE, tile, 0)

        @pl.when(k > 0)
        def _():
            def tile(i, carry):
                at = tile_at(i, TILE)
                hold[(k - 1) * 2 + r, at, :] = (p_own[at, :] + p_recv[n % 2, at, :].astype(F32)).astype(BF16)
                return carry
            lax.fori_loop(0, own // TILE, tile, 0)

            @pl.when(edge & (k == 1))
            def _():
                for h in range(PARTS):
                    send_sum(k, r, h).start()

            @pl.when(edge & (k > 1) & (r == 1))
            def _():
                for q in BOTH:
                    for h in range(PARTS):
                        send_sum(k, 1 - q, h).start()

    def hidden_step(n, buf, sem):
        for copy in load_u(n):
            copy.wait()

        @pl.when(n > 0)
        def _():
            for copy in keep(n - 1):
                copy.wait()
        gys.landed(n, buf, sem)

        def hidden_tile(i, carry):
            at = pl.ds(pl.multiple_of(i * 256, 256), 256)
            grad_h = dot_cols(wd_v[...], buf[at, :])
            gate = ug_b[:, at].astype(F32)
            up = uu_b[:, at].astype(F32)
            sig = jax.nn.sigmoid(gate)
            act = gate * sig
            z_b[:, at] = (act * up).astype(BF16)
            grad_up = (grad_h * act).astype(BF16)
            grad_gate = (grad_h * up * (sig * (1.0 + gate * (1.0 - sig)))).astype(BF16)
            du_b[:, at] = grad_up
            dg_b[:, at] = grad_gate
            dut_b[at, :] = grad_up.T
            dgt_b[at, :] = grad_gate.T
            return carry
        lax.fori_loop(0, ROWS // 256, hidden_tile, 0)
        for copy in keep(n):
            copy.start()

        @pl.when(n < LAST)
        def _():
            for copy in load_u(n + 1):
                copy.start()

        @pl.when((n > 0) & (n % 2 == 0))
        def _():
            finish(n - 1)

        @pl.when(n > 0)
        def _():
            swap(n - 1).wait_send()

        def part_tile(j, carry):
            at = tile_at(j, WIDE)
            part = dot_plain(dgt_b[...], wg_v[:, at]) + dot_plain(dut_b[...], wu_v[:, at])
            p_own[:, at] = part[:own]
            p_send[:, at] = part[own:].astype(BF16)
            return carry
        lax.fori_loop(0, hidden // WIDE, part_tile, 0)
        swap(n).start()

    gys.load(0, gy_b, gy_sem)
    for copy in loads:
        copy.wait()
    hidden_step(0, gy_b, gy_sem)

    def hidden_pair(k, carry):
        finish(2 * k)
        for h in BOTH:
            gys.relay_row(k + 1, h, held=True)
            gys.relay_over(k, h)

            @pl.when(edge & (k == 3))
            def _():
                for side in BOTH:
                    @pl.when(z // 2 == 1 - side)
                    def _():
                        xs.relay(1, h, side)

        gys.load(2 * k + 1, x_b, x_sem)

        @pl.when(k < 3)
        def _():
            gys.load(2 * k + 2, gy_b, gy_sem)

        @pl.when(inner & (k == 1))
        def _():
            xs.start_row()
            xs.start_rest()
            for side in BOTH:
                @pl.when(z == 1 + side)
                def _():
                    for h in BOTH:
                        xs.relay(1, h, side)

        @pl.when(edge & (k == 2))
        def _():
            xs.start_rest()

        @pl.when(inner & (k == 3))
        def _():
            for side in BOTH:
                @pl.when(z == 2 - side)
                def _():
                    for h in BOTH:
                        xs.relay(1, h, side)
        hidden_step(2 * k + 1, x_b, x_sem)

        @pl.when(k < 3)
        def _():
            hidden_step(2 * k + 2, gy_b, gy_sem)
        return carry

    lax.fori_loop(0, 4, hidden_pair, 0)
    finish(LAST)
    for copy in keep(LAST):
        copy.wait()
    swap(LAST).wait_send()

    def carry_on(k, m):
        r, h = 1 - m // PARTS, m % PARTS
        col = column(k)
        up = (col - z + 3) // 4
        slot = m % 2
        take_sum(1 - up, col, r, h, slot).wait()
        mine = hold.at[(k - 1) * 2 + r, tile_at(h, PART), :]
        mine[...] = (mine[...].astype(F32) + stage[slot].astype(F32)).astype(BF16)
        send_sum(k, r, h).start()

    def settle(side, r):
        def part(h, carry):
            take_sum(side, z, r, h, h % 2).wait()
            at = tile_at(h, PART)
            own_sum[r, at, :] = own_sum[r, at, :] + stage[h % 2].astype(F32)
            return carry
        lax.fori_loop(0, PARTS, part, 0)

    def give(h):
        rows = pl.ds(h * QUARTER, QUARTER)
        return remote(p_send.at[rows, :], y_in.at[rows, :], yss_sem.at[h], ysr_sem.at[h], over)

    def give_over():
        for h in BOTH:
            def tile(i, carry):
                at = pl.ds(pl.multiple_of(h * QUARTER + i * 32, 32), 32)
                p_send[at, :] = own_sum[1, at, :].astype(BF16)
                return carry
            lax.fori_loop(0, QUARTER // 32, tile, 0)
            give(h).start()

    def weight_step(n):
        xs.load(n, x_b, x_sem)
        for i, c in ((0, core), (1, 1 - core)):
            @pl.when((n > 0) | (i == 1))
            def _():
                gys.block(n, c, gy_b, gy_sem, i).start()

        @pl.when(n == 0)
        def _():
            pltpu.make_async_copy(gy, gy_b.at[pl.ds(0, own), :], gy_sem.at[0]).start()
        back = [pltpu.make_async_copy(b.at[n], a, keep_sem.at[i])
                for i, (a, b) in enumerate(((z_b, z_all), (dg_b, dg_all), (du_b, du_all)))]
        for copy in back:
            copy.start()
        for copy in back:
            copy.wait()
        gys.landed(n, gy_b, gy_sem)
        xs.landed(n, x_b, x_sem)

        def tile(j, carry):
            at = tile_at(j, WIDE)
            acc_d[:, at] += dot_plain(z_b[...], gy_b[:, at])
            return carry
        lax.fori_loop(0, hidden // WIDE, tile, 0)

    def weight_rest():
        def tile(j, carry):
            at = tile_at(j, WIDE)
            acc_g[:, at] += dot_plain(dg_b[...], x_b[:, at])
            acc_u[:, at] += dot_plain(du_b[...], x_b[:, at])
            return carry
        lax.fori_loop(0, hidden // WIDE, tile, 0)

    def late_step(i, carry):
        @pl.when(inner)
        def _():
            carry_on(2, 2 * i)
            carry_on(2, 2 * i + 1)

        @pl.when(i < 2)
        def _():
            for h in BOTH:
                xs.relay_row(i + 2, h)
        xs.relay_over(i // 2, i % 2)

        @pl.when(i < 2)
        def _():
            weight_step(i)
            weight_rest()

        @pl.when(inner & (i > 1))
        def _():
            settle(z - 1, i - 2)
        return carry

    lax.fori_loop(0, 4, late_step, 0)

    def pass_two(m, carry):
        carry_on(3, m)
        carry_on(1, m - 2)
        return carry

    @pl.when(inner)
    def _():
        carry_on(3, 0)
        settle(2 - z, 1)
        give_over()
        carry_on(3, 1)
        lax.fori_loop(2, PARTS, pass_two, 0)
        settle(2 - z, 0)
    for h in BOTH:
        xs.relay_over(2, h)

    @pl.when(inner)
    def _():
        lax.fori_loop(PARTS, 2 * PARTS, pass_two, 0)
    for h in BOTH:
        xs.relay_over(3, h)

    norm_loads = [pltpu.make_async_copy(src, x_b.at[pl.ds(k * own, own), :], x_sem.at[k])
                  for k, src in enumerate((xin, gres))]
    for copy in norm_loads:
        copy.start()

    @pl.when(inner)
    def _():
        carry_on(1, 2 * PARTS - 2)
        carry_on(1, 2 * PARTS - 1)

    @pl.when(edge)
    def _():
        settle((3 - z) // 3, 1)
        give_over()
        settle((3 - z) // 3, 0)
    for copy in norm_loads:
        copy.wait()

    def row(s, d, c):
        source = (pos + (CHIPS - s if d == 0 else s)) % CHIPS
        return pl.multiple_of(device(source, c) * 2 * QUARTER + d * QUARTER, QUARTER)

    def block_load(s, d, k):
        c = core if k == 0 else 1 - core
        at = pl.ds((2 * k + d) * QUARTER, QUARTER)
        return pltpu.make_async_copy(ds_all.at[pl.ds(row(s, d, c), QUARTER), :], gy_b.at[at, :], gy_sem.at[2 * k + d])

    def ds_next(s, d, h, src=None):
        rows = pl.ds(pl.multiple_of(row(s - 1, d, core) + h * HALF, HALF), HALF)
        return remote(ds_all.at[rows, :] if src is None else src, ds_all.at[rows, :],
                      ds_ss.at[s, 2 * d + h], ds_rs.at[s, 2 * d + h], onward[d])

    def ds_here(s, d, h):
        rows = pl.ds(pl.multiple_of(row(s, d, core) + h * HALF, HALF), HALF)
        return remote(ds_all.at[rows, :], ds_all.at[rows, :],
                      ds_ss.at[s, 2 * d + h], ds_rs.at[s, 2 * d + h], onward[d])

    def ds_twin(s, d, h, src=None):
        rows = pl.ds(pl.multiple_of(row(s, d, core) + h * HALF, HALF), HALF)
        return remote(ds_all.at[rows, :] if src is None else src, ds_all.at[rows, :],
                      ds_ps.at[s, 2 * d + h], ds_pr.at[s, 2 * d + h], twin)

    def ds_from_twin(s, d, h):
        rows = pl.ds(pl.multiple_of(row(s, d, 1 - core) + h * HALF, HALF), HALF)
        return remote(ds_all.at[rows, :], ds_all.at[rows, :],
                      ds_ps.at[s, 2 * d + h], ds_pr.at[s, 2 * d + h], twin)

    gain = gamma[...].astype(F32)[None, :]
    for d in BOTH:
        give(d).wait_recv()
    for h in BOTH:
        for d in BOTH:
            def norm_tile(i, carry):
                here = pl.ds(pl.multiple_of(d * QUARTER + h * HALF + i * 16, 16), 16)
                skip = pl.ds(pl.multiple_of(2 * QUARTER + d * QUARTER + h * HALF + i * 16, 16), 16)
                grad_x = (own_sum[0, here, :] + y_in[here, :].astype(F32)).astype(BF16).astype(F32)
                xin_f = x_b[here, :].astype(F32)
                inv_rms = lax.rsqrt(jnp.mean(xin_f * xin_f, axis=-1, keepdims=True) + NORM_EPS)
                scaled = grad_x * gain
                proj = jnp.mean(scaled * xin_f, axis=-1, keepdims=True)
                grad_s = (x_b[skip, :].astype(F32)
                          + inv_rms * (scaled - xin_f * (inv_rms * inv_rms) * proj)).astype(BF16)
                out_ds[here, :] = grad_s
                return carry
            lax.fori_loop(0, HALF // 16, norm_tile, 0)
            mine = out_ds.at[pl.ds(d * QUARTER + h * HALF, HALF), :]
            ds_next(1, d, h, mine).start()
            ds_twin(0, d, h, mine).start()

    for d in BOTH:
        gy_b[pl.ds(d * QUARTER, QUARTER), :] = out_ds[pl.ds(d * QUARTER, QUARTER), :]

    def project(s):
        for d in BOTH:
            for h in BOTH:
                ds_from_twin(s, d, h).wait_recv()
            block_load(s, d, 1).start()
        for d in BOTH:
            block_load(s, d, 1).wait()
        for k in BOTH:
            for d in BOTH:
                c = core if k == 0 else 1 - core
                rows = pl.ds(row(s, d, c), QUARTER)
                at = pl.ds((2 * k + d) * QUARTER, QUARTER)
                z_b[pl.ds(0, QUARTER), at] = att_v[rows, :].T
        grad_o = dot_cols(gy_b[...], wo_v[...]).astype(BF16)
        for k in BOTH:
            for d in BOTH:
                c = core if k == 0 else 1 - core
                do_v[pl.ds(row(s, d, c), QUARTER), :] = grad_o[(2 * k + d) * QUARTER:(2 * k + d + 1) * QUARTER]
        for j in range(0, hidden, WIDE):
            acc_o[:, j:j + WIDE] += dot_plain(z_b[:QUARTER, :], gy_b[:, j:j + WIDE])

    def ds_relay(s, h):
        for d in BOTH:
            ds_here(s, d, h).wait_recv()

            @pl.when(s < LAST)
            def _():
                ds_next(s + 1, d, h).start()
            ds_twin(s, d, h).start()

    def ds_step(s, carry):
        ds_relay(s, 0)
        project(s - 1)

        @pl.when(s < LAST)
        def _():
            weight_step(s + 1)
        ds_relay(s, 1)
        for d in BOTH:
            block_load(s, d, 0).start()

        @pl.when(s < LAST)
        def _():
            weight_rest()
        for d in BOTH:
            block_load(s, d, 0).wait()
        return carry

    lax.fori_loop(1, CHIPS, ds_step, 0)
    project(LAST)

    def drain(s, carry):
        for d in BOTH:
            for h in BOTH:
                ds_twin(s, d, h).wait_send()

            @pl.when(s > 0)
            def _():
                for h in BOTH:
                    ds_here(s, d, h).wait_send()
        return carry
    lax.fori_loop(0, CHIPS, drain, 0)

    def drain_columns(col, carry):
        gys.drain(col)
        xs.drain(col)

        @pl.when(col > 0)
        def _():
            for r in BOTH:
                for h in range(PARTS):
                    send_sum(col, r, h).wait_send()
        return carry
    lax.fori_loop(0, 4, drain_columns, 0)
    for h in BOTH:
        give(h).wait_send()


def write_out(*refs):
    count = len(refs) // 2
    copies = [pltpu.make_async_copy(refs[i], refs[count + i], refs[-1].at[i]) for i in range(count)]
    for copy in copies:
        copy.start()
    for copy in copies:
        copy.wait()


def solution(mesh):
    token_spec = P(("dp", "tp"), None)
    split_cols = P("dp", "tp")
    weight_cols = P(None, "tp")
    weight_rows = P("tp", None)

    def local_backward(x_norm, grad_y, u_gate, u_up, w_gate, w_up, w_down, x_in, gamma, grad_res, attn_out, w_out):
        own, hidden = x_norm.shape
        tokens, ffn = u_gate.shape
        cols = attn_out.shape[1]
        anywhere = pl.BlockSpec(memory_space=pl.ANY)
        inside = pl.BlockSpec(memory_space=pltpu.VMEM)
        shape = jax.ShapeDtypeStruct
        dma = pltpu.SemaphoreType.DMA
        pair = (2,)
        stream_sems = [dma((2, 4, 2))] + [dma((4, 2))] * 3 + [dma((2, 4, 2))] * 2
        outs = pl.pallas_call(
            kernel,
            out_shape=[
                pltpu.VMEM((own, hidden), BF16), pltpu.VMEM((tokens, cols), BF16),
                pltpu.VMEM((ffn, hidden), F32), pltpu.VMEM((ffn, hidden), F32), pltpu.VMEM((ffn, hidden), F32),
                pltpu.VMEM((cols, hidden), F32),
                shape((tokens, hidden), BF16), shape((tokens, hidden), BF16), shape((tokens, hidden), BF16),
                shape((tokens, hidden), BF16),
                shape((CHIPS, ffn, ROWS), BF16), shape((CHIPS, ffn, ROWS), BF16), shape((CHIPS, ffn, ROWS), BF16),
            ],
            in_specs=[anywhere] * 8 + [inside] + [anywhere] * 3,
            out_specs=[inside] * 6 + [anywhere] * 7,
            scratch_shapes=[
                pltpu.VMEM((ffn, hidden), BF16), pltpu.VMEM((ffn, hidden), BF16), pltpu.VMEM((ffn, hidden), BF16),
                pltpu.VMEM((ROWS, hidden), BF16), pltpu.VMEM((ROWS, hidden), BF16),
                pltpu.VMEM((ffn, ROWS), BF16), pltpu.VMEM((ffn, ROWS), BF16),
                pltpu.VMEM((ffn, ROWS), BF16), pltpu.VMEM((ffn, ROWS), BF16), pltpu.VMEM((ffn, ROWS), BF16),
                pltpu.VMEM((ROWS, ffn), BF16), pltpu.VMEM((ROWS, ffn), BF16),
                pltpu.VMEM((own, hidden), F32), pltpu.VMEM((own, hidden), BF16), pltpu.VMEM((2, own, hidden), BF16),
                pltpu.VMEM((6, own, hidden), BF16), pltpu.VMEM((2, own, hidden), F32),
                pltpu.VMEM((2, PART, hidden), BF16), pltpu.VMEM((own, hidden), BF16),
                pltpu.VMEM((tokens, cols), BF16), pltpu.VMEM((cols, hidden), BF16),
                *stream_sems,
                *stream_sems,
                *[dma((CHIPS, 4))] * 4,
                dma, dma(pair), dma((3, 2, PARTS)), dma((2, 4, 2, PARTS)), dma(pair), dma(pair),
                dma((5,)), dma((4,)), dma(pair), dma((4,)), dma((3,)), dma(pair),
            ],
            compiler_params=pltpu.CompilerParams(
                collective_id=0, has_side_effects=True, vmem_limit_bytes=44 * 2 ** 20),
            name="mlp_backward",
        )(x_norm, grad_y, u_gate.T, u_up.T, w_gate.T, w_up.T, w_down, x_in, gamma, grad_res, attn_out, w_out)
        results = outs[:6]
        grad_sum, grad_attn, gw_gate, gw_up, gw_down, gw_out = pl.pallas_call(
            write_out,
            out_shape=[shape(a.shape, a.dtype) for a in results],
            in_specs=[inside] * len(results),
            out_specs=[anywhere] * len(results),
            scratch_shapes=[dma((len(results),))],
            compiler_params=pltpu.CompilerParams(vmem_limit_bytes=2 ** 20),
            name="write_out",
        )(*results)
        return grad_sum, grad_attn, gw_gate.T, gw_up.T, gw_down, gw_out

    return jax.shard_map(
        local_backward,
        mesh=mesh,
        in_specs=(token_spec, token_spec, split_cols, split_cols, weight_cols, weight_cols, weight_rows,
                  token_spec, P(None), token_spec, split_cols, weight_rows),
        out_specs=(token_spec, split_cols, split_cols, split_cols, token_spec, token_spec),
        check_vma=False,
    )
```

```python
import jax
import jax.numpy as jnp
from jax import lax
from jax.experimental import pallas as pl
from jax.experimental.pallas import tpu as pltpu
from jax.sharding import PartitionSpec as P

NORM_EPS = 1e-5
MESH = pl.DeviceIdType.MESH
BF16 = jnp.bfloat16
F32 = jnp.float32

CHIPS = 8
QUARTER = 128
HALF = 64
ROWS = 4 * QUARTER
LAST = CHIPS - 1
BOTH = (0, 1)
TILE = 32
WIDE = 512
PART = 64
PARTS = 2 * QUARTER // PART
SPARE = 64


def tile_at(i, size, base=0):
    return pl.ds(pl.multiple_of(base + i * size, size), size)


def dot_cols(a, b):
    return lax.dot_general(a, b, (((1,), (1,)), ((), ())), preferred_element_type=F32)


def dot_plain(a, b):
    return lax.dot_general(a, b, (((1,), (0,)), ((), ())), preferred_element_type=F32)


def kernel(x, gy, ug, uu, wg, wu, wd, xin, gamma, gres, att, wo,
           out_ds, do_v, acc_g, acc_u, acc_d, acc_o, gy_all, x_all, ds_all, rs_in, z_all, dg_all, du_all,
           wg_v, wu_v, wd_v,
           gy_b, x_b, ug_b, uu_b, z_b, dg_b, du_b, dgt_b, dut_b,
           p_own, p_send, p_recv, hold, own_sum, stage, y_in,
           att_v, wo_v,
           gy_zs, gy_zr, gy_ys, gy_yr, gy_ts, gy_tr, x_zs, x_zr, x_ys, x_yr, x_ts, x_tr, e_zs, e_zr, e_ts, e_tr,
           ds_ss, ds_rs, ds_ps, ds_pr, ps_sem, pr_sem, rss_sem, rsr_sem, yss_sem, ysr_sem,
           w_sem, gy_sem, x_sem, u_sem, keep_sem, stage_sem):
    hidden = gy.shape[1]
    own = gy.shape[0]
    t = lax.axis_index("tp")
    core = t % 2
    y = (t // 2) % 2
    z = t // 4
    edge = z % 3 == 0
    inner = z % 3 != 0
    pos = z + y * (7 - 2 * z)

    def device(chip, c):
        upper = chip // 4
        return 4 * (chip + upper * (7 - 2 * chip)) + 2 * upper + c

    onward = (device((pos + 1) % CHIPS, core), device((pos + LAST) % CHIPS, core))
    twin = t + 1 - 2 * core
    over = t + 2 - 4 * y
    beside = (t + 4 - 4 * (z // 3), t - 4 + 4 * ((3 - z) // 3))

    def signal(other):
        pl.semaphore_signal(barrier, inc=1, device_id={"tp": other}, device_id_type=MESH)

    barrier = pltpu.get_barrier_semaphore()
    signal(over)
    signal(twin)

    @pl.when(z < 3)
    def _():
        signal(beside[0])

    @pl.when(z > 0)
    def _():
        signal(beside[1])

    @pl.when(edge)
    def _():
        pl.semaphore_wait(barrier, 3)

    @pl.when(inner)
    def _():
        pl.semaphore_wait(barrier, 4)

    def remote(src, dst, send, recv, to):
        return pltpu.make_async_remote_copy(src_ref=src, dst_ref=dst, send_sem=send, recv_sem=recv,
                                            device_id={"tp": to}, device_id_type=MESH)

    def column(k):
        far = z // 2
        near = z + far * (3 - 2 * z)
        late = k // 2
        col = (1 - near) * k + near * ((1 - late) * (1 - k) + late * k)
        return col + far * (3 - 2 * col)

    def line(r):
        return y + r - 2 * y * r

    def first_row(col, r, c):
        return pl.multiple_of(((col * 2 + line(r)) * 2 + c) * own, own)

    def half(col, r, c, h):
        return pl.ds(pl.multiple_of(first_row(col, r, c) + h * QUARTER, QUARTER), QUARTER)

    class Stream:
        def __init__(self, own_ref, full, zs, zr, ys, yr, ts, tr, spare=None):
            self.own, self.full = own_ref, full
            self.spare = spare
            self.zs, self.zr, self.ys, self.yr, self.ts, self.tr = zs, zr, ys, yr, ts, tr

        def part(self, col, r, c, h, short=False):
            if short and self.spare is not None and h == 1:
                start = pl.multiple_of(first_row(col, r, c) + QUARTER, QUARTER)
                return self.full.at[pl.ds(start, QUARTER - SPARE), :]
            return self.full.at[half(col, r, c, h), :]

        def either(self, col, h, act):
            if self.spare is None or h == 0:
                act(False)
                return
            thin = (col % 3 != 0) & (col != z)
            pl.when(thin)(lambda: act(True))
            pl.when(jnp.logical_not(thin))(lambda: act(False))

        def spare_part(self, col, c):
            start = pl.multiple_of(first_row(col, 1, c) + 2 * QUARTER - SPARE, 16)
            return self.full.at[pl.ds(start, SPARE), :]

        def spare_along(self, col, side):
            dst = self.spare_part(col, core)
            return remote(dst, dst, self.spare[0].at[side, col], self.spare[1].at[col], beside[side])

        def spare_hand(self, col, c):
            dst = self.spare_part(col, c)
            return remote(dst, dst, self.spare[2].at[col], self.spare[3].at[col], twin)

        def spare_start(self):
            @pl.when(inner)
            def _():
                for side in BOTH:
                    self.spare_along(z, side).start()

        def spare_relay(self, dist):
            for side in BOTH:
                col = z - dist if side == 0 else z + dist

                @pl.when((col == 1) | (col == 2))
                def _():
                    self.spare_along(col, side).wait_recv()

                    @pl.when(z < 3 if side == 0 else z > 0)
                    def _():
                        self.spare_along(col, side).start()
                    self.spare_hand(col, core).start()

        def mine(self, h):
            return self.own.at[pl.ds(h * QUARTER, QUARTER), :]

        def along(self, col, h, side, src=None):
            dst = self.part(col, 0, core, h)
            return remote(dst if src is None else src, dst, self.zs.at[side, col, h], self.zr.at[col, h], beside[side])

        def across(self, col, h, src=None, short=False):
            dst = self.part(col, 0, core, h, short)
            return remote(dst if src is None else src, dst, self.ys.at[col, h], self.yr.at[col, h], over)

        def from_over(self, col, h, short):
            dst = self.part(col, 1, core, h, short)
            return remote(dst, dst, self.ys.at[col, h], self.yr.at[col, h], over)

        def hand(self, col, r, h, src=None, short=False):
            dst = self.part(col, r, core, h, short)
            return remote(dst if src is None else src, dst, self.ts.at[r, col, h], self.tr.at[r, col, h], twin)

        def from_twin(self, col, r, h, short=False):
            dst = self.part(col, r, 1 - core, h, short)
            return remote(dst, dst, self.ts.at[r, col, h], self.tr.at[r, col, h], twin)

        def relay(self, dist, h, side, held=False):
            col = z - dist if side == 0 else z + dist
            self.along(col, h, side).wait_recv()

            @pl.when(z < 3 if side == 0 else z > 0)
            def _():
                self.along(col, h, side).start()
            self.hand(col, 0, h).start()
            if not held:
                self.either(col, h, lambda short: self.across(col, h, short=short).start())
            else:
                second = inner & (dist == 1) & (z == 2 - side)

                @pl.when(jnp.logical_not(second))
                def _():
                    self.across(col, h).start()

        def relay_row(self, dist, h, held=False):
            @pl.when(z >= dist)
            def _():
                self.relay(dist, h, 0, held)

            @pl.when(z + dist < 4)
            def _():
                self.relay(dist, h, 1, held)

            if held and h == 1:
                @pl.when(inner & (dist == 1))
                def _():
                    for q in BOTH:
                        self.across(column(2), q).start()

        def relay_over(self, k, h):
            col = column(k)

            def act(short):
                self.from_over(col, h, short).wait_recv()
                self.hand(col, 1, h, short=short).start()
            self.either(col, h, act)

        def start_row(self):
            for h in BOTH:
                @pl.when(z < 3)
                def _():
                    self.along(z, h, 0, self.mine(h)).start()

                @pl.when(z > 0)
                def _():
                    self.along(z, h, 1, self.mine(h)).start()

        def start_rest(self):
            for h in BOTH:
                self.across(z, h, self.mine(h)).start()
                self.hand(z, 0, h, self.mine(h)).start()

        def load(self, n, buf, sem):
            k, r = n // 2, n % 2

            @pl.when(n == 0)
            def _():
                pltpu.make_async_copy(self.own, buf.at[pl.ds(0, own), :], sem.at[0]).start()

            @pl.when(n > 0)
            def _():
                self.block(n, core, buf, sem, 0).start()
            if self.spare is None:
                for h in BOTH:
                    self.from_twin(column(k), r, h).wait_recv()
            else:
                cut = (k > 0) & (r == 1) & (column(k) % 3 != 0)
                self.from_twin(column(k), r, 0).wait_recv()

                @pl.when(cut)
                def _():
                    self.from_twin(column(k), r, 1, True).wait_recv()
                    self.spare_hand(column(k), 1 - core).wait_recv()

                @pl.when(jnp.logical_not(cut))
                def _():
                    self.from_twin(column(k), r, 1).wait_recv()
            self.block(n, 1 - core, buf, sem, 1).start()

        def block(self, n, c, buf, sem, i):
            rows = pl.ds(first_row(column(n // 2), n % 2, c), own)
            return pltpu.make_async_copy(self.full.at[rows, :], buf.at[pl.ds(i * own, own), :], sem.at[i])

        def landed(self, n, buf, sem):
            for i in BOTH:
                self.block(n, core, buf, sem, i).wait()

        def drain(self, col):
            for h in BOTH:
                self.hand(col, 0, h).wait_send()

                def act(short):
                    self.across(col, h, short=short).wait_send()
                    self.hand(col, 1, h, short=short).wait_send()
                    if short:
                        self.spare_hand(col, core).wait_send()
                self.either(col, h, act)
            for side in BOTH:
                @pl.when((z < 3) & (col <= z) if side == 0 else (z > 0) & (col >= z))
                def _():
                    for h in BOTH:
                        self.along(col, h, side).wait_send()
                    if self.spare is not None:
                        @pl.when(col % 3 != 0)
                        def _():
                            self.spare_along(col, side).wait_send()

    gys = Stream(gy, gy_all, gy_zs, gy_zr, gy_ys, gy_yr, gy_ts, gy_tr)
    xs = Stream(x, x_all, x_zs, x_zr, x_ys, x_yr, x_ts, x_tr, (e_zs, e_zr, e_ts, e_tr))
    gys.start_row()
    gys.start_rest()

    @pl.when(edge)
    def _():
        xs.start_row()

    loads = [pltpu.make_async_copy(a, b, w_sem.at[i]) for i, (a, b) in enumerate(
        ((wd, wd_v), (wg, wg_v), (wu, wu_v), (att, att_v), (wo, wo_v)))]
    for copy in loads:
        copy.start()

    def load_u(n):
        copies = []
        for i in BOTH:
            c = core if i == 0 else 1 - core
            rows = pl.ds(first_row(column(n // 2), n % 2, c), own)
            at = pl.ds(i * own, own)
            copies.append(pltpu.make_async_copy(ug.at[:, rows], ug_b.at[:, at], u_sem.at[i]))
            copies.append(pltpu.make_async_copy(uu.at[:, rows], uu_b.at[:, at], u_sem.at[2 + i]))
        return copies

    for copy in load_u(0):
        copy.start()

    acc_g[...] = jnp.zeros_like(acc_g)
    acc_u[...] = jnp.zeros_like(acc_u)
    acc_d[...] = jnp.zeros_like(acc_d)
    acc_o[...] = jnp.zeros_like(acc_o)

    def keep(n):
        return [pltpu.make_async_copy(a, b.at[n], keep_sem.at[i])
                for i, (a, b) in enumerate(((z_b, z_all), (dg_b, dg_all), (du_b, du_all)))]

    def swap(n):
        return remote(p_send, p_recv.at[n % 2], ps_sem, pr_sem.at[n % 2], twin)

    def rs_slot(side, col, r, h):
        return (rs_in.at[tile_at(((side * 4 + col) * 2 + line(r)) * PARTS + h, PART), :],
                rsr_sem.at[side, col, line(r), h])

    def send_sum(k, r, h):
        col = column(k)
        up = (col - z + 3) // 4
        dst, sem = rs_slot(1 - up, col, r, h)
        return remote(hold.at[(k - 1) * 2 + r, tile_at(h, PART), :], dst,
                      rss_sem.at[k - 1, r, h], sem, t - 4 + 8 * up)

    def take_sum(side, col, r, h, slot):
        src, sem = rs_slot(side, col, r, h)
        remote(stage.at[slot], src, rss_sem.at[0, 0, 0], sem, twin).wait_recv()
        copy = pltpu.make_async_copy(src, stage.at[slot], stage_sem.at[slot])
        copy.start()
        return copy

    def finish(n):
        k, r = n // 2, n % 2
        swap(n).wait_recv()

        @pl.when(k == 0)
        def _():
            def tile(i, carry):
                at = tile_at(i, TILE)
                own_sum[r, at, :] = p_own[at, :] + p_recv[n % 2, at, :].astype(F32)
                return carry
            lax.fori_loop(0, own // TILE, tile, 0)

        @pl.when(k > 0)
        def _():
            def tile(i, carry):
                at = tile_at(i, TILE)
                hold[(k - 1) * 2 + r, at, :] = (p_own[at, :] + p_recv[n % 2, at, :].astype(F32)).astype(BF16)
                return carry
            lax.fori_loop(0, own // TILE, tile, 0)

            @pl.when(edge & (k == 1))
            def _():
                for h in range(PARTS):
                    send_sum(k, r, h).start()

            @pl.when(edge & (k > 1) & (r == 1))
            def _():
                for h in range(PARTS):
                    send_sum(k, 1, h).start()

            @pl.when(edge & (k == 3) & (r == 1))
            def _():
                for h in range(PARTS):
                    send_sum(3, 0, h).start()

    def hidden_step(n, buf, sem):
        for copy in load_u(n):
            copy.wait()

        @pl.when(n > 0)
        def _():
            for copy in keep(n - 1):
                copy.wait()
        gys.landed(n, buf, sem)

        def hidden_tile(i, carry):
            at = pl.ds(pl.multiple_of(i * 256, 256), 256)
            grad_h = dot_cols(wd_v[...], buf[at, :])
            gate = ug_b[:, at].astype(F32)
            up = uu_b[:, at].astype(F32)
            sig = jax.nn.sigmoid(gate)
            act = gate * sig
            z_b[:, at] = (act * up).astype(BF16)
            grad_up = (grad_h * act).astype(BF16)
            grad_gate = (grad_h * up * (sig * (1.0 + gate * (1.0 - sig)))).astype(BF16)
            du_b[:, at] = grad_up
            dg_b[:, at] = grad_gate
            dut_b[at, :] = grad_up.T
            dgt_b[at, :] = grad_gate.T
            return carry
        lax.fori_loop(0, ROWS // 256, hidden_tile, 0)
        for copy in keep(n):
            copy.start()

        @pl.when(n < LAST)
        def _():
            for copy in load_u(n + 1):
                copy.start()

        @pl.when((n > 0) & (n % 2 == 0))
        def _():
            finish(n - 1)

        @pl.when(n > 0)
        def _():
            swap(n - 1).wait_send()

        def part_tile(j, carry):
            at = tile_at(j, WIDE)
            part = dot_plain(dgt_b[...], wg_v[:, at]) + dot_plain(dut_b[...], wu_v[:, at])
            p_own[:, at] = part[:own]
            p_send[:, at] = part[own:].astype(BF16)
            return carry
        lax.fori_loop(0, hidden // WIDE, part_tile, 0)
        swap(n).start()

    gys.load(0, gy_b, gy_sem)
    for copy in loads:
        copy.wait()
    hidden_step(0, gy_b, gy_sem)

    def hidden_pair(k, carry):
        finish(2 * k)
        for h in BOTH:
            gys.relay_row(k + 1, h, held=True)
            gys.relay_over(k, h)

            @pl.when(edge & (k == 3))
            def _():
                for side in BOTH:
                    @pl.when(z // 2 == 1 - side)
                    def _():
                        xs.relay(1, h, side)

        @pl.when(inner & (k == 1))
        def _():
            xs.start_row()
            xs.start_rest()
            for side in BOTH:
                @pl.when(z == 1 + side)
                def _():
                    for h in BOTH:
                        xs.relay(1, h, side)

        gys.load(2 * k + 1, x_b, x_sem)

        @pl.when(k < 3)
        def _():
            gys.load(2 * k + 2, gy_b, gy_sem)

        @pl.when(edge & (k == 2))
        def _():
            xs.start_rest()

        @pl.when(inner & (k == 3))
        def _():
            for side in BOTH:
                @pl.when(z == 2 - side)
                def _():
                    for h in BOTH:
                        xs.relay(1, h, side)
        hidden_step(2 * k + 1, x_b, x_sem)

        @pl.when(k < 3)
        def _():
            hidden_step(2 * k + 2, gy_b, gy_sem)
        return carry

    lax.fori_loop(0, 4, hidden_pair, 0)
    finish(LAST)
    for copy in keep(LAST):
        copy.wait()
    swap(LAST).wait_send()

    def carry_on(k, m):
        r, h = 1 - m // PARTS, m % PARTS
        col = column(k)
        up = (col - z + 3) // 4
        slot = m % 2
        take_sum(1 - up, col, r, h, slot).wait()
        mine = hold.at[(k - 1) * 2 + r, tile_at(h, PART), :]
        mine[...] = (mine[...].astype(F32) + stage[slot].astype(F32)).astype(BF16)
        send_sum(k, r, h).start()

    def settle(side, r):
        def part(h, carry):
            take_sum(side, z, r, h, h % 2).wait()
            at = tile_at(h, PART)
            own_sum[r, at, :] = own_sum[r, at, :] + stage[h % 2].astype(F32)
            return carry
        lax.fori_loop(0, PARTS, part, 0)

    def give(h):
        rows = pl.ds(h * QUARTER, QUARTER)
        return remote(p_send.at[rows, :], y_in.at[rows, :], yss_sem.at[h], ysr_sem.at[h], over)

    def give_over():
        for h in BOTH:
            def tile(i, carry):
                at = pl.ds(pl.multiple_of(h * QUARTER + i * 32, 32), 32)
                p_send[at, :] = own_sum[1, at, :].astype(BF16)
                return carry
            lax.fori_loop(0, QUARTER // 32, tile, 0)
            give(h).start()

    def weight_step(n):
        xs.load(n, x_b, x_sem)
        for i, c in ((0, core), (1, 1 - core)):
            @pl.when((n > 0) | (i == 1))
            def _():
                gys.block(n, c, gy_b, gy_sem, i).start()

        @pl.when(n == 0)
        def _():
            pltpu.make_async_copy(gy, gy_b.at[pl.ds(0, own), :], gy_sem.at[0]).start()
        back = [pltpu.make_async_copy(b.at[n], a, keep_sem.at[i])
                for i, (a, b) in enumerate(((z_b, z_all), (dg_b, dg_all), (du_b, du_all)))]
        for copy in back:
            copy.start()
        for copy in back:
            copy.wait()
        gys.landed(n, gy_b, gy_sem)
        xs.landed(n, x_b, x_sem)

        def tile(j, carry):
            at = tile_at(j, WIDE)
            acc_d[:, at] += dot_plain(z_b[...], gy_b[:, at])
            return carry
        lax.fori_loop(0, hidden // WIDE, tile, 0)

    def weight_rest():
        def tile(j, carry):
            at = tile_at(j, WIDE)
            acc_g[:, at] += dot_plain(dg_b[...], x_b[:, at])
            acc_u[:, at] += dot_plain(du_b[...], x_b[:, at])
            return carry
        lax.fori_loop(0, hidden // WIDE, tile, 0)

    def late_step(i, carry):
        @pl.when(inner & (i < 2))
        def _():
            carry_on(2, 2 * i)
            carry_on(2, 2 * i + 1)

        @pl.when(inner & (i > 1))
        def _():
            carry_on(3, 2 * i - 4)
            carry_on(3, 2 * i - 3)

        @pl.when(i < 2)
        def _():
            for h in BOTH:
                xs.relay_row(i + 2, h)

        for h in BOTH:
            @pl.when(i == h)
            def _():
                xs.relay_over(0, h)
                if h == 1:
                    xs.spare_start()

                    @pl.when(edge)
                    def _():
                        for q in range(PARTS):
                            send_sum(2, 0, q).start()

            @pl.when(i == 2 + h)
            def _():
                xs.relay_over(1, h)

        @pl.when(i < 2)
        def _():
            weight_step(i)
            weight_rest()

        @pl.when(inner & (i > 1))
        def _():
            settle(z - 1, i - 2)
        return carry

    lax.fori_loop(0, 4, late_step, 0)

    @pl.when(inner)
    def _():
        settle(2 - z, 1)
        give_over()

        def both_ways(m, carry):
            carry_on(1, m)
            carry_on(3, m + PARTS)
            return carry
        lax.fori_loop(0, PARTS, both_ways, 0)
    for h in BOTH:
        xs.relay_over(2, h)

    @pl.when(edge)
    def _():
        settle((3 - z) // 3, 1)
        give_over()
    xs.spare_relay(1)

    @pl.when(inner)
    def _():
        def both_ways(m, carry):
            carry_on(1, m)
            carry_on(2, m)
            return carry
        lax.fori_loop(PARTS, 2 * PARTS, both_ways, 0)
    xs.spare_relay(2)
    for h in BOTH:
        xs.relay_over(3, h)

    norm_loads = [pltpu.make_async_copy(src, x_b.at[pl.ds(k * own, own), :], x_sem.at[k])
                  for k, src in enumerate((xin, gres))]
    for copy in norm_loads:
        copy.start()

    @pl.when(inner)
    def _():
        settle(2 - z, 0)

    @pl.when(edge)
    def _():
        settle((3 - z) // 3, 0)
    for copy in norm_loads:
        copy.wait()

    def row(s, d, c):
        source = (pos + (CHIPS - s if d == 0 else s)) % CHIPS
        return pl.multiple_of(device(source, c) * 2 * QUARTER + d * QUARTER, QUARTER)

    def block_load(s, d, k):
        c = core if k == 0 else 1 - core
        at = pl.ds((2 * k + d) * QUARTER, QUARTER)
        return pltpu.make_async_copy(ds_all.at[pl.ds(row(s, d, c), QUARTER), :], gy_b.at[at, :], gy_sem.at[2 * k + d])

    def ds_next(s, d, h, src=None):
        rows = pl.ds(pl.multiple_of(row(s - 1, d, core) + h * HALF, HALF), HALF)
        return remote(ds_all.at[rows, :] if src is None else src, ds_all.at[rows, :],
                      ds_ss.at[s, 2 * d + h], ds_rs.at[s, 2 * d + h], onward[d])

    def ds_here(s, d, h):
        rows = pl.ds(pl.multiple_of(row(s, d, core) + h * HALF, HALF), HALF)
        return remote(ds_all.at[rows, :], ds_all.at[rows, :],
                      ds_ss.at[s, 2 * d + h], ds_rs.at[s, 2 * d + h], onward[d])

    def ds_twin(s, d, h, src=None):
        rows = pl.ds(pl.multiple_of(row(s, d, core) + h * HALF, HALF), HALF)
        return remote(ds_all.at[rows, :] if src is None else src, ds_all.at[rows, :],
                      ds_ps.at[s, 2 * d + h], ds_pr.at[s, 2 * d + h], twin)

    def ds_from_twin(s, d, h):
        rows = pl.ds(pl.multiple_of(row(s, d, 1 - core) + h * HALF, HALF), HALF)
        return remote(ds_all.at[rows, :], ds_all.at[rows, :],
                      ds_ps.at[s, 2 * d + h], ds_pr.at[s, 2 * d + h], twin)

    gain = gamma[...].astype(F32)[None, :]
    for d in BOTH:
        give(d).wait_recv()
    for h in BOTH:
        for d in BOTH:
            def norm_tile(i, carry):
                here = pl.ds(pl.multiple_of(d * QUARTER + h * HALF + i * 16, 16), 16)
                skip = pl.ds(pl.multiple_of(2 * QUARTER + d * QUARTER + h * HALF + i * 16, 16), 16)
                grad_x = (own_sum[0, here, :] + y_in[here, :].astype(F32)).astype(BF16).astype(F32)
                xin_f = x_b[here, :].astype(F32)
                inv_rms = lax.rsqrt(jnp.mean(xin_f * xin_f, axis=-1, keepdims=True) + NORM_EPS)
                scaled = grad_x * gain
                proj = jnp.mean(scaled * xin_f, axis=-1, keepdims=True)
                grad_s = (x_b[skip, :].astype(F32)
                          + inv_rms * (scaled - xin_f * (inv_rms * inv_rms) * proj)).astype(BF16)
                out_ds[here, :] = grad_s
                return carry
            lax.fori_loop(0, HALF // 16, norm_tile, 0)
            mine = out_ds.at[pl.ds(d * QUARTER + h * HALF, HALF), :]
            ds_next(1, d, h, mine).start()
            ds_twin(0, d, h, mine).start()

    for d in BOTH:
        gy_b[pl.ds(d * QUARTER, QUARTER), :] = out_ds[pl.ds(d * QUARTER, QUARTER), :]

    def project(s):
        for d in BOTH:
            for h in BOTH:
                ds_from_twin(s, d, h).wait_recv()
            block_load(s, d, 1).start()
        for d in BOTH:
            block_load(s, d, 1).wait()
        for k in BOTH:
            for d in BOTH:
                c = core if k == 0 else 1 - core
                rows = pl.ds(row(s, d, c), QUARTER)
                at = pl.ds((2 * k + d) * QUARTER, QUARTER)
                z_b[pl.ds(0, QUARTER), at] = att_v[rows, :].T
        grad_o = dot_cols(gy_b[...], wo_v[...]).astype(BF16)
        for k in BOTH:
            for d in BOTH:
                c = core if k == 0 else 1 - core
                do_v[pl.ds(row(s, d, c), QUARTER), :] = grad_o[(2 * k + d) * QUARTER:(2 * k + d + 1) * QUARTER]
        for j in range(0, hidden, WIDE):
            acc_o[:, j:j + WIDE] += dot_plain(z_b[:QUARTER, :], gy_b[:, j:j + WIDE])

    def ds_relay(s, h):
        for d in BOTH:
            ds_here(s, d, h).wait_recv()

            @pl.when(s < LAST)
            def _():
                ds_next(s + 1, d, h).start()
            ds_twin(s, d, h).start()

    def ds_step(s, carry):
        ds_relay(s, 0)
        project(s - 1)

        @pl.when(s < LAST)
        def _():
            weight_step(s + 1)
        ds_relay(s, 1)
        for d in BOTH:
            block_load(s, d, 0).start()

        @pl.when(s < LAST)
        def _():
            weight_rest()
        for d in BOTH:
            block_load(s, d, 0).wait()
        return carry

    lax.fori_loop(1, CHIPS, ds_step, 0)
    project(LAST)

    def drain(s, carry):
        for d in BOTH:
            for h in BOTH:
                ds_twin(s, d, h).wait_send()

            @pl.when(s > 0)
            def _():
                for h in BOTH:
                    ds_here(s, d, h).wait_send()
        return carry
    lax.fori_loop(0, CHIPS, drain, 0)

    def drain_columns(col, carry):
        gys.drain(col)
        xs.drain(col)

        @pl.when(col > 0)
        def _():
            for r in BOTH:
                for h in range(PARTS):
                    send_sum(col, r, h).wait_send()
        return carry
    lax.fori_loop(0, 4, drain_columns, 0)
    for h in BOTH:
        give(h).wait_send()


def write_out(*refs):
    count = len(refs) // 2
    copies = [pltpu.make_async_copy(refs[i], refs[count + i], refs[-1].at[i]) for i in range(count)]
    for copy in copies:
        copy.start()
    for copy in copies:
        copy.wait()


def solution(mesh):
    token_spec = P(("dp", "tp"), None)
    split_cols = P("dp", "tp")
    weight_cols = P(None, "tp")
    weight_rows = P("tp", None)

    def local_backward(x_norm, grad_y, u_gate, u_up, w_gate, w_up, w_down, x_in, gamma, grad_res, attn_out, w_out):
        own, hidden = x_norm.shape
        tokens, ffn = u_gate.shape
        cols = attn_out.shape[1]
        anywhere = pl.BlockSpec(memory_space=pl.ANY)
        inside = pl.BlockSpec(memory_space=pltpu.VMEM)
        shape = jax.ShapeDtypeStruct
        dma = pltpu.SemaphoreType.DMA
        pair = (2,)
        stream_sems = [dma((2, 4, 2))] + [dma((4, 2))] * 3 + [dma((2, 4, 2))] * 2
        outs = pl.pallas_call(
            kernel,
            out_shape=[
                pltpu.VMEM((own, hidden), BF16), pltpu.VMEM((tokens, cols), BF16),
                pltpu.VMEM((ffn, hidden), F32), pltpu.VMEM((ffn, hidden), F32), pltpu.VMEM((ffn, hidden), F32),
                pltpu.VMEM((cols, hidden), F32),
                shape((tokens, hidden), BF16), shape((tokens, hidden), BF16), shape((tokens, hidden), BF16),
                shape((tokens, hidden), BF16),
                shape((CHIPS, ffn, ROWS), BF16), shape((CHIPS, ffn, ROWS), BF16), shape((CHIPS, ffn, ROWS), BF16),
            ],
            in_specs=[anywhere] * 8 + [inside] + [anywhere] * 3,
            out_specs=[inside] * 6 + [anywhere] * 7,
            scratch_shapes=[
                pltpu.VMEM((ffn, hidden), BF16), pltpu.VMEM((ffn, hidden), BF16), pltpu.VMEM((ffn, hidden), BF16),
                pltpu.VMEM((ROWS, hidden), BF16), pltpu.VMEM((ROWS, hidden), BF16),
                pltpu.VMEM((ffn, ROWS), BF16), pltpu.VMEM((ffn, ROWS), BF16),
                pltpu.VMEM((ffn, ROWS), BF16), pltpu.VMEM((ffn, ROWS), BF16), pltpu.VMEM((ffn, ROWS), BF16),
                pltpu.VMEM((ROWS, ffn), BF16), pltpu.VMEM((ROWS, ffn), BF16),
                pltpu.VMEM((own, hidden), F32), pltpu.VMEM((own, hidden), BF16), pltpu.VMEM((2, own, hidden), BF16),
                pltpu.VMEM((6, own, hidden), BF16), pltpu.VMEM((2, own, hidden), F32),
                pltpu.VMEM((2, PART, hidden), BF16), pltpu.VMEM((own, hidden), BF16),
                pltpu.VMEM((tokens, cols), BF16), pltpu.VMEM((cols, hidden), BF16),
                *stream_sems,
                *stream_sems, dma((2, 4)), *[dma((4,))] * 3,
                *[dma((CHIPS, 4))] * 4,
                dma, dma(pair), dma((3, 2, PARTS)), dma((2, 4, 2, PARTS)), dma(pair), dma(pair),
                dma((5,)), dma((4,)), dma(pair), dma((4,)), dma((3,)), dma(pair),
            ],
            compiler_params=pltpu.CompilerParams(
                collective_id=0, has_side_effects=True, vmem_limit_bytes=44 * 2 ** 20),
            name="mlp_backward",
        )(x_norm, grad_y, u_gate.T, u_up.T, w_gate.T, w_up.T, w_down, x_in, gamma, grad_res, attn_out, w_out)
        results = outs[:6]
        grad_sum, grad_attn, gw_gate, gw_up, gw_down, gw_out = pl.pallas_call(
            write_out,
            out_shape=[shape(a.shape, a.dtype) for a in results],
            in_specs=[inside] * len(results),
            out_specs=[anywhere] * len(results),
            scratch_shapes=[dma((len(results),))],
            compiler_params=pltpu.CompilerParams(vmem_limit_bytes=2 ** 20),
            name="write_out",
        )(*results)
        return grad_sum, grad_attn, gw_gate.T, gw_up.T, gw_down, gw_out

    return jax.shard_map(
        local_backward,
        mesh=mesh,
        in_specs=(token_spec, token_spec, split_cols, split_cols, weight_cols, weight_cols, weight_rows,
                  token_spec, P(None), token_spec, split_cols, weight_rows),
        out_specs=(token_spec, split_cols, split_cols, split_cols, token_spec, token_spec),
        check_vma=False,
    )
```

```python
import jax
import jax.numpy as jnp
from jax import lax
from jax.experimental import pallas as pl
from jax.experimental.pallas import tpu as pltpu
from jax.sharding import PartitionSpec as P

NORM_EPS = 1e-5
MESH = pl.DeviceIdType.MESH
BF16 = jnp.bfloat16
F32 = jnp.float32

CHIPS = 8
QUARTER = 128
HALF = 64
ROWS = 4 * QUARTER
LAST = CHIPS - 1
BOTH = (0, 1)
TILE = 32
WIDE = 512
PART = 64
PARTS = 2 * QUARTER // PART
SPARE = 64


def part_of(q):
    return 2 * (q % 2) + q // 2


def tile_at(i, size, base=0):
    return pl.ds(pl.multiple_of(base + i * size, size), size)


def dot_cols(a, b):
    return lax.dot_general(a, b, (((1,), (1,)), ((), ())), preferred_element_type=F32)


def dot_plain(a, b):
    return lax.dot_general(a, b, (((1,), (0,)), ((), ())), preferred_element_type=F32)


def kernel(x, gy, ug, uu, wg, wu, wd, xin, gamma, gres, att, wo,
           out_ds, do_v, acc_g, acc_u, acc_d, acc_o, gy_all, x_all, ds_all, rs_in, z_all, dg_all, du_all,
           wg_v, wu_v, wd_v,
           gy_b, x_b, ug_b, uu_b, z_b, dg_b, du_b, dgt_b, dut_b,
           p_own, p_send, p_recv, hold, own_sum, stage, y_in,
           att_v, wo_v,
           gy_zs, gy_zr, gy_ys, gy_yr, gy_ts, gy_tr, x_zs, x_zr, x_ys, x_yr, x_ts, x_tr, e_zs, e_zr, e_ts, e_tr,
           ds_ss, ds_rs, ds_ps, ds_pr, ps_sem, pr_sem, rss_sem, rsr_sem, yss_sem, ysr_sem,
           w_sem, gy_sem, x_sem, u_sem, keep_sem, stage_sem):
    hidden = gy.shape[1]
    own = gy.shape[0]
    t = lax.axis_index("tp")
    core = t % 2
    y = (t // 2) % 2
    z = t // 4
    edge = z % 3 == 0
    inner = z % 3 != 0
    pos = z + y * (7 - 2 * z)

    def device(chip, c):
        upper = chip // 4
        return 4 * (chip + upper * (7 - 2 * chip)) + 2 * upper + c

    onward = (device((pos + 1) % CHIPS, core), device((pos + LAST) % CHIPS, core))
    twin = t + 1 - 2 * core
    over = t + 2 - 4 * y
    beside = (t + 4 - 4 * (z // 3), t - 4 + 4 * ((3 - z) // 3))

    def signal(other):
        pl.semaphore_signal(barrier, inc=1, device_id={"tp": other}, device_id_type=MESH)

    barrier = pltpu.get_barrier_semaphore()
    signal(over)
    signal(twin)

    @pl.when(z < 3)
    def _():
        signal(beside[0])

    @pl.when(z > 0)
    def _():
        signal(beside[1])

    @pl.when(edge)
    def _():
        pl.semaphore_wait(barrier, 3)

    @pl.when(inner)
    def _():
        pl.semaphore_wait(barrier, 4)

    def remote(src, dst, send, recv, to):
        return pltpu.make_async_remote_copy(src_ref=src, dst_ref=dst, send_sem=send, recv_sem=recv,
                                            device_id={"tp": to}, device_id_type=MESH)

    def column(k):
        far = z // 2
        near = z + far * (3 - 2 * z)
        late = k // 2
        col = (1 - near) * k + near * ((1 - late) * (1 - k) + late * k)
        return col + far * (3 - 2 * col)

    def line(r):
        return y + r - 2 * y * r

    def first_row(col, r, c):
        return pl.multiple_of(((col * 2 + line(r)) * 2 + c) * own, own)

    def half(col, r, c, h):
        return pl.ds(pl.multiple_of(first_row(col, r, c) + h * QUARTER, QUARTER), QUARTER)

    class Stream:
        def __init__(self, own_ref, full, zs, zr, ys, yr, ts, tr, spare=None):
            self.own, self.full = own_ref, full
            self.spare = spare
            self.zs, self.zr, self.ys, self.yr, self.ts, self.tr = zs, zr, ys, yr, ts, tr

        def part(self, col, r, c, h, short=False):
            if short and self.spare is not None and h == 1:
                start = pl.multiple_of(first_row(col, r, c) + QUARTER, QUARTER)
                return self.full.at[pl.ds(start, QUARTER - SPARE), :]
            return self.full.at[half(col, r, c, h), :]

        def either(self, col, h, act):
            if self.spare is None or h == 0:
                act(False)
                return
            thin = (col % 3 != 0) & (col != z)
            pl.when(thin)(lambda: act(True))
            pl.when(jnp.logical_not(thin))(lambda: act(False))

        def spare_part(self, col, c):
            start = pl.multiple_of(first_row(col, 1, c) + 2 * QUARTER - SPARE, 16)
            return self.full.at[pl.ds(start, SPARE), :]

        def spare_along(self, col, side):
            dst = self.spare_part(col, core)
            return remote(dst, dst, self.spare[0].at[side, col], self.spare[1].at[col], beside[side])

        def spare_hand(self, col, c):
            dst = self.spare_part(col, c)
            return remote(dst, dst, self.spare[2].at[col], self.spare[3].at[col], twin)

        def spare_start(self):
            @pl.when(inner)
            def _():
                for side in BOTH:
                    self.spare_along(z, side).start()

        def spare_relay(self, dist):
            for side in BOTH:
                col = z - dist if side == 0 else z + dist

                @pl.when((col == 1) | (col == 2))
                def _():
                    self.spare_along(col, side).wait_recv()

                    @pl.when(z < 3 if side == 0 else z > 0)
                    def _():
                        self.spare_along(col, side).start()
                    self.spare_hand(col, core).start()

        def mine(self, h):
            return self.own.at[pl.ds(h * QUARTER, QUARTER), :]

        def along(self, col, h, side, src=None):
            dst = self.part(col, 0, core, h)
            return remote(dst if src is None else src, dst, self.zs.at[side, col, h], self.zr.at[col, h], beside[side])

        def across(self, col, h, src=None, short=False):
            dst = self.part(col, 0, core, h, short)
            return remote(dst if src is None else src, dst, self.ys.at[col, h], self.yr.at[col, h], over)

        def from_over(self, col, h, short):
            dst = self.part(col, 1, core, h, short)
            return remote(dst, dst, self.ys.at[col, h], self.yr.at[col, h], over)

        def hand(self, col, r, h, src=None, short=False):
            dst = self.part(col, r, core, h, short)
            return remote(dst if src is None else src, dst, self.ts.at[r, col, h], self.tr.at[r, col, h], twin)

        def from_twin(self, col, r, h, short=False):
            dst = self.part(col, r, 1 - core, h, short)
            return remote(dst, dst, self.ts.at[r, col, h], self.tr.at[r, col, h], twin)

        def relay(self, dist, h, side, held=False):
            col = z - dist if side == 0 else z + dist
            self.along(col, h, side).wait_recv()

            @pl.when(z < 3 if side == 0 else z > 0)
            def _():
                self.along(col, h, side).start()
            self.hand(col, 0, h).start()
            if not held:
                self.either(col, h, lambda short: self.across(col, h, short=short).start())
            else:
                second = inner & (dist == 1) & (z == 2 - side)

                @pl.when(jnp.logical_not(second))
                def _():
                    self.across(col, h).start()

        def relay_row(self, dist, h, held=False):
            @pl.when(z >= dist)
            def _():
                self.relay(dist, h, 0, held)

            @pl.when(z + dist < 4)
            def _():
                self.relay(dist, h, 1, held)

            if held and h == 1:
                @pl.when(inner & (dist == 1))
                def _():
                    for q in BOTH:
                        self.across(column(2), q).start()

        def relay_over(self, k, h):
            col = column(k)

            def act(short):
                self.from_over(col, h, short).wait_recv()
                self.hand(col, 1, h, short=short).start()
            self.either(col, h, act)

        def start_row(self):
            for h in BOTH:
                @pl.when(z < 3)
                def _():
                    self.along(z, h, 0, self.mine(h)).start()

                @pl.when(z > 0)
                def _():
                    self.along(z, h, 1, self.mine(h)).start()

        def start_rest(self):
            for h in BOTH:
                self.across(z, h, self.mine(h)).start()
                self.hand(z, 0, h, self.mine(h)).start()

        def load(self, n, buf, sem):
            k, r = n // 2, n % 2

            @pl.when(n == 0)
            def _():
                pltpu.make_async_copy(self.own, buf.at[pl.ds(0, own), :], sem.at[0]).start()

            @pl.when(n > 0)
            def _():
                self.block(n, core, buf, sem, 0).start()
            if self.spare is None:
                for h in BOTH:
                    self.from_twin(column(k), r, h).wait_recv()
            else:
                cut = (k > 0) & (r == 1) & (column(k) % 3 != 0)
                self.from_twin(column(k), r, 0).wait_recv()

                @pl.when(cut)
                def _():
                    self.from_twin(column(k), r, 1, True).wait_recv()
                    self.spare_hand(column(k), 1 - core).wait_recv()

                @pl.when(jnp.logical_not(cut))
                def _():
                    self.from_twin(column(k), r, 1).wait_recv()
            self.block(n, 1 - core, buf, sem, 1).start()

        def block(self, n, c, buf, sem, i):
            rows = pl.ds(first_row(column(n // 2), n % 2, c), own)
            return pltpu.make_async_copy(self.full.at[rows, :], buf.at[pl.ds(i * own, own), :], sem.at[i])

        def landed(self, n, buf, sem):
            for i in BOTH:
                self.block(n, core, buf, sem, i).wait()

        def drain(self, col):
            for h in BOTH:
                self.hand(col, 0, h).wait_send()

                def act(short):
                    self.across(col, h, short=short).wait_send()
                    self.hand(col, 1, h, short=short).wait_send()
                    if short:
                        self.spare_hand(col, core).wait_send()
                self.either(col, h, act)
            for side in BOTH:
                @pl.when((z < 3) & (col <= z) if side == 0 else (z > 0) & (col >= z))
                def _():
                    for h in BOTH:
                        self.along(col, h, side).wait_send()
                    if self.spare is not None:
                        @pl.when(col % 3 != 0)
                        def _():
                            self.spare_along(col, side).wait_send()

    gys = Stream(gy, gy_all, gy_zs, gy_zr, gy_ys, gy_yr, gy_ts, gy_tr)
    xs = Stream(x, x_all, x_zs, x_zr, x_ys, x_yr, x_ts, x_tr, (e_zs, e_zr, e_ts, e_tr))
    gys.start_row()
    gys.start_rest()

    @pl.when(edge)
    def _():
        xs.start_row()

    loads = [pltpu.make_async_copy(a, b, w_sem.at[i]) for i, (a, b) in enumerate(
        ((wd, wd_v), (wg, wg_v), (wu, wu_v), (att, att_v), (wo, wo_v)))]
    for copy in loads:
        copy.start()

    def load_u(n):
        copies = []
        for i in BOTH:
            c = core if i == 0 else 1 - core
            rows = pl.ds(first_row(column(n // 2), n % 2, c), own)
            at = pl.ds(i * own, own)
            copies.append(pltpu.make_async_copy(ug.at[:, rows], ug_b.at[:, at], u_sem.at[i]))
            copies.append(pltpu.make_async_copy(uu.at[:, rows], uu_b.at[:, at], u_sem.at[2 + i]))
        return copies

    for copy in load_u(0):
        copy.start()

    acc_g[...] = jnp.zeros_like(acc_g)
    acc_u[...] = jnp.zeros_like(acc_u)
    acc_d[...] = jnp.zeros_like(acc_d)
    acc_o[...] = jnp.zeros_like(acc_o)

    def keep(n):
        return [pltpu.make_async_copy(a, b.at[n], keep_sem.at[i])
                for i, (a, b) in enumerate(((z_b, z_all), (dg_b, dg_all), (du_b, du_all)))]

    def swap(n):
        return remote(p_send, p_recv.at[n % 2], ps_sem, pr_sem.at[n % 2], twin)

    def rs_slot(side, col, r, h):
        return (rs_in.at[tile_at(((side * 4 + col) * 2 + line(r)) * PARTS + h, PART), :],
                rsr_sem.at[side, col, line(r), h])

    def send_sum(k, r, h):
        col = column(k)
        up = (col - z + 3) // 4
        dst, sem = rs_slot(1 - up, col, r, h)
        return remote(hold.at[(k - 1) * 2 + r, tile_at(h, PART), :], dst,
                      rss_sem.at[k - 1, r, h], sem, t - 4 + 8 * up)

    def take_sum(side, col, r, h, slot):
        src, sem = rs_slot(side, col, r, h)
        remote(stage.at[slot], src, rss_sem.at[0, 0, 0], sem, twin).wait_recv()
        copy = pltpu.make_async_copy(src, stage.at[slot], stage_sem.at[slot])
        copy.start()
        return copy

    def finish(n):
        k, r = n // 2, n % 2
        swap(n).wait_recv()

        @pl.when(k == 0)
        def _():
            def tile(i, carry):
                at = tile_at(i, TILE)
                own_sum[r, at, :] = p_own[at, :] + p_recv[n % 2, at, :].astype(F32)
                return carry
            lax.fori_loop(0, own // TILE, tile, 0)

        @pl.when(k > 0)
        def _():
            def tile(i, carry):
                at = tile_at(i, TILE)
                hold[(k - 1) * 2 + r, at, :] = (p_own[at, :] + p_recv[n % 2, at, :].astype(F32)).astype(BF16)
                return carry
            lax.fori_loop(0, own // TILE, tile, 0)

            @pl.when(edge & (k == 1))
            def _():
                for q in range(PARTS):
                    send_sum(k, r, part_of(q)).start()

            @pl.when(edge & (k > 1) & (r == 1))
            def _():
                for q in range(PARTS):
                    send_sum(k, 1, part_of(q)).start()

            @pl.when(edge & (k == 3) & (r == 1))
            def _():
                for q in range(PARTS):
                    send_sum(3, 0, part_of(q)).start()

    def hidden_step(n, buf, sem):
        for copy in load_u(n):
            copy.wait()

        @pl.when(n > 0)
        def _():
            for copy in keep(n - 1):
                copy.wait()
        gys.landed(n, buf, sem)

        def hidden_tile(i, carry):
            at = pl.ds(pl.multiple_of(i * 256, 256), 256)
            grad_h = dot_cols(wd_v[...], buf[at, :])
            gate = ug_b[:, at].astype(F32)
            up = uu_b[:, at].astype(F32)
            sig = jax.nn.sigmoid(gate)
            act = gate * sig
            z_b[:, at] = (act * up).astype(BF16)
            grad_up = (grad_h * act).astype(BF16)
            grad_gate = (grad_h * up * (sig * (1.0 + gate * (1.0 - sig)))).astype(BF16)
            du_b[:, at] = grad_up
            dg_b[:, at] = grad_gate
            dut_b[at, :] = grad_up.T
            dgt_b[at, :] = grad_gate.T
            return carry
        lax.fori_loop(0, ROWS // 256, hidden_tile, 0)
        for copy in keep(n):
            copy.start()

        @pl.when(n < LAST)
        def _():
            for copy in load_u(n + 1):
                copy.start()

        @pl.when((n > 0) & (n % 2 == 0))
        def _():
            finish(n - 1)

        @pl.when(n > 0)
        def _():
            swap(n - 1).wait_send()

        def part_tile(j, carry):
            at = tile_at(j, WIDE)
            part = dot_plain(dgt_b[...], wg_v[:, at]) + dot_plain(dut_b[...], wu_v[:, at])
            p_own[:, at] = part[:own]
            p_send[:, at] = part[own:].astype(BF16)
            return carry
        lax.fori_loop(0, hidden // WIDE, part_tile, 0)
        swap(n).start()

    gys.load(0, gy_b, gy_sem)
    for copy in loads:
        copy.wait()
    hidden_step(0, gy_b, gy_sem)

    def hidden_pair(k, carry):
        finish(2 * k)
        for h in BOTH:
            gys.relay_row(k + 1, h, held=True)
            gys.relay_over(k, h)

            @pl.when(edge & (k == 3))
            def _():
                for side in BOTH:
                    @pl.when(z // 2 == 1 - side)
                    def _():
                        xs.relay(1, h, side)

        @pl.when(inner & (k == 1))
        def _():
            xs.start_row()
            xs.start_rest()
            for side in BOTH:
                @pl.when(z == 1 + side)
                def _():
                    for h in BOTH:
                        xs.relay(1, h, side)

        gys.load(2 * k + 1, x_b, x_sem)

        @pl.when(k < 3)
        def _():
            gys.load(2 * k + 2, gy_b, gy_sem)

        @pl.when(edge & (k == 2))
        def _():
            xs.start_rest()

        @pl.when(inner & (k == 3))
        def _():
            for side in BOTH:
                @pl.when(z == 2 - side)
                def _():
                    for h in BOTH:
                        xs.relay(1, h, side)
        hidden_step(2 * k + 1, x_b, x_sem)

        @pl.when(k < 3)
        def _():
            hidden_step(2 * k + 2, gy_b, gy_sem)
        return carry

    lax.fori_loop(0, 4, hidden_pair, 0)
    finish(LAST)
    for copy in keep(LAST):
        copy.wait()
    swap(LAST).wait_send()

    def carry_on(k, m):
        r, h = 1 - m // PARTS, part_of(m % PARTS)
        col = column(k)
        up = (col - z + 3) // 4
        slot = m % 2
        take_sum(1 - up, col, r, h, slot).wait()
        mine = hold.at[(k - 1) * 2 + r, tile_at(h, PART), :]
        mine[...] = (mine[...].astype(F32) + stage[slot].astype(F32)).astype(BF16)
        send_sum(k, r, h).start()

    def settle_part(side, r, h, slot):
        take_sum(side, z, r, h, slot).wait()
        at = tile_at(h, PART)
        own_sum[r, at, :] = own_sum[r, at, :] + stage[slot].astype(F32)

    def settle(side, r):
        def part(q, carry):
            settle_part(side, r, part_of(q), q % 2)
            return carry
        lax.fori_loop(0, PARTS, part, 0)

    def give(h):
        rows = pl.ds(h * PART, PART)
        return remote(p_send.at[rows, :], y_in.at[rows, :], yss_sem.at[h], ysr_sem.at[h], over)

    def give_over():
        for q in range(PARTS):
            rows = pl.ds(part_of(q) * PART, PART)
            p_send[rows, :] = own_sum[1, rows, :].astype(BF16)
            give(part_of(q)).start()

    def weight_step(n):
        xs.load(n, x_b, x_sem)
        for i, c in ((0, core), (1, 1 - core)):
            @pl.when((n > 0) | (i == 1))
            def _():
                gys.block(n, c, gy_b, gy_sem, i).start()

        @pl.when(n == 0)
        def _():
            pltpu.make_async_copy(gy, gy_b.at[pl.ds(0, own), :], gy_sem.at[0]).start()
        back = [pltpu.make_async_copy(b.at[n], a, keep_sem.at[i])
                for i, (a, b) in enumerate(((z_b, z_all), (dg_b, dg_all), (du_b, du_all)))]
        for copy in back:
            copy.start()
        for copy in back:
            copy.wait()
        gys.landed(n, gy_b, gy_sem)
        xs.landed(n, x_b, x_sem)

        def tile(j, carry):
            at = tile_at(j, WIDE)
            acc_d[:, at] += dot_plain(z_b[...], gy_b[:, at])
            return carry
        lax.fori_loop(0, hidden // WIDE, tile, 0)

    def weight_rest():
        def tile(j, carry):
            at = tile_at(j, WIDE)
            acc_g[:, at] += dot_plain(dg_b[...], x_b[:, at])
            acc_u[:, at] += dot_plain(du_b[...], x_b[:, at])
            return carry
        lax.fori_loop(0, hidden // WIDE, tile, 0)

    def late_step(i, carry):
        @pl.when(inner & (i < 2))
        def _():
            carry_on(2, 2 * i)
            carry_on(2, 2 * i + 1)

        @pl.when(inner & (i > 1))
        def _():
            carry_on(3, 2 * i - 4)
            carry_on(3, 2 * i - 3)

        @pl.when(i < 2)
        def _():
            for h in BOTH:
                xs.relay_row(i + 2, h)

        for h in BOTH:
            @pl.when(i == h)
            def _():
                xs.relay_over(0, h)
                if h == 1:
                    xs.spare_start()

                    @pl.when(edge)
                    def _():
                        for q in range(PARTS):
                            send_sum(2, 0, part_of(q)).start()

            @pl.when(i == 2 + h)
            def _():
                xs.relay_over(1, h)

        @pl.when(i < 2)
        def _():
            weight_step(i)
            weight_rest()

        @pl.when(inner & (i > 1))
        def _():
            settle(z - 1, i - 2)
        return carry

    lax.fori_loop(0, 4, late_step, 0)

    @pl.when(inner)
    def _():
        settle(2 - z, 1)
        give_over()

        def both_ways(m, carry):
            carry_on(1, m)
            carry_on(3, m + PARTS)
            return carry
        lax.fori_loop(0, PARTS, both_ways, 0)
    for h in BOTH:
        xs.relay_over(2, h)

    @pl.when(edge)
    def _():
        settle((3 - z) // 3, 1)
        give_over()
    xs.spare_relay(1)

    @pl.when(inner)
    def _():
        def both_ways(m, carry):
            carry_on(1, m)
            carry_on(2, m)
            return carry
        lax.fori_loop(PARTS, 2 * PARTS, both_ways, 0)
    xs.spare_relay(2)
    for h in BOTH:
        xs.relay_over(3, h)

    norm_loads = [pltpu.make_async_copy(src, x_b.at[pl.ds(k * own, own), :], x_sem.at[k])
                  for k, src in enumerate((xin, gres))]
    for copy in norm_loads:
        copy.start()

    for copy in norm_loads:
        copy.wait()

    def row(s, d, c):
        source = (pos + (CHIPS - s if d == 0 else s)) % CHIPS
        return pl.multiple_of(device(source, c) * 2 * QUARTER + d * QUARTER, QUARTER)

    def block_load(s, d, k):
        c = core if k == 0 else 1 - core
        at = pl.ds((2 * k + d) * QUARTER, QUARTER)
        return pltpu.make_async_copy(ds_all.at[pl.ds(row(s, d, c), QUARTER), :], gy_b.at[at, :], gy_sem.at[2 * k + d])

    def ds_next(s, d, h, src=None):
        rows = pl.ds(pl.multiple_of(row(s - 1, d, core) + h * HALF, HALF), HALF)
        return remote(ds_all.at[rows, :] if src is None else src, ds_all.at[rows, :],
                      ds_ss.at[s, 2 * d + h], ds_rs.at[s, 2 * d + h], onward[d])

    def ds_here(s, d, h):
        rows = pl.ds(pl.multiple_of(row(s, d, core) + h * HALF, HALF), HALF)
        return remote(ds_all.at[rows, :], ds_all.at[rows, :],
                      ds_ss.at[s, 2 * d + h], ds_rs.at[s, 2 * d + h], onward[d])

    def ds_twin(s, d, h, src=None):
        rows = pl.ds(pl.multiple_of(row(s, d, core) + h * HALF, HALF), HALF)
        return remote(ds_all.at[rows, :] if src is None else src, ds_all.at[rows, :],
                      ds_ps.at[s, 2 * d + h], ds_pr.at[s, 2 * d + h], twin)

    def ds_from_twin(s, d, h):
        rows = pl.ds(pl.multiple_of(row(s, d, 1 - core) + h * HALF, HALF), HALF)
        return remote(ds_all.at[rows, :], ds_all.at[rows, :],
                      ds_ps.at[s, 2 * d + h], ds_pr.at[s, 2 * d + h], twin)

    gain = gamma[...].astype(F32)[None, :]
    for h in BOTH:
        for d in BOTH:
            settle_part((3 - z) // 2, 0, 2 * d + h, d)
            give(2 * d + h).wait_recv()

            def norm_tile(i, carry):
                here = pl.ds(pl.multiple_of(d * QUARTER + h * HALF + i * 16, 16), 16)
                skip = pl.ds(pl.multiple_of(2 * QUARTER + d * QUARTER + h * HALF + i * 16, 16), 16)
                grad_x = (own_sum[0, here, :] + y_in[here, :].astype(F32)).astype(BF16).astype(F32)
                xin_f = x_b[here, :].astype(F32)
                inv_rms = lax.rsqrt(jnp.mean(xin_f * xin_f, axis=-1, keepdims=True) + NORM_EPS)
                scaled = grad_x * gain
                proj = jnp.mean(scaled * xin_f, axis=-1, keepdims=True)
                grad_s = (x_b[skip, :].astype(F32)
                          + inv_rms * (scaled - xin_f * (inv_rms * inv_rms) * proj)).astype(BF16)
                out_ds[here, :] = grad_s
                return carry
            lax.fori_loop(0, HALF // 16, norm_tile, 0)
            mine = out_ds.at[pl.ds(d * QUARTER + h * HALF, HALF), :]
            ds_next(1, d, h, mine).start()
            ds_twin(0, d, h, mine).start()

    for d in BOTH:
        gy_b[pl.ds(d * QUARTER, QUARTER), :] = out_ds[pl.ds(d * QUARTER, QUARTER), :]

    def project(s):
        for d in BOTH:
            for h in BOTH:
                ds_from_twin(s, d, h).wait_recv()
            block_load(s, d, 1).start()
        for d in BOTH:
            block_load(s, d, 1).wait()
        for k in BOTH:
            for d in BOTH:
                c = core if k == 0 else 1 - core
                rows = pl.ds(row(s, d, c), QUARTER)
                at = pl.ds((2 * k + d) * QUARTER, QUARTER)
                z_b[pl.ds(0, QUARTER), at] = att_v[rows, :].T
        grad_o = dot_cols(gy_b[...], wo_v[...]).astype(BF16)
        for k in BOTH:
            for d in BOTH:
                c = core if k == 0 else 1 - core
                do_v[pl.ds(row(s, d, c), QUARTER), :] = grad_o[(2 * k + d) * QUARTER:(2 * k + d + 1) * QUARTER]
        for j in range(0, hidden, WIDE):
            acc_o[:, j:j + WIDE] += dot_plain(z_b[:QUARTER, :], gy_b[:, j:j + WIDE])

    def ds_relay(s, h):
        for d in BOTH:
            ds_here(s, d, h).wait_recv()

            @pl.when(s < LAST)
            def _():
                ds_next(s + 1, d, h).start()
            ds_twin(s, d, h).start()

    def drain_columns(col, carry):
        gys.drain(col)
        xs.drain(col)

        @pl.when(col > 0)
        def _():
            for r in BOTH:
                for h in range(PARTS):
                    send_sum(col, r, h).wait_send()
        return carry

    def ds_step(s, carry):
        ds_relay(s, 0)
        project(s - 1)

        @pl.when(s < LAST)
        def _():
            weight_step(s + 1)

        @pl.when(s == LAST)
        def _():
            lax.fori_loop(0, 4, drain_columns, 0)
            for q in range(PARTS):
                give(q).wait_send()
        ds_relay(s, 1)
        for d in BOTH:
            block_load(s, d, 0).start()

        @pl.when(s < LAST)
        def _():
            weight_rest()
        for d in BOTH:
            block_load(s, d, 0).wait()
        return carry

    lax.fori_loop(1, CHIPS, ds_step, 0)
    project(LAST)

    def drain(s, carry):
        for d in BOTH:
            for h in BOTH:
                ds_twin(s, d, h).wait_send()

            @pl.when(s > 0)
            def _():
                for h in BOTH:
                    ds_here(s, d, h).wait_send()
        return carry
    lax.fori_loop(0, CHIPS, drain, 0)


def write_out(*refs):
    count = len(refs) // 2
    copies = [pltpu.make_async_copy(refs[i], refs[count + i], refs[-1].at[i]) for i in range(count)]
    for copy in copies:
        copy.start()
    for copy in copies:
        copy.wait()


def solution(mesh):
    token_spec = P(("dp", "tp"), None)
    split_cols = P("dp", "tp")
    weight_cols = P(None, "tp")
    weight_rows = P("tp", None)

    def local_backward(x_norm, grad_y, u_gate, u_up, w_gate, w_up, w_down, x_in, gamma, grad_res, attn_out, w_out):
        own, hidden = x_norm.shape
        tokens, ffn = u_gate.shape
        cols = attn_out.shape[1]
        anywhere = pl.BlockSpec(memory_space=pl.ANY)
        inside = pl.BlockSpec(memory_space=pltpu.VMEM)
        shape = jax.ShapeDtypeStruct
        dma = pltpu.SemaphoreType.DMA
        pair = (2,)
        stream_sems = [dma((2, 4, 2))] + [dma((4, 2))] * 3 + [dma((2, 4, 2))] * 2
        outs = pl.pallas_call(
            kernel,
            out_shape=[
                pltpu.VMEM((own, hidden), BF16), pltpu.VMEM((tokens, cols), BF16),
                pltpu.VMEM((ffn, hidden), F32), pltpu.VMEM((ffn, hidden), F32), pltpu.VMEM((ffn, hidden), F32),
                pltpu.VMEM((cols, hidden), F32),
                shape((tokens, hidden), BF16), shape((tokens, hidden), BF16), shape((tokens, hidden), BF16),
                shape((tokens, hidden), BF16),
                shape((CHIPS, ffn, ROWS), BF16), shape((CHIPS, ffn, ROWS), BF16), shape((CHIPS, ffn, ROWS), BF16),
            ],
            in_specs=[anywhere] * 8 + [inside] + [anywhere] * 3,
            out_specs=[inside] * 6 + [anywhere] * 7,
            scratch_shapes=[
                pltpu.VMEM((ffn, hidden), BF16), pltpu.VMEM((ffn, hidden), BF16), pltpu.VMEM((ffn, hidden), BF16),
                pltpu.VMEM((ROWS, hidden), BF16), pltpu.VMEM((ROWS, hidden), BF16),
                pltpu.VMEM((ffn, ROWS), BF16), pltpu.VMEM((ffn, ROWS), BF16),
                pltpu.VMEM((ffn, ROWS), BF16), pltpu.VMEM((ffn, ROWS), BF16), pltpu.VMEM((ffn, ROWS), BF16),
                pltpu.VMEM((ROWS, ffn), BF16), pltpu.VMEM((ROWS, ffn), BF16),
                pltpu.VMEM((own, hidden), F32), pltpu.VMEM((own, hidden), BF16), pltpu.VMEM((2, own, hidden), BF16),
                pltpu.VMEM((6, own, hidden), BF16), pltpu.VMEM((2, own, hidden), F32),
                pltpu.VMEM((2, PART, hidden), BF16), pltpu.VMEM((own, hidden), BF16),
                pltpu.VMEM((tokens, cols), BF16), pltpu.VMEM((cols, hidden), BF16),
                *stream_sems,
                *stream_sems, dma((2, 4)), *[dma((4,))] * 3,
                *[dma((CHIPS, 4))] * 4,
                dma, dma(pair), dma((3, 2, PARTS)), dma((2, 4, 2, PARTS)), dma((PARTS,)), dma((PARTS,)),
                dma((5,)), dma((4,)), dma(pair), dma((4,)), dma((3,)), dma(pair),
            ],
            compiler_params=pltpu.CompilerParams(
                collective_id=0, has_side_effects=True, vmem_limit_bytes=44 * 2 ** 20),
            name="mlp_backward",
        )(x_norm, grad_y, u_gate.T, u_up.T, w_gate.T, w_up.T, w_down, x_in, gamma, grad_res, attn_out, w_out)
        results = outs[:6]
        grad_sum, grad_attn, gw_gate, gw_up, gw_down, gw_out = pl.pallas_call(
            write_out,
            out_shape=[shape(a.shape, a.dtype) for a in results],
            in_specs=[inside] * len(results),
            out_specs=[anywhere] * len(results),
            scratch_shapes=[dma((len(results),))],
            compiler_params=pltpu.CompilerParams(vmem_limit_bytes=2 ** 20),
            name="write_out",
        )(*results)
        return grad_sum, grad_attn, gw_gate.T, gw_up.T, gw_down, gw_out

    return jax.shard_map(
        local_backward,
        mesh=mesh,
        in_specs=(token_spec, token_spec, split_cols, split_cols, weight_cols, weight_cols, weight_rows,
                  token_spec, P(None), token_spec, split_cols, weight_rows),
        out_specs=(token_spec, split_cols, split_cols, split_cols, token_spec, token_spec),
        check_vma=False,
    )
```

```python
import jax
import jax.numpy as jnp
from jax import lax
from jax.experimental import pallas as pl
from jax.experimental.pallas import tpu as pltpu
from jax.sharding import PartitionSpec as P

NORM_EPS = 1e-5
MESH = pl.DeviceIdType.MESH
BF16 = jnp.bfloat16
F32 = jnp.float32

CHIPS = 8
QUARTER = 128
HALF = 64
ROWS = 4 * QUARTER
LAST = CHIPS - 1
BOTH = (0, 1)
TILE = 32
WIDE = 512
PART = 64
PARTS = 2 * QUARTER // PART
SPARE = 64


def part_of(q):
    return 2 * (q % 2) + q // 2


def tile_at(i, size, base=0):
    return pl.ds(pl.multiple_of(base + i * size, size), size)


def dot_cols(a, b):
    return lax.dot_general(a, b, (((1,), (1,)), ((), ())), preferred_element_type=F32)


def dot_plain(a, b):
    return lax.dot_general(a, b, (((1,), (0,)), ((), ())), preferred_element_type=F32)


def kernel(x, gy, ug, uu, wg, wu, wd, xin, gamma, gres, att, wo,
           out_ds, do_v, acc_g, acc_u, acc_d, acc_o, gy_all, x_all, ds_all, rs_in, z_all, dg_all, du_all,
           wg_v, wu_v, wd_v,
           gy_b, x_b, ug_b, uu_b, z_b, dg_b, du_b, dgt_b, dut_b,
           p_own, p_send, p_recv, hold, own_sum, stage, y_in,
           att_v, wo_v,
           gy_zs, gy_zr, gy_ys, gy_yr, gy_ts, gy_tr, x_zs, x_zr, x_ys, x_yr, x_ts, x_tr, e_zs, e_zr, e_ts, e_tr,
           ds_ss, ds_rs, ds_ps, ds_pr, ps_sem, pr_sem, rss_sem, rsr_sem, yss_sem, ysr_sem,
           w_sem, gy_sem, x_sem, u_sem, keep_sem, stage_sem):
    hidden = gy.shape[1]
    own = gy.shape[0]
    t = lax.axis_index("tp")
    core = t % 2
    y = (t // 2) % 2
    z = t // 4
    edge = z % 3 == 0
    inner = z % 3 != 0
    pos = z + y * (7 - 2 * z)

    def device(chip, c):
        upper = chip // 4
        return 4 * (chip + upper * (7 - 2 * chip)) + 2 * upper + c

    onward = (device((pos + 1) % CHIPS, core), device((pos + LAST) % CHIPS, core))
    twin = t + 1 - 2 * core
    over = t + 2 - 4 * y
    beside = (t + 4 - 4 * (z // 3), t - 4 + 4 * ((3 - z) // 3))

    def signal(other):
        pl.semaphore_signal(barrier, inc=1, device_id={"tp": other}, device_id_type=MESH)

    barrier = pltpu.get_barrier_semaphore()
    signal(over)
    signal(twin)

    @pl.when(z < 3)
    def _():
        signal(beside[0])

    @pl.when(z > 0)
    def _():
        signal(beside[1])

    @pl.when(edge)
    def _():
        pl.semaphore_wait(barrier, 3)

    @pl.when(inner)
    def _():
        pl.semaphore_wait(barrier, 4)

    def remote(src, dst, send, recv, to):
        return pltpu.make_async_remote_copy(src_ref=src, dst_ref=dst, send_sem=send, recv_sem=recv,
                                            device_id={"tp": to}, device_id_type=MESH)

    def column(k):
        far = z // 2
        near = z + far * (3 - 2 * z)
        late = k // 2
        col = (1 - near) * k + near * ((1 - late) * (1 - k) + late * k)
        return col + far * (3 - 2 * col)

    def line(r):
        return y + r - 2 * y * r

    def first_row(col, r, c):
        return pl.multiple_of(((col * 2 + line(r)) * 2 + c) * own, own)

    def half(col, r, c, h):
        return pl.ds(pl.multiple_of(first_row(col, r, c) + h * QUARTER, QUARTER), QUARTER)

    class Stream:
        def __init__(self, own_ref, full, zs, zr, ys, yr, ts, tr, spare=None):
            self.own, self.full = own_ref, full
            self.spare = spare
            self.zs, self.zr, self.ys, self.yr, self.ts, self.tr = zs, zr, ys, yr, ts, tr

        def part(self, col, r, c, h, short=False):
            if short and self.spare is not None and h == 1:
                start = pl.multiple_of(first_row(col, r, c) + QUARTER, QUARTER)
                return self.full.at[pl.ds(start, QUARTER - SPARE), :]
            return self.full.at[half(col, r, c, h), :]

        def either(self, col, h, act):
            if self.spare is None or h == 0:
                act(False)
                return
            thin = (col % 3 != 0) & (col != z)
            pl.when(thin)(lambda: act(True))
            pl.when(jnp.logical_not(thin))(lambda: act(False))

        def spare_part(self, col, c):
            start = pl.multiple_of(first_row(col, 1, c) + 2 * QUARTER - SPARE, 16)
            return self.full.at[pl.ds(start, SPARE), :]

        def spare_along(self, col, side):
            dst = self.spare_part(col, core)
            return remote(dst, dst, self.spare[0].at[side, col], self.spare[1].at[col], beside[side])

        def spare_hand(self, col, c):
            dst = self.spare_part(col, c)
            return remote(dst, dst, self.spare[2].at[col], self.spare[3].at[col], twin)

        def spare_start(self):
            @pl.when(inner)
            def _():
                for side in BOTH:
                    self.spare_along(z, side).start()

        def spare_relay(self, dist):
            for side in BOTH:
                col = z - dist if side == 0 else z + dist

                @pl.when((col == 1) | (col == 2))
                def _():
                    self.spare_along(col, side).wait_recv()

                    @pl.when(z < 3 if side == 0 else z > 0)
                    def _():
                        self.spare_along(col, side).start()
                    self.spare_hand(col, core).start()

        def mine(self, h):
            return self.own.at[pl.ds(h * QUARTER, QUARTER), :]

        def along(self, col, h, side, src=None):
            dst = self.part(col, 0, core, h)
            return remote(dst if src is None else src, dst, self.zs.at[side, col, h], self.zr.at[col, h], beside[side])

        def across(self, col, h, src=None, short=False):
            dst = self.part(col, 0, core, h, short)
            return remote(dst if src is None else src, dst, self.ys.at[col, h], self.yr.at[col, h], over)

        def from_over(self, col, h, short):
            dst = self.part(col, 1, core, h, short)
            return remote(dst, dst, self.ys.at[col, h], self.yr.at[col, h], over)

        def hand(self, col, r, h, src=None, short=False):
            dst = self.part(col, r, core, h, short)
            return remote(dst if src is None else src, dst, self.ts.at[r, col, h], self.tr.at[r, col, h], twin)

        def from_twin(self, col, r, h, short=False):
            dst = self.part(col, r, 1 - core, h, short)
            return remote(dst, dst, self.ts.at[r, col, h], self.tr.at[r, col, h], twin)

        def relay(self, dist, h, side, held=False):
            col = z - dist if side == 0 else z + dist
            self.along(col, h, side).wait_recv()

            @pl.when(z < 3 if side == 0 else z > 0)
            def _():
                self.along(col, h, side).start()
            self.hand(col, 0, h).start()
            if not held:
                self.either(col, h, lambda short: self.across(col, h, short=short).start())
            else:
                second = inner & (dist == 1) & (z == 2 - side)

                @pl.when(jnp.logical_not(second))
                def _():
                    self.across(col, h).start()

        def relay_row(self, dist, h, held=False):
            @pl.when(z >= dist)
            def _():
                self.relay(dist, h, 0, held)

            @pl.when(z + dist < 4)
            def _():
                self.relay(dist, h, 1, held)

            if held and h == 1:
                @pl.when(inner & (dist == 1))
                def _():
                    for q in BOTH:
                        self.across(column(2), q).start()

        def relay_over(self, k, h):
            col = column(k)

            def act(short):
                self.from_over(col, h, short).wait_recv()
                self.hand(col, 1, h, short=short).start()
            self.either(col, h, act)

        def start_row(self):
            for h in BOTH:
                @pl.when(z < 3)
                def _():
                    self.along(z, h, 0, self.mine(h)).start()

                @pl.when(z > 0)
                def _():
                    self.along(z, h, 1, self.mine(h)).start()

        def start_rest(self):
            for h in BOTH:
                self.across(z, h, self.mine(h)).start()
                self.hand(z, 0, h, self.mine(h)).start()

        def load(self, n, buf, sem):
            k, r = n // 2, n % 2

            @pl.when(n == 0)
            def _():
                pltpu.make_async_copy(self.own, buf.at[pl.ds(0, own), :], sem.at[0]).start()

            @pl.when(n > 0)
            def _():
                self.block(n, core, buf, sem, 0).start()
            if self.spare is None:
                for h in BOTH:
                    self.from_twin(column(k), r, h).wait_recv()
            else:
                cut = (k > 0) & (r == 1) & (column(k) % 3 != 0)
                self.from_twin(column(k), r, 0).wait_recv()

                @pl.when(cut)
                def _():
                    self.from_twin(column(k), r, 1, True).wait_recv()
                    self.spare_hand(column(k), 1 - core).wait_recv()

                @pl.when(jnp.logical_not(cut))
                def _():
                    self.from_twin(column(k), r, 1).wait_recv()
            self.block(n, 1 - core, buf, sem, 1).start()

        def block(self, n, c, buf, sem, i):
            rows = pl.ds(first_row(column(n // 2), n % 2, c), own)
            return pltpu.make_async_copy(self.full.at[rows, :], buf.at[pl.ds(i * own, own), :], sem.at[i])

        def landed(self, n, buf, sem):
            for i in BOTH:
                self.block(n, core, buf, sem, i).wait()

        def drain(self, col):
            for h in BOTH:
                self.hand(col, 0, h).wait_send()

                def act(short):
                    self.across(col, h, short=short).wait_send()
                    self.hand(col, 1, h, short=short).wait_send()
                    if short:
                        self.spare_hand(col, core).wait_send()
                self.either(col, h, act)
            for side in BOTH:
                @pl.when((z < 3) & (col <= z) if side == 0 else (z > 0) & (col >= z))
                def _():
                    for h in BOTH:
                        self.along(col, h, side).wait_send()
                    if self.spare is not None:
                        @pl.when(col % 3 != 0)
                        def _():
                            self.spare_along(col, side).wait_send()

    gys = Stream(gy, gy_all, gy_zs, gy_zr, gy_ys, gy_yr, gy_ts, gy_tr)
    xs = Stream(x, x_all, x_zs, x_zr, x_ys, x_yr, x_ts, x_tr, (e_zs, e_zr, e_ts, e_tr))
    gys.start_row()
    gys.start_rest()

    @pl.when(edge)
    def _():
        xs.start_row()

    loads = [pltpu.make_async_copy(a, b, w_sem.at[i]) for i, (a, b) in enumerate(
        ((wd, wd_v), (wg, wg_v), (wu, wu_v), (att, att_v), (wo, wo_v)))]
    for copy in loads:
        copy.start()

    def load_u(n):
        copies = []
        for i in BOTH:
            c = core if i == 0 else 1 - core
            rows = pl.ds(first_row(column(n // 2), n % 2, c), own)
            at = pl.ds(i * own, own)
            copies.append(pltpu.make_async_copy(ug.at[:, rows], ug_b.at[:, at], u_sem.at[i]))
            copies.append(pltpu.make_async_copy(uu.at[:, rows], uu_b.at[:, at], u_sem.at[2 + i]))
        return copies

    for copy in load_u(0):
        copy.start()

    acc_g[...] = jnp.zeros_like(acc_g)
    acc_u[...] = jnp.zeros_like(acc_u)
    acc_d[...] = jnp.zeros_like(acc_d)
    acc_o[...] = jnp.zeros_like(acc_o)

    def keep(n):
        return [pltpu.make_async_copy(a, b.at[n], keep_sem.at[i])
                for i, (a, b) in enumerate(((z_b, z_all), (dg_b, dg_all), (du_b, du_all)))]

    def swap(n):
        return remote(p_send, p_recv.at[n % 2], ps_sem, pr_sem.at[n % 2], twin)

    def rs_slot(side, col, r, h):
        return (rs_in.at[tile_at(((side * 4 + col) * 2 + line(r)) * PARTS + h, PART), :],
                rsr_sem.at[side, col, line(r), h])

    def send_sum(k, r, h):
        col = column(k)
        up = (col - z + 3) // 4
        dst, sem = rs_slot(1 - up, col, r, h)
        return remote(hold.at[(k - 1) * 2 + r, tile_at(h, PART), :], dst,
                      rss_sem.at[k - 1, r, h], sem, t - 4 + 8 * up)

    def take_sum(side, col, r, h, slot):
        src, sem = rs_slot(side, col, r, h)
        remote(stage.at[slot], src, rss_sem.at[0, 0, 0], sem, twin).wait_recv()
        copy = pltpu.make_async_copy(src, stage.at[slot], stage_sem.at[slot])
        copy.start()
        return copy

    def finish(n):
        k, r = n // 2, n % 2
        swap(n).wait_recv()

        @pl.when(k == 0)
        def _():
            def tile(i, carry):
                at = tile_at(i, TILE)
                own_sum[r, at, :] = p_own[at, :] + p_recv[n % 2, at, :].astype(F32)
                return carry
            lax.fori_loop(0, own // TILE, tile, 0)

        @pl.when(k > 0)
        def _():
            def tile(i, carry):
                at = tile_at(i, TILE)
                hold[(k - 1) * 2 + r, at, :] = (p_own[at, :] + p_recv[n % 2, at, :].astype(F32)).astype(BF16)
                return carry
            lax.fori_loop(0, own // TILE, tile, 0)

            @pl.when(edge & (k == 1))
            def _():
                for q in range(PARTS):
                    send_sum(k, r, part_of(q)).start()

            @pl.when(edge & (k > 1) & (r == 1))
            def _():
                for q in range(PARTS):
                    send_sum(k, 1, part_of(q)).start()

            @pl.when(edge & (k == 3) & (r == 1))
            def _():
                for q in range(PARTS):
                    send_sum(3, 0, part_of(q)).start()

    def hidden_step(n, buf, sem):
        for copy in load_u(n):
            copy.wait()

        @pl.when(n > 0)
        def _():
            for copy in keep(n - 1):
                copy.wait()
        gys.landed(n, buf, sem)

        def hidden_tile(i, carry):
            at = pl.ds(pl.multiple_of(i * 256, 256), 256)
            grad_h = dot_cols(wd_v[...], buf[at, :])
            gate = ug_b[:, at].astype(F32)
            up = uu_b[:, at].astype(F32)
            sig = jax.nn.sigmoid(gate)
            act = gate * sig
            z_b[:, at] = (act * up).astype(BF16)
            grad_up = (grad_h * act).astype(BF16)
            grad_gate = (grad_h * up * (sig * (1.0 + gate * (1.0 - sig)))).astype(BF16)
            du_b[:, at] = grad_up
            dg_b[:, at] = grad_gate
            dut_b[at, :] = grad_up.T
            dgt_b[at, :] = grad_gate.T
            return carry
        lax.fori_loop(0, ROWS // 256, hidden_tile, 0)
        for copy in keep(n):
            copy.start()

        @pl.when(n < LAST)
        def _():
            for copy in load_u(n + 1):
                copy.start()

        @pl.when((n > 0) & (n % 2 == 0))
        def _():
            finish(n - 1)

        @pl.when(n > 0)
        def _():
            swap(n - 1).wait_send()

        def part_tile(j, carry):
            at = tile_at(j, WIDE)
            part = dot_plain(dgt_b[...], wg_v[:, at]) + dot_plain(dut_b[...], wu_v[:, at])
            p_own[:, at] = part[:own]
            p_send[:, at] = part[own:].astype(BF16)
            return carry
        lax.fori_loop(0, hidden // WIDE, part_tile, 0)
        swap(n).start()

    gys.load(0, gy_b, gy_sem)
    for copy in loads:
        copy.wait()
    hidden_step(0, gy_b, gy_sem)

    def hidden_pair(k, carry):
        finish(2 * k)
        for h in BOTH:
            gys.relay_row(k + 1, h, held=True)
            gys.relay_over(k, h)

            @pl.when(edge & (k == 3))
            def _():
                for side in BOTH:
                    @pl.when(z // 2 == 1 - side)
                    def _():
                        xs.relay(1, h, side)

        @pl.when(inner & (k == 1))
        def _():
            xs.start_row()
            xs.start_rest()
            for side in BOTH:
                @pl.when(z == 1 + side)
                def _():
                    for h in BOTH:
                        xs.relay(1, h, side)

        gys.load(2 * k + 1, x_b, x_sem)

        @pl.when(k < 3)
        def _():
            gys.load(2 * k + 2, gy_b, gy_sem)

        @pl.when(edge & (k == 2))
        def _():
            xs.start_rest()

        @pl.when(inner & (k == 3))
        def _():
            for side in BOTH:
                @pl.when(z == 2 - side)
                def _():
                    for h in BOTH:
                        xs.relay(1, h, side)
        hidden_step(2 * k + 1, x_b, x_sem)

        @pl.when(k < 3)
        def _():
            hidden_step(2 * k + 2, gy_b, gy_sem)
        return carry

    lax.fori_loop(0, 4, hidden_pair, 0)
    def carry_on(k, m):
        r, h = 1 - m // PARTS, part_of(m % PARTS)
        col = column(k)
        up = (col - z + 3) // 4
        slot = m % 2
        take_sum(1 - up, col, r, h, slot).wait()
        mine = hold.at[(k - 1) * 2 + r, tile_at(h, PART), :]
        mine[...] = (mine[...].astype(F32) + stage[slot].astype(F32)).astype(BF16)
        send_sum(k, r, h).start()

    @pl.when(inner)
    def _():
        carry_on(2, 0)
        carry_on(2, 1)
    finish(LAST)
    for copy in keep(LAST):
        copy.wait()
    swap(LAST).wait_send()

    def settle_part(side, r, h, slot):
        take_sum(side, z, r, h, slot).wait()
        at = tile_at(h, PART)
        own_sum[r, at, :] = own_sum[r, at, :] + stage[slot].astype(F32)

    def settle(side, r):
        def part(q, carry):
            settle_part(side, r, part_of(q), q % 2)
            return carry
        lax.fori_loop(0, PARTS, part, 0)

    def give(h):
        rows = pl.ds(h * PART, PART)
        return remote(p_send.at[rows, :], y_in.at[rows, :], yss_sem.at[h], ysr_sem.at[h], over)

    def give_over():
        for q in range(PARTS):
            rows = pl.ds(part_of(q) * PART, PART)
            p_send[rows, :] = own_sum[1, rows, :].astype(BF16)
            give(part_of(q)).start()

    def weight_step(n):
        xs.load(n, x_b, x_sem)
        for i, c in ((0, core), (1, 1 - core)):
            @pl.when((n > 0) | (i == 1))
            def _():
                gys.block(n, c, gy_b, gy_sem, i).start()

        @pl.when(n == 0)
        def _():
            pltpu.make_async_copy(gy, gy_b.at[pl.ds(0, own), :], gy_sem.at[0]).start()
        back = [pltpu.make_async_copy(b.at[n], a, keep_sem.at[i])
                for i, (a, b) in enumerate(((z_b, z_all), (dg_b, dg_all), (du_b, du_all)))]
        for copy in back:
            copy.start()
        for copy in back:
            copy.wait()
        gys.landed(n, gy_b, gy_sem)
        xs.landed(n, x_b, x_sem)

        def tile(j, carry):
            at = tile_at(j, WIDE)
            acc_d[:, at] += dot_plain(z_b[...], gy_b[:, at])
            return carry
        lax.fori_loop(0, hidden // WIDE, tile, 0)

    def weight_rest():
        def tile(j, carry):
            at = tile_at(j, WIDE)
            acc_g[:, at] += dot_plain(dg_b[...], x_b[:, at])
            acc_u[:, at] += dot_plain(du_b[...], x_b[:, at])
            return carry
        lax.fori_loop(0, hidden // WIDE, tile, 0)

    def late_step(i, carry):
        @pl.when(inner & (i == 1))
        def _():
            carry_on(2, 2)
            carry_on(2, 3)

        @pl.when(inner & (i > 1))
        def _():
            carry_on(3, 2 * i - 4)
            carry_on(3, 2 * i - 3)

        @pl.when(i < 2)
        def _():
            for h in BOTH:
                xs.relay_row(i + 2, h)

        for h in BOTH:
            @pl.when(i == h)
            def _():
                xs.relay_over(0, h)
                if h == 1:
                    xs.spare_start()

                    @pl.when(edge)
                    def _():
                        for q in range(PARTS):
                            send_sum(2, 0, part_of(q)).start()

            @pl.when(i == 2 + h)
            def _():
                xs.relay_over(1, h)

        @pl.when(i < 2)
        def _():
            weight_step(i)
            weight_rest()

        @pl.when(inner & (i > 1))
        def _():
            settle(z - 1, i - 2)
        return carry

    lax.fori_loop(0, 4, late_step, 0)

    @pl.when(inner)
    def _():
        settle(2 - z, 1)
        give_over()

        def both_ways(m, carry):
            carry_on(1, m)
            carry_on(3, m + PARTS)
            return carry
        lax.fori_loop(0, PARTS, both_ways, 0)
    for h in BOTH:
        xs.relay_over(2, h)

    @pl.when(edge)
    def _():
        settle((3 - z) // 3, 1)
        give_over()
    xs.spare_relay(1)

    @pl.when(inner)
    def _():
        def both_ways(m, carry):
            carry_on(1, m)
            carry_on(2, m)
            return carry
        lax.fori_loop(PARTS, 2 * PARTS, both_ways, 0)
    xs.spare_relay(2)
    for h in BOTH:
        xs.relay_over(3, h)

    norm_loads = [pltpu.make_async_copy(src, x_b.at[pl.ds(k * own, own), :], x_sem.at[k])
                  for k, src in enumerate((xin, gres))]
    for copy in norm_loads:
        copy.start()

    for copy in norm_loads:
        copy.wait()

    def row(s, d, c):
        source = (pos + (CHIPS - s if d == 0 else s)) % CHIPS
        return pl.multiple_of(device(source, c) * 2 * QUARTER + d * QUARTER, QUARTER)

    def block_load(s, d, k):
        c = core if k == 0 else 1 - core
        at = pl.ds((2 * k + d) * QUARTER, QUARTER)
        return pltpu.make_async_copy(ds_all.at[pl.ds(row(s, d, c), QUARTER), :], gy_b.at[at, :], gy_sem.at[2 * k + d])

    def ds_next(s, d, h, src=None):
        rows = pl.ds(pl.multiple_of(row(s - 1, d, core) + h * HALF, HALF), HALF)
        return remote(ds_all.at[rows, :] if src is None else src, ds_all.at[rows, :],
                      ds_ss.at[s, 2 * d + h], ds_rs.at[s, 2 * d + h], onward[d])

    def ds_here(s, d, h):
        rows = pl.ds(pl.multiple_of(row(s, d, core) + h * HALF, HALF), HALF)
        return remote(ds_all.at[rows, :], ds_all.at[rows, :],
                      ds_ss.at[s, 2 * d + h], ds_rs.at[s, 2 * d + h], onward[d])

    def ds_twin(s, d, h, src=None):
        rows = pl.ds(pl.multiple_of(row(s, d, core) + h * HALF, HALF), HALF)
        return remote(ds_all.at[rows, :] if src is None else src, ds_all.at[rows, :],
                      ds_ps.at[s, 2 * d + h], ds_pr.at[s, 2 * d + h], twin)

    def ds_from_twin(s, d, h):
        rows = pl.ds(pl.multiple_of(row(s, d, 1 - core) + h * HALF, HALF), HALF)
        return remote(ds_all.at[rows, :], ds_all.at[rows, :],
                      ds_ps.at[s, 2 * d + h], ds_pr.at[s, 2 * d + h], twin)

    gain = gamma[...].astype(F32)[None, :]
    for h in BOTH:
        for d in BOTH:
            settle_part((3 - z) // 2, 0, 2 * d + h, d)
            give(2 * d + h).wait_recv()

            def norm_tile(i, carry):
                here = pl.ds(pl.multiple_of(d * QUARTER + h * HALF + i * 16, 16), 16)
                skip = pl.ds(pl.multiple_of(2 * QUARTER + d * QUARTER + h * HALF + i * 16, 16), 16)
                grad_x = (own_sum[0, here, :] + y_in[here, :].astype(F32)).astype(BF16).astype(F32)
                xin_f = x_b[here, :].astype(F32)
                inv_rms = lax.rsqrt(jnp.mean(xin_f * xin_f, axis=-1, keepdims=True) + NORM_EPS)
                scaled = grad_x * gain
                proj = jnp.mean(scaled * xin_f, axis=-1, keepdims=True)
                grad_s = (x_b[skip, :].astype(F32)
                          + inv_rms * (scaled - xin_f * (inv_rms * inv_rms) * proj)).astype(BF16)
                out_ds[here, :] = grad_s
                return carry
            lax.fori_loop(0, HALF // 16, norm_tile, 0)
            mine = out_ds.at[pl.ds(d * QUARTER + h * HALF, HALF), :]
            ds_next(1, d, h, mine).start()
            ds_twin(0, d, h, mine).start()

    for d in BOTH:
        gy_b[pl.ds(d * QUARTER, QUARTER), :] = out_ds[pl.ds(d * QUARTER, QUARTER), :]

    def project(s):
        for d in BOTH:
            for h in BOTH:
                ds_from_twin(s, d, h).wait_recv()
            block_load(s, d, 1).start()
        for d in BOTH:
            block_load(s, d, 1).wait()
        for k in BOTH:
            for d in BOTH:
                c = core if k == 0 else 1 - core
                rows = pl.ds(row(s, d, c), QUARTER)
                at = pl.ds((2 * k + d) * QUARTER, QUARTER)
                z_b[pl.ds(0, QUARTER), at] = att_v[rows, :].T
        grad_o = dot_cols(gy_b[...], wo_v[...]).astype(BF16)
        for k in BOTH:
            for d in BOTH:
                c = core if k == 0 else 1 - core
                do_v[pl.ds(row(s, d, c), QUARTER), :] = grad_o[(2 * k + d) * QUARTER:(2 * k + d + 1) * QUARTER]
        for j in range(0, hidden, WIDE):
            acc_o[:, j:j + WIDE] += dot_plain(z_b[:QUARTER, :], gy_b[:, j:j + WIDE])

    def ds_relay(s, h):
        for d in BOTH:
            ds_here(s, d, h).wait_recv()

            @pl.when(s < LAST)
            def _():
                ds_next(s + 1, d, h).start()
            ds_twin(s, d, h).start()

    def drain_columns(col, carry):
        gys.drain(col)
        xs.drain(col)

        @pl.when(col > 0)
        def _():
            for r in BOTH:
                for h in range(PARTS):
                    send_sum(col, r, h).wait_send()
        return carry

    def ds_step(s, carry):
        ds_relay(s, 0)
        project(s - 1)

        @pl.when(s < LAST)
        def _():
            weight_step(s + 1)

        @pl.when(s == LAST)
        def _():
            lax.fori_loop(0, 4, drain_columns, 0)
            for q in range(PARTS):
                give(q).wait_send()
        ds_relay(s, 1)
        for d in BOTH:
            block_load(s, d, 0).start()

        @pl.when(s < LAST)
        def _():
            weight_rest()
        for d in BOTH:
            block_load(s, d, 0).wait()
        return carry

    lax.fori_loop(1, CHIPS, ds_step, 0)
    project(LAST)

    def drain(s, carry):
        for d in BOTH:
            for h in BOTH:
                ds_twin(s, d, h).wait_send()

            @pl.when(s > 0)
            def _():
                for h in BOTH:
                    ds_here(s, d, h).wait_send()
        return carry
    lax.fori_loop(0, CHIPS, drain, 0)


def write_out(*refs):
    count = len(refs) // 2
    copies = [pltpu.make_async_copy(refs[i], refs[count + i], refs[-1].at[i]) for i in range(count)]
    for copy in copies:
        copy.start()
    for copy in copies:
        copy.wait()


def solution(mesh):
    token_spec = P(("dp", "tp"), None)
    split_cols = P("dp", "tp")
    weight_cols = P(None, "tp")
    weight_rows = P("tp", None)

    def local_backward(x_norm, grad_y, u_gate, u_up, w_gate, w_up, w_down, x_in, gamma, grad_res, attn_out, w_out):
        own, hidden = x_norm.shape
        tokens, ffn = u_gate.shape
        cols = attn_out.shape[1]
        anywhere = pl.BlockSpec(memory_space=pl.ANY)
        inside = pl.BlockSpec(memory_space=pltpu.VMEM)
        shape = jax.ShapeDtypeStruct
        dma = pltpu.SemaphoreType.DMA
        pair = (2,)
        stream_sems = [dma((2, 4, 2))] + [dma((4, 2))] * 3 + [dma((2, 4, 2))] * 2
        outs = pl.pallas_call(
            kernel,
            out_shape=[
                pltpu.VMEM((own, hidden), BF16), pltpu.VMEM((tokens, cols), BF16),
                pltpu.VMEM((ffn, hidden), F32), pltpu.VMEM((ffn, hidden), F32), pltpu.VMEM((ffn, hidden), F32),
                pltpu.VMEM((cols, hidden), F32),
                shape((tokens, hidden), BF16), shape((tokens, hidden), BF16), shape((tokens, hidden), BF16),
                shape((tokens, hidden), BF16),
                shape((CHIPS, ffn, ROWS), BF16), shape((CHIPS, ffn, ROWS), BF16), shape((CHIPS, ffn, ROWS), BF16),
            ],
            in_specs=[anywhere] * 8 + [inside] + [anywhere] * 3,
            out_specs=[inside] * 6 + [anywhere] * 7,
            scratch_shapes=[
                pltpu.VMEM((ffn, hidden), BF16), pltpu.VMEM((ffn, hidden), BF16), pltpu.VMEM((ffn, hidden), BF16),
                pltpu.VMEM((ROWS, hidden), BF16), pltpu.VMEM((ROWS, hidden), BF16),
                pltpu.VMEM((ffn, ROWS), BF16), pltpu.VMEM((ffn, ROWS), BF16),
                pltpu.VMEM((ffn, ROWS), BF16), pltpu.VMEM((ffn, ROWS), BF16), pltpu.VMEM((ffn, ROWS), BF16),
                pltpu.VMEM((ROWS, ffn), BF16), pltpu.VMEM((ROWS, ffn), BF16),
                pltpu.VMEM((own, hidden), F32), pltpu.VMEM((own, hidden), BF16), pltpu.VMEM((2, own, hidden), BF16),
                pltpu.VMEM((6, own, hidden), BF16), pltpu.VMEM((2, own, hidden), F32),
                pltpu.VMEM((2, PART, hidden), BF16), pltpu.VMEM((own, hidden), BF16),
                pltpu.VMEM((tokens, cols), BF16), pltpu.VMEM((cols, hidden), BF16),
                *stream_sems,
                *stream_sems, dma((2, 4)), *[dma((4,))] * 3,
                *[dma((CHIPS, 4))] * 4,
                dma, dma(pair), dma((3, 2, PARTS)), dma((2, 4, 2, PARTS)), dma((PARTS,)), dma((PARTS,)),
                dma((5,)), dma((4,)), dma(pair), dma((4,)), dma((3,)), dma(pair),
            ],
            compiler_params=pltpu.CompilerParams(
                collective_id=0, has_side_effects=True, vmem_limit_bytes=44 * 2 ** 20),
            name="mlp_backward",
        )(x_norm, grad_y, u_gate.T, u_up.T, w_gate.T, w_up.T, w_down, x_in, gamma, grad_res, attn_out, w_out)
        results = outs[:6]
        grad_sum, grad_attn, gw_gate, gw_up, gw_down, gw_out = pl.pallas_call(
            write_out,
            out_shape=[shape(a.shape, a.dtype) for a in results],
            in_specs=[inside] * len(results),
            out_specs=[anywhere] * len(results),
            scratch_shapes=[dma((len(results),))],
            compiler_params=pltpu.CompilerParams(vmem_limit_bytes=2 ** 20),
            name="write_out",
        )(*results)
        return grad_sum, grad_attn, gw_gate.T, gw_up.T, gw_down, gw_out

    return jax.shard_map(
        local_backward,
        mesh=mesh,
        in_specs=(token_spec, token_spec, split_cols, split_cols, weight_cols, weight_cols, weight_rows,
                  token_spec, P(None), token_spec, split_cols, weight_rows),
        out_specs=(token_spec, split_cols, split_cols, split_cols, token_spec, token_spec),
        check_vma=False,
    )
```
